128 devices in a mesh: gx: 8 (over z, core), gy: 16 (over x, y).
Axes of the slice: x: 4, y: 4, z: 4, core: 2. Of those that a mesh axis runs over, the one named last changes fastest.
Arguments:
- phase_box: bfloat16 [1024, 32, 1024], P(('gx', 'gy')), may hold values from 0 to 1
- matrix_density: float32 [256, 512, 128], P('gx', 'gy'), may hold values from 0.1 to 1
- box_corner: int32 [3, 1024], P(None, ('gx', 'gy')), may hold values from 0 to 480, as said below
Outputs:
- phase_next: bfloat16 [1024, 32, 1024], P(('gx', 'gy'))
- matrix_next: float32 [256, 512, 128], P('gx', 'gy')
The draws below stay inside these ranges and needn't reach their ends.
Inputs may be any that keep to these rules, and one draw needn't show every extreme that they name: Every box lies inside the grid. Cell c is kept by device c // 8 of gx+gy, whose gx index equals box_corner[0, c] // 32. Among the cells of one device at most 1 have the same box_corner[1] // 32, and in every draw each device has 1 such cells for some value.
All inputs are finite; a program needn't handle non-finite values.
Results may differ from the reference program's by a relative error of at most 0.0095.
Values may be sent and summed in bfloat16 or wider, within the bound.
A program may use at most 128 MiB of HBM per device.

```python
import jax
import jax.numpy as jnp
from jax import lax

B = 32
SX = 32
SY = 32
NZ = 128
CELLS_DEV = 8
CAP = 1
CELLS = 1024
NX = 256
NY = 512
N_GX = 8
N_GY = 16


def draw_box_corner(key, part):
    keys = jax.random.split(key, 7)
    slot_number = N_GY * CAP
    cell_group = max(N_GY // 4, 1)
    home_slot = jnp.arange(slot_number, dtype=jnp.int32) // CAP
    anchor = jax.random.randint(keys[0], (N_GX, 1), 0, N_GY)
    sure_choice = jax.random.randint(keys[1], (N_GX, 1), 0, cell_group)
    relative_offset = (home_slot[None, :] - anchor) % N_GY
    reward_extra = jnp.where(relative_offset < cell_group, 2 ** 20, 0) + jnp.where(relative_offset == sure_choice, 2 ** 22, 0)
    random_jitter = jax.random.randint(keys[2], (N_GX, N_GY, slot_number), 0, 2 ** 20)
    score_values = (random_jitter + reward_extra[:, None, :]) * slot_number + jnp.arange(slot_number, dtype=jnp.int32)
    chosen = lax.top_k(score_values.astype(jnp.int32), CELLS_DEV)[1] // CAP
    shuffle = jax.random.randint(keys[3], (N_GX, N_GY, CELLS_DEV), 0, 2 ** 16) * CELLS_DEV + jnp.arange(CELLS_DEV, dtype=jnp.int32)
    order = jnp.argsort(shuffle, axis=-1)
    homes = jnp.take_along_axis(chosen, order, axis=-1).astype(jnp.int32)
    row_number = jnp.arange(N_GX, dtype=jnp.int32)[:, None, None]
    limit_x = jnp.minimum(SX, N_GX * SX - B + 1 - row_number * SX)
    first_dim = row_number * SX + jax.random.randint(keys[4], (N_GX, N_GY, CELLS_DEV), 0, limit_x)
    limit_y = jnp.minimum(SY, N_GY * SY - B + 1 - homes * SY)
    second_dim = homes * SY + jax.random.randint(keys[5], (N_GX, N_GY, CELLS_DEV), 0, limit_y)
    third_dim = jax.random.randint(keys[6], (N_GX, N_GY, CELLS_DEV), 0, NZ - B + 1)
    return jnp.stack([first_dim, second_dim, third_dim]).reshape(3, N_GX * N_GY * CELLS_DEV).astype(jnp.int32)


def steps_of(stream_key, extent, shards, low, largest):
    loudness = 1.0
    for axis_at, parts in shards:
        steps = jax.random.uniform(jax.random.fold_in(jax.random.fold_in(stream_key, 6), axis_at), (parts,), jnp.float32, low / len(shards), largest / len(shards))
        loudness = loudness * jnp.repeat(jnp.exp(steps), extent[axis_at] // parts).reshape((-1,) + (1,) * (len(extent) - 1 - axis_at))
    return loudness


def setup_inputs(seed: int = 0) -> dict:
    seeds = jax.random.split(jax.random.key(seed), 4)
    return {
        "phase_box": jnp.clip(1.0 * jax.random.uniform(seeds[0], (CELLS, B, B * B), jnp.float32) ** steps_of(seeds[0], (CELLS, B, B * B), ((0, 128),), -0.2, 0.2), 0.0, 1.0).astype(jnp.bfloat16),
        "matrix_density": jnp.clip(0.1 + 0.9 * jax.random.uniform(seeds[1], (NX, NY, NZ), jnp.float32) ** steps_of(seeds[1], (NX, NY, NZ), ((0, 8), (1, 16)), -0.2, 0.2), 0.1, 1.0),
        "box_corner": draw_box_corner(jax.random.fold_in(seeds[3], 71), 0),
    }


time_step = 0.1
well_depth = 4.0
matrix_drive = 1.0
repel_rate = 2.0
decay_rate = 0.5


def laplace(volume):
    box_edge = volume.shape[1]
    box_area = volume.shape[2]
    depth_pos = jnp.arange(box_area, dtype=jnp.int32) % box_edge
    pad_one = jnp.zeros(volume.shape[:2] + (1,), jnp.float32)
    pad_row = jnp.zeros(volume.shape[:2] + (box_edge,), jnp.float32)
    pad_slab = jnp.zeros((volume.shape[0], 1, box_area), jnp.float32)
    upward = jnp.where(depth_pos < box_edge - 1, jnp.concatenate([volume[:, :, 1:], pad_one], 2), 0.0)
    downward = jnp.where(depth_pos > 0, jnp.concatenate([pad_one, volume[:, :, :-1]], 2), 0.0)
    beside = jnp.concatenate([volume[:, :, box_edge:], pad_row], 2) + jnp.concatenate([pad_row, volume[:, :, :-box_edge]], 2)
    across = jnp.concatenate([volume[:, 1:], pad_slab], 1) + jnp.concatenate([pad_slab, volume[:, :-1]], 1)
    return upward + downward + beside + across - 6.0 * volume


def advance(current, density, crowding):
    others = crowding - current * current
    reaction = well_depth * current * (1.0 - current) * (current - 0.5 + matrix_drive * (density - 0.5))
    return current + time_step * (laplace(current) + reaction - repel_rate * current * others)


def cell_index(first_dim, second_dim, third_dim, row_length, grid_depth, box_edge):
    leading = jnp.arange(box_edge, dtype=jnp.int32)
    within = jnp.arange(box_edge * box_edge, dtype=jnp.int32)
    offset = leading[:, None] * (row_length * grid_depth) + (within // box_edge)[None, :] * grid_depth + (within % box_edge)[None, :]
    anchor = (first_dim * row_length + second_dim) * grid_depth + third_dim
    return (anchor[:, None, None] + offset[None]).astype(jnp.int32)


def reference(phase_box, matrix_density, box_corner):
    grid_shape = matrix_density.shape
    flat_density = matrix_density.reshape(-1)
    blocks = CELLS // CELLS_DEV
    corners = jnp.moveaxis(box_corner.reshape(3, blocks, CELLS_DEV), 1, 0)
    phases = phase_box.reshape(blocks, CELLS_DEV, B, B * B)

    def add_square(running, payload):
        corner, volume = payload
        flat_index = cell_index(corner[0], corner[1], corner[2], NY, NZ, B)
        current = volume.astype(jnp.float32)
        return running.at[flat_index].add(current * current), None

    crowding, _ = lax.scan(add_square, jnp.zeros(flat_density.shape, jnp.float32), (corners, phases))

    def update(payload):
        corner, volume = payload
        flat_index = cell_index(corner[0], corner[1], corner[2], NY, NZ, B)
        return advance(volume.astype(jnp.float32), flat_density[flat_index], crowding[flat_index]).astype(jnp.bfloat16)

    updated = lax.map(update, (corners, phases))

    def add_phase(running, payload):
        corner, volume = payload
        flat_index = cell_index(corner[0], corner[1], corner[2], NY, NZ, B)
        return running.at[flat_index].add(volume.astype(jnp.float32)), None

    deposit, _ = lax.scan(add_phase, jnp.zeros(flat_density.shape, jnp.float32), (corners, updated))
    matrix_next = matrix_density - decay_rate * matrix_density * deposit.reshape(grid_shape)
    return updated.reshape(CELLS, B, B * B), matrix_next
```

```python
import jax
import jax.numpy as jnp
from jax import lax
from jax.experimental import pallas as pl
from jax.experimental.pallas import tpu as pltpu
from jax.sharding import PartitionSpec as P

B = 32
LANES = 128
GROUP = LANES // B


def shifted(block, axis, distance):
    devices = range(lax.axis_size(axis))
    route = [(i - distance, i) for i in devices if i - distance in devices]
    return lax.ppermute(block, axis, route)


def lane_index():
    return lax.broadcasted_iota(jnp.int32, (B, LANES), 1)


def crowd_kernel(places, boxes, wide):
    wide[...] = jnp.zeros_like(wide)
    lane = lane_index()

    def one(s, carry):
        @pl.when(places[s, 3] > 0)
        def _():
            lx, ly, lz = places[s, 0], places[s, 1], places[s, 2]
            inside = (lane >= lz) & (lane < lz + B)
            for j in range(B // GROUP):
                v = boxes[s, :, j * LANES : (j + 1) * LANES].astype(jnp.float32)
                v = v * v
                for i in range(GROUP):
                    r = pltpu.roll(v, lax.rem(lz + (LANES - B * i), LANES), 1)
                    at = (ly + (GROUP * j + i), pl.ds(lx, B), slice(None))
                    wide[at] = wide[at] + jnp.where(inside, r, 0.0)

        return carry

    lax.fori_loop(0, boxes.shape[0], one, 0)


def update_kernel(places, boxes, crowd, density, settled, wide):
    wide[...] = jnp.zeros_like(wide)
    lane = lane_index()
    row = lax.broadcasted_iota(jnp.int32, (B, LANES), 0)
    depth = lax.rem(lane, B)
    columns = B // GROUP

    def one(s, carry):
        @pl.when(places[s, 3] > 0)
        def _():
            lx, ly, lz = places[s, 0], places[s, 1], places[s, 2]
            inside = (lane >= lz) & (lane < lz + B)

            def column(j):
                return boxes[s, :, j * LANES : (j + 1) * LANES].astype(jnp.float32)

            none = jnp.zeros((B, LANES), jnp.float32)
            before, p = none, column(0)
            for j in range(columns):
                after = column(j + 1) if j + 1 < columns else none
                cr, dn = none, none
                for i in range(GROUP):
                    at = (ly + (GROUP * j + i), pl.ds(lx, B), slice(None))
                    amount = lax.rem(LANES + B * i - lz, LANES)
                    c = pltpu.roll(crowd[at], amount, 1)
                    d = pltpu.roll(density[at], amount, 1)
                    if i == 0:
                        cr, dn = c, d
                    else:
                        cr = jnp.where(lane >= B * i, c, cr)
                        dn = jnp.where(lane >= B * i, d, dn)
                up = jnp.where(depth < B - 1, pltpu.roll(p, LANES - 1, 1), 0.0)
                down = jnp.where(depth > 0, pltpu.roll(p, 1, 1), 0.0)
                beyond = pltpu.roll(jnp.where(lane < B, after, p), LANES - B, 1)
                behind = pltpu.roll(jnp.where(lane >= LANES - B, before, p), B, 1)
                across = jnp.where(row < B - 1, pltpu.roll(p, B - 1, 0), 0.0) + jnp.where(
                    row > 0, pltpu.roll(p, 1, 0), 0.0
                )
                lap = up + down + beyond + behind + across - 6.0 * p
                others = cr - p * p
                reaction = 4.0 * p * (1.0 - p) * (p - 0.5 + (dn - 0.5))
                new = (p + 0.1 * (lap + reaction - 2.0 * p * others)).astype(jnp.bfloat16)
                settled[s, :, j * LANES : (j + 1) * LANES] = new
                v = new.astype(jnp.float32)
                for i in range(GROUP):
                    r = pltpu.roll(v, lax.rem(lz + (LANES - B * i), LANES), 1)
                    at = (ly + (GROUP * j + i), pl.ds(lx, B), slice(None))
                    wide[at] = wide[at] + jnp.where(inside, r, 0.0)
                before, p = p, after

        @pl.when(places[s, 3] <= 0)
        def _():
            settled[s] = jnp.zeros(settled.shape[1:], settled.dtype)

        return carry

    lax.fori_loop(0, boxes.shape[0], one, 0)


def in_vmem(n):
    return [pl.BlockSpec(memory_space=pltpu.VMEM)] * n


def per_device(phase_box, matrix_density, box_corner):
    slab_rows, slab_cols, grid_depth = matrix_density.shape
    peers = lax.axis_size("gy")
    home = box_corner[1] // slab_cols
    local = jnp.stack(
        [
            box_corner[0] - lax.axis_index("gx") * slab_rows,
            box_corner[1] - home * slab_cols,
            box_corner[2],
            jnp.ones_like(home),
        ],
        1,
    )
    outbox = jnp.zeros((peers,) + phase_box.shape[1:], jnp.bfloat16).at[home].set(phase_box)
    places = jnp.zeros((peers, 4), jnp.int32).at[home].set(local)
    places = lax.all_to_all(places, "gy", 0, 0, tiled=True)
    boxes = lax.all_to_all(outbox, "gy", 0, 0, tiled=True)

    field = jax.ShapeDtypeStruct((2 * slab_cols, 2 * slab_rows, grid_depth), jnp.float32)
    smem = [pl.BlockSpec(memory_space=pltpu.SMEM)]
    crowd = pl.pallas_call(
        crowd_kernel,
        out_shape=field,
        in_specs=smem + in_vmem(1),
        out_specs=in_vmem(1)[0],
        name="crowd",
    )(places, boxes)

    turned = jnp.swapaxes(matrix_density, 0, 1)
    low = turned.astype(jnp.bfloat16)
    wide = jnp.concatenate([low, shifted(low, "gx", -1)], 1)
    density = jnp.concatenate([wide, shifted(wide, "gy", -1)], 0).astype(jnp.float32)

    sent = crowd.astype(jnp.bfloat16)
    crowd = crowd + jnp.concatenate(
        [shifted(sent[:, slab_rows:], "gx", 1), shifted(sent[:, :slab_rows], "gx", -1)], 1
    ).astype(jnp.float32)
    sent = crowd.astype(jnp.bfloat16)
    crowd = crowd + jnp.concatenate(
        [shifted(sent[slab_cols:], "gy", 1), shifted(sent[:slab_cols], "gy", -1)], 0
    ).astype(jnp.float32)

    settled, deposit = pl.pallas_call(
        update_kernel,
        out_shape=(jax.ShapeDtypeStruct(boxes.shape, jnp.bfloat16), field),
        in_specs=smem + in_vmem(3),
        out_specs=tuple(in_vmem(2)),
        name="update",
    )(places, boxes, crowd, density)

    returned = lax.all_to_all(settled, "gy", 0, 0, tiled=True)
    phase_next = returned[home]
    sent = deposit[:, slab_rows:].astype(jnp.bfloat16)
    deposit = deposit[:, :slab_rows] + shifted(sent, "gx", 1).astype(jnp.float32)
    sent = deposit[slab_cols:].astype(jnp.bfloat16)
    deposit = deposit[:slab_cols] + shifted(sent, "gy", 1).astype(jnp.float32)
    matrix_next = matrix_density - 0.5 * matrix_density * jnp.swapaxes(deposit, 0, 1)
    return phase_next, matrix_next


def solution(mesh):
    return jax.shard_map(
        per_device,
        mesh=mesh,
        in_specs=(P(("gx", "gy"), None, None), P("gx", "gy", None), P(None, ("gx", "gy"))),
        out_specs=(P(("gx", "gy"), None, None), P("gx", "gy", None)),
        check_vma=False,
    )
```

```python
import jax
import jax.numpy as jnp
from jax import lax
from jax.experimental import pallas as pl
from jax.experimental.pallas import tpu as pltpu
from jax.sharding import PartitionSpec as P

B = 32
LANES = 128
GROUP = LANES // B
SIDE = 4
OFFSETS = [
    (2, 2), (2, 1), (2, 3), (1, 2), (3, 2), (2, 0), (0, 2), (1, 1),
    (3, 3), (1, 3), (3, 1), (0, 1), (0, 3), (1, 0), (3, 0),
]


def signal(axis, target):
    pl.semaphore_signal(
        pltpu.get_barrier_semaphore(),
        inc=1,
        device_id={axis: target},
        device_id_type=pl.DeviceIdType.MESH,
    )


def remote(src, dst, send, recv, axis, target):
    return pltpu.make_async_remote_copy(
        src_ref=src,
        dst_ref=dst,
        send_sem=send,
        recv_sem=recv,
        device_id={axis: target},
        device_id_type=pl.DeviceIdType.MESH,
    )


def peers_of(me):
    high, low = me // SIDE, lax.rem(me, SIDE)
    there = [lax.rem(high + p, SIDE) * SIDE + lax.rem(low + q, SIDE) for p, q in OFFSETS]
    back = [
        lax.rem(high + SIDE - p, SIDE) * SIDE + lax.rem(low + SIDE - q, SIDE) for p, q in OFFSETS
    ]
    return there, back


def gather_kernel(
    source, phase, table, low, boxes, places, density,
    outbox, half, send, recv, table_send, table_recv, rim_send, rim_recv, own,
):
    me, row = lax.axis_index("gy"), lax.axis_index("gx")
    columns, rows = lax.axis_size("gy"), lax.axis_size("gx")
    edge = low.shape[0]
    there, back = peers_of(me)
    for target in there:
        signal("gy", target)

    @pl.when(row > 0)
    def _():
        signal("gx", row - 1)

    @pl.when(row < rows - 1)
    def _():
        signal("gx", row + 1)

    def fill(s, carry):
        outbox[s] = phase[source[s]]
        return carry

    lax.fori_loop(0, columns, fill, 0)
    half[:edge] = low[...]

    @pl.when(me == columns - 1)
    def _():
        half[edge:] = jnp.zeros((edge,) + half.shape[1:], half.dtype)

    neighbours = (row > 0).astype(jnp.int32) + (row < rows - 1).astype(jnp.int32)
    pl.semaphore_wait(pltpu.get_barrier_semaphore(), len(OFFSETS) + neighbours)

    along_y = remote(low, half.at[pl.ds(edge, edge)], rim_send.at[0], rim_recv.at[0], "gy", me - 1)

    @pl.when(me > 0)
    def _():
        along_y.start()

    sends = []
    for k, target in enumerate(there):
        sends.append(
            remote(table.at[target], places.at[me], table_send.at[k], table_recv.at[k], "gy", target)
        )
        sends[-1].start()
    for k, target in enumerate(there):
        sends.append(remote(outbox.at[target], boxes.at[me], send.at[k], recv.at[k], "gy", target))
        sends[-1].start()
    stays = [
        pltpu.make_async_copy(outbox.at[me], boxes.at[me], own.at[0]),
        pltpu.make_async_copy(table.at[me], places.at[me], own.at[1]),
    ]
    for copy in stays:
        copy.start()

    @pl.when(me < columns - 1)
    def _():
        along_y.wait_recv()

    kept = pltpu.make_async_copy(half, density.at[:, pl.ds(0, edge)], own.at[2])
    kept.start()
    along_x = remote(
        half, density.at[:, pl.ds(edge, edge)], rim_send.at[1], rim_recv.at[1], "gx", row - 1
    )

    @pl.when(row > 0)
    def _():
        along_x.start()
        along_x.wait_send()

    @pl.when(row < rows - 1)
    def _():
        along_x.wait_recv()

    @pl.when(me > 0)
    def _():
        along_y.wait_send()

    for k, sender in enumerate(back):
        remote(table.at[me], places.at[sender], table_send.at[k], table_recv.at[k], "gy", sender).wait_recv()
        remote(outbox.at[me], boxes.at[sender], send.at[k], recv.at[k], "gy", sender).wait_recv()
    for copy in sends:
        copy.wait_send()
    for copy in stays + [kept]:
        copy.wait()


def rim_kernel(own, crowd, from_x, full, from_y, x_send, x_recv, y_send, y_recv):
    me, row = lax.axis_index("gy"), lax.axis_index("gx")
    columns, rows = lax.axis_size("gy"), lax.axis_size("gx")
    edge = own.shape[1] // 2
    part = edge // 2
    sides = (
        (row < rows - 1, row + 1, slice(edge, 2 * edge), 0),
        (row > 0, row - 1, slice(0, edge), 1),
    )
    count = 0
    for axis, at, size in (("gx", row, rows), ("gy", me, columns)):
        for there, target in ((at > 0, at - 1), (at < size - 1, at + 1)):
            count += there.astype(jnp.int32)

            @pl.when(there)
            def _():
                signal(axis, target)

    pl.semaphore_wait(pltpu.get_barrier_semaphore(), count)
    chunks = [slice(p, p + part) for p in (0, edge, part, edge + part)]

    def along_x(c, side):
        _, target, half, k = sides[side]
        return remote(
            own.at[chunks[c], half],
            from_x.at[k, chunks[c]],
            x_send.at[k, c],
            x_recv.at[k, c],
            "gx",
            target,
        )

    def along_y(c):
        start = chunks[c].start
        up = start >= edge
        target = me + 1 if up else me - 1
        rest = slice(start % edge, start % edge + part)
        copy = remote(
            full.at[chunks[c]], from_y.at[int(up), rest], y_send.at[c], y_recv.at[c], "gy", target
        )
        sends = me < columns - 1 if up else me > 0
        takes = me > 0 if up else me < columns - 1
        return copy, sends, takes

    for c in range(len(chunks)):
        for side in range(2):

            @pl.when(sides[side][0])
            def _():
                along_x(c, side).start()

    for c, rest in enumerate(chunks):
        for side in range(2):
            takes, half = sides[1 - side][0], slice(edge, 2 * edge) if side else slice(0, edge)

            @pl.when(takes)
            def _():
                along_x(c, side).wait_recv()
                full[rest, half] = own[rest, half] + from_x[side, rest]

            @pl.when(jnp.logical_not(takes))
            def _():
                full[rest, half] = own[rest, half]

        copy, sends, _ = along_y(c)

        @pl.when(sends)
        def _():
            copy.start()

    for c in range(len(chunks)):
        copy, sends, takes = along_y(c)
        up = chunks[c].start >= edge
        start = chunks[c].start % edge
        rest = slice(start, start + part)
        rows_in = slice(start, start + part) if up else slice(edge + start, edge + start + part)

        @pl.when(takes)
        def _():
            copy.wait_recv()
            crowd[rows_in] = full[rows_in].astype(jnp.float32) + from_y[int(up), rest].astype(jnp.float32)

        @pl.when(jnp.logical_not(takes))
        def _():
            crowd[rows_in] = full[rows_in].astype(jnp.float32)

        @pl.when(sends)
        def _():
            copy.wait_send()

        for side in range(2):

            @pl.when(sides[side][0])
            def _():
                along_x(c, side).wait_send()


def return_kernel(
    settled, wide, returned, deposit, from_x, outgoing, from_y,
    send, recv, x_send, x_recv, y_send, y_recv, own,
):
    me, row = lax.axis_index("gy"), lax.axis_index("gx")
    columns, rows = lax.axis_size("gy"), lax.axis_size("gx")
    edge = wide.shape[1] // 2
    there, back = peers_of(me)
    for target in there:
        signal("gy", target)

    @pl.when(row > 0)
    def _():
        signal("gx", row - 1)

    @pl.when(row < rows - 1)
    def _():
        signal("gx", row + 1)

    neighbours = (row > 0).astype(jnp.int32) + (row < rows - 1).astype(jnp.int32)
    pl.semaphore_wait(pltpu.get_barrier_semaphore(), len(OFFSETS) + neighbours)

    halves = (slice(edge, 2 * edge), slice(0, edge))

    def along_x(k):
        return remote(
            wide.at[halves[k], pl.ds(edge, edge)], from_x.at[k], x_send.at[k], x_recv.at[k], "gx", row + 1
        )

    @pl.when(row < rows - 1)
    def _():
        for k in range(2):
            along_x(k).start()

    sends = []
    for k, target in enumerate(there):
        sends.append(
            remote(settled.at[target], returned.at[me], send.at[k], recv.at[k], "gy", target)
        )
        sends[-1].start()
    stays = pltpu.make_async_copy(settled.at[me], returned.at[me], own.at[0])
    stays.start()

    @pl.when(row > 0)
    def _():
        along_x(0).wait_recv()
        outgoing[...] = wide[edge:, :edge] + from_x[0]

    @pl.when(row == 0)
    def _():
        outgoing[...] = wide[edge:, :edge]

    along_y = remote(outgoing, from_y, y_send.at[0], y_recv.at[0], "gy", me + 1)

    @pl.when(me < columns - 1)
    def _():
        along_y.start()

    @pl.when(row > 0)
    def _():
        along_x(1).wait_recv()
        deposit[...] = wide[:edge, :edge].astype(jnp.float32) + from_x[1].astype(jnp.float32)

    @pl.when(row == 0)
    def _():
        deposit[...] = wide[:edge, :edge].astype(jnp.float32)

    @pl.when(me > 0)
    def _():
        along_y.wait_recv()
        deposit[...] = deposit[...] + from_y[...].astype(jnp.float32)

    for k, sender in enumerate(back):
        remote(settled.at[me], returned.at[sender], send.at[k], recv.at[k], "gy", sender).wait_recv()
    for copy in sends:
        copy.wait_send()
    stays.wait()

    @pl.when(me < columns - 1)
    def _():
        along_y.wait_send()

    @pl.when(row < rows - 1)
    def _():
        for k in range(2):
            along_x(k).wait_send()


def lane_index():
    return lax.broadcasted_iota(jnp.int32, (B, LANES), 1)


def fetch_places(table, places, sem):
    copy = pltpu.make_async_copy(table.at[:, 0], places, sem)
    copy.start()
    copy.wait()


def crowd_kernel(table, boxes, out, wide, places, sem):
    fetch_places(table, places, sem)
    wide[...] = jnp.zeros_like(wide)
    lane = lane_index()

    def one(s, carry):
        @pl.when(places[s, 3] > 0)
        def _():
            lx, ly, lz = places[s, 0], places[s, 1], places[s, 2]
            inside = (lane >= lz) & (lane < lz + B)
            for j in range(B // GROUP):
                v = boxes[s, :, j * LANES : (j + 1) * LANES].astype(jnp.float32)
                v = v * v
                for i in range(GROUP):
                    r = pltpu.roll(v, lax.rem(lz + (LANES - B * i), LANES), 1)
                    at = (ly + (GROUP * j + i), pl.ds(lx, B), slice(None))
                    wide[at] = wide[at] + jnp.where(inside, r, 0.0)

        return carry

    lax.fori_loop(0, boxes.shape[0], one, 0)
    out[...] = wide[...].astype(out.dtype)


def update_kernel(table, boxes, crowd, low, settled, out, density, wide, places, sem):
    fetch_places(table, places, sem)
    density[...] = low[...].astype(jnp.float32)
    wide[...] = jnp.zeros_like(wide)
    lane = lane_index()
    row = lax.broadcasted_iota(jnp.int32, (B, LANES), 0)
    depth = lax.rem(lane, B)
    columns = B // GROUP

    def one(s, carry):
        @pl.when(places[s, 3] > 0)
        def _():
            lx, ly, lz = places[s, 0], places[s, 1], places[s, 2]
            inside = (lane >= lz) & (lane < lz + B)

            def column(j):
                return boxes[s, :, j * LANES : (j + 1) * LANES].astype(jnp.float32)

            none = jnp.zeros((B, LANES), jnp.float32)
            before, p = none, column(0)
            for j in range(columns):
                after = column(j + 1) if j + 1 < columns else none
                cr, dn = none, none
                for i in range(GROUP):
                    at = (ly + (GROUP * j + i), pl.ds(lx, B), slice(None))
                    amount = lax.rem(LANES + B * i - lz, LANES)
                    c = pltpu.roll(crowd[at], amount, 1)
                    d = pltpu.roll(density[at], amount, 1)
                    if i == 0:
                        cr, dn = c, d
                    else:
                        cr = jnp.where(lane >= B * i, c, cr)
                        dn = jnp.where(lane >= B * i, d, dn)
                up = jnp.where(depth < B - 1, pltpu.roll(p, LANES - 1, 1), 0.0)
                down = jnp.where(depth > 0, pltpu.roll(p, 1, 1), 0.0)
                beyond = pltpu.roll(jnp.where(lane < B, after, p), LANES - B, 1)
                behind = pltpu.roll(jnp.where(lane >= LANES - B, before, p), B, 1)
                across = jnp.where(row < B - 1, pltpu.roll(p, B - 1, 0), 0.0) + jnp.where(
                    row > 0, pltpu.roll(p, 1, 0), 0.0
                )
                lap = up + down + beyond + behind + across - 6.0 * p
                others = cr - p * p
                reaction = 4.0 * p * (1.0 - p) * (p - 0.5 + (dn - 0.5))
                new = (p + 0.1 * (lap + reaction - 2.0 * p * others)).astype(jnp.bfloat16)
                settled[s, :, j * LANES : (j + 1) * LANES] = new
                v = new.astype(jnp.float32)
                for i in range(GROUP):
                    r = pltpu.roll(v, lax.rem(lz + (LANES - B * i), LANES), 1)
                    at = (ly + (GROUP * j + i), pl.ds(lx, B), slice(None))
                    wide[at] = wide[at] + jnp.where(inside, r, 0.0)
                before, p = p, after

        @pl.when(places[s, 3] <= 0)
        def _():
            settled[s] = jnp.zeros(settled.shape[1:], settled.dtype)

        return carry

    lax.fori_loop(0, boxes.shape[0], one, 0)
    out[...] = wide[...].astype(out.dtype)


VMEM = pl.BlockSpec(memory_space=pltpu.VMEM)
ANY = pl.BlockSpec(memory_space=pl.ANY)
SMEM = pl.BlockSpec(memory_space=pltpu.SMEM)
LIMIT = 24 * 2**20


def like(shape, dtype):
    return jax.ShapeDtypeStruct(shape, dtype)


def dma(*shape):
    return pltpu.SemaphoreType.DMA(shape)


def linked(number):
    return pltpu.CompilerParams(
        collective_id=number, has_side_effects=True, vmem_limit_bytes=LIMIT
    )


def per_device(phase_box, matrix_density, box_corner):
    slab_rows, slab_cols, grid_depth = matrix_density.shape
    peers = lax.axis_size("gy")
    cells = phase_box.shape[0]
    home = box_corner[1] // slab_cols
    local = jnp.stack(
        [
            box_corner[0] - lax.axis_index("gx") * slab_rows,
            box_corner[1] - home * slab_cols,
            box_corner[2],
            jnp.ones_like(home),
        ],
        1,
    )
    match = (home[None, :] == jnp.arange(peers, dtype=jnp.int32)[:, None]).astype(jnp.int32)
    source = jnp.sum(match * jnp.arange(cells, dtype=jnp.int32)[None, :], 1)
    table = jnp.sum(match[:, :, None] * local[None], 1)
    table = jnp.pad(jnp.broadcast_to(table[:, None], (peers, 8, 4)), ((0, 0), (0, 0), (0, LANES - 4)))
    low = jnp.swapaxes(matrix_density, 0, 1).astype(jnp.bfloat16)

    bf16, f32 = jnp.bfloat16, jnp.float32
    hops = len(OFFSETS)
    slots = (peers,) + phase_box.shape[1:]
    wide = (2 * slab_cols, 2 * slab_rows, grid_depth)
    half = (2 * slab_cols, slab_rows, grid_depth)
    quarter = (slab_cols, slab_rows, grid_depth)
    boxes, places, density = pl.pallas_call(
        gather_kernel,
        out_shape=(like(slots, bf16), like(table.shape, jnp.int32), like(wide, bf16)),
        in_specs=[SMEM, VMEM, VMEM, VMEM],
        out_specs=(ANY, ANY, ANY),
        scratch_shapes=[
            pltpu.VMEM(slots, bf16),
            pltpu.VMEM(half, bf16),
            dma(hops), dma(hops), dma(hops), dma(hops), dma(2), dma(2), dma(3),
        ],
        compiler_params=linked(0),
        name="gather",
    )(source, phase_box, table, low)

    spots = [pltpu.SMEM((peers, LANES), jnp.int32), dma()]
    quiet = pltpu.CompilerParams(vmem_limit_bytes=LIMIT)
    crowd = pl.pallas_call(
        crowd_kernel,
        out_shape=like(wide, bf16),
        in_specs=[ANY, VMEM],
        out_specs=VMEM,
        scratch_shapes=[pltpu.VMEM(wide, f32)] + spots,
        compiler_params=quiet,
        name="crowd",
    )(places, boxes)

    crowd = pl.pallas_call(
        rim_kernel,
        out_shape=like(wide, f32),
        in_specs=[VMEM],
        out_specs=VMEM,
        scratch_shapes=[
            pltpu.VMEM((2,) + half, bf16),
            pltpu.VMEM(wide, bf16),
            pltpu.VMEM((2, slab_cols) + wide[1:], bf16),
            dma(2, 4), dma(2, 4), dma(4), dma(4),
        ],
        compiler_params=linked(1),
        name="rim",
    )(crowd)

    settled, deposit = pl.pallas_call(
        update_kernel,
        out_shape=(like(slots, bf16), like(wide, bf16)),
        in_specs=[ANY, VMEM, VMEM, VMEM],
        out_specs=(VMEM, VMEM),
        scratch_shapes=[pltpu.VMEM(wide, f32), pltpu.VMEM(wide, f32)] + spots,
        compiler_params=quiet,
        name="update",
    )(places, boxes, crowd, density)

    returned, deposit = pl.pallas_call(
        return_kernel,
        out_shape=(like(slots, bf16), like(quarter, f32)),
        in_specs=[VMEM, VMEM],
        out_specs=(ANY, VMEM),
        scratch_shapes=[
            pltpu.VMEM((2,) + quarter, bf16),
            pltpu.VMEM(quarter, bf16),
            pltpu.VMEM(quarter, bf16),
            dma(hops), dma(hops), dma(2), dma(2), dma(1), dma(1), dma(1),
        ],
        compiler_params=linked(2),
        name="return",
    )(settled, deposit)

    phase_next = returned[home]
    matrix_next = matrix_density - 0.5 * matrix_density * jnp.swapaxes(deposit, 0, 1)
    return phase_next, matrix_next


def solution(mesh):
    return jax.shard_map(
        per_device,
        mesh=mesh,
        in_specs=(P(("gx", "gy"), None, None), P("gx", "gy", None), P(None, ("gx", "gy"))),
        out_specs=(P(("gx", "gy"), None, None), P("gx", "gy", None)),
        check_vma=False,
    )
```

```python
import jax
import jax.numpy as jnp
from jax import lax
from jax.experimental import pallas as pl
from jax.experimental.pallas import tpu as pltpu
from jax.sharding import PartitionSpec as P

B = 32
LANES = 128
GROUP = LANES // B
SIDE = 4

def signal(axis, target):
    pl.semaphore_signal(
        pltpu.get_barrier_semaphore(),
        inc=1,
        device_id={axis: target},
        device_id_type=pl.DeviceIdType.MESH,
    )


def remote(src, dst, send, recv, axis, target):
    return pltpu.make_async_remote_copy(
        src_ref=src,
        dst_ref=dst,
        send_sem=send,
        recv_sem=recv,
        device_id={axis: target},
        device_id_type=pl.DeviceIdType.MESH,
    )


def greet():
    me, row = lax.axis_index("gy"), lax.axis_index("gx")
    columns, rows = lax.axis_size("gy"), lax.axis_size("gx")
    high, low = me // SIDE, lax.rem(me, SIDE)
    count = 0
    for step in (1, SIDE - 1):
        signal("gy", lax.rem(high + step, SIDE) * SIDE + low)
        signal("gy", high * SIDE + lax.rem(low + step, SIDE))
        count += 2
    for axis, at, size, step in (("gx", row, rows, 1), ("gx", row, rows, -1)):
        there = (at < size - 1) if step > 0 else (at > 0)
        count += there.astype(jnp.int32)

        @pl.when(there)
        def _():
            signal(axis, at + step)

    for step in (1, -1):
        far = (low == (SIDE - 1 if step > 0 else 0)) & (
            (me < columns - 1) if step > 0 else (me > 0)
        )
        count += far.astype(jnp.int32)

        @pl.when(far)
        def _():
            signal("gy", me + step)

    return count


class Exchange:
    def __init__(self, src, dst, stage, relay, send, recv, own, share_y):
        self.src, self.dst, self.stage, self.relay = src, dst, stage, relay
        self.send, self.recv, self.own = send, recv, own
        me = lax.axis_index("gy")
        self.at = (me // SIDE, lax.rem(me, SIDE))
        self.share = (SIDE // 2, share_y)
        self.rows = src.shape[2] // 2

    def turn(self, axis, step):
        return lax.rem(self.at[axis] + SIDE + step, SIDE)

    def device(self, axis, step):
        other, moved = self.at[1 - axis], self.turn(axis, step)
        return moved * SIDE + other if axis == 0 else other * SIDE + moved

    def whole(self, ref, half, first, second):
        rest = pl.ds(half * self.rows, self.rows)
        return ref.at[first, second, rest]

    def block(self, half, stage, goal, part):
        if stage == 1:
            return self.stage.at[half, part, goal]
        return self.whole(self.src, half, *((goal, part) if half == 0 else (part, goal)))

    def place(self, half, stage, origin, part):
        if stage == 0:
            return self.stage.at[half, origin, part]
        return self.whole(self.dst, half, *((part, origin) if half == 0 else (origin, part)))

    def copies(self, half, stage):
        axis = (half + stage) % 2
        share = self.share[axis]
        parts = (pl.ds(0, share), pl.ds(share, SIDE - share))
        sizes = (share, SIDE - share)
        every = pl.ds(0, SIDE)
        out = []
        for kind in ("relay", "direct", "forward"):
            for side in range(2):
                step = 1 if side == 0 else -1
                if kind == "direct":
                    src = self.block(half, stage, self.turn(axis, step), every)
                    dst = self.place(half, stage, self.at[axis], every)
                else:
                    hold = self.relay.at[half, stage, side, pl.ds(0, sizes[side])]
                    if kind == "relay":
                        src, dst = self.block(half, stage, self.turn(axis, 2), parts[side]), hold
                    else:
                        src = hold
                        dst = self.place(half, stage, self.turn(axis, -step), parts[side])
                at = (half, stage, len(out))
                out.append(
                    remote(src, dst, self.send.at[at], self.recv.at[at], "gy", self.device(axis, step))
                )
        return out

    def prepare(self):
        x, y = self.at
        self.stage[0, x] = self.src[x, :, : self.rows]
        self.stage[1, y] = self.src[:, y, self.rows :]

    def start(self, stage, half):
        copies = self.copies(half, stage)
        for copy in copies[:4]:
            copy.start()
        if stage == 1:
            self.kept(half).start()

    def forward(self, stage, half):
        copies = self.copies(half, stage)
        for side in range(2):
            copies[side].wait_recv()
            copies[4 + side].start()

    def arrive(self, stage, half):
        for copy in self.copies(half, stage)[2:]:
            copy.wait_recv()

    def kept(self, half):
        axis = (half + 1) % 2
        every = pl.ds(0, SIDE)
        return pltpu.make_async_copy(
            self.block(half, 1, self.at[axis], every),
            self.place(half, 1, self.at[axis], every),
            self.own.at[half],
        )

    def finish(self):
        for half in range(2):
            for stage in range(2):
                for copy in self.copies(half, stage):
                    copy.wait_send()
            self.kept(half).wait()


def gather_kernel(
    source, phase, table, low, boxes, places, density,
    outbox, stage, relay, half, send, recv, table_send, table_recv,
    y_send, y_recv, x_send, x_recv, own,
):
    me, row = lax.axis_index("gy"), lax.axis_index("gx")
    columns, rows = lax.axis_size("gy"), lax.axis_size("gx")
    edge = low.shape[0]
    part = edge // 2
    barrier = pltpu.get_barrier_semaphore()
    others = [lax.rem(me + k, columns) for k in range(1, columns)]
    senders = [lax.rem(me + columns - k, columns) for k in range(1, columns)]
    for target in others:
        signal("gy", target)

    @pl.when(row > 0)
    def _():
        signal("gx", row - 1)

    @pl.when(row < rows - 1)
    def _():
        signal("gx", row + 1)

    def fill(s, carry):
        outbox[s // SIDE, lax.rem(s, SIDE)] = phase[source[s]]
        return carry

    lax.fori_loop(0, columns, fill, 0)

    @pl.when(me == columns - 1)
    def _():
        half[...] = jnp.zeros_like(half)

    boxes_out = Exchange(outbox, boxes, stage, relay, send, recv, own, 3)
    boxes_out.prepare()

    neighbours = (row > 0).astype(jnp.int32) + (row < rows - 1).astype(jnp.int32)
    pl.semaphore_wait(barrier, columns - 1 + neighbours)

    def along_y(k):
        rest = pl.ds(k * part, part)
        return remote(low.at[rest], half.at[rest], y_send.at[k], y_recv.at[k], "gy", me - 1)

    def along_x(k):
        src = low if k == 2 else half.at[pl.ds(k * part, part)]
        rest = pl.ds(0, edge) if k == 2 else pl.ds(edge + k * part, part)
        dst = density.at[rest, pl.ds(edge, edge)]
        return remote(src, dst, x_send.at[k], x_recv.at[k], "gx", row - 1)

    def keep(k):
        src = low if k == 2 else half.at[pl.ds(k * part, part)]
        rest = pl.ds(0, edge) if k == 2 else pl.ds(edge + k * part, part)
        return pltpu.make_async_copy(src, density.at[rest, pl.ds(0, edge)], own.at[2 + k])

    def start_y(k):
        @pl.when(me > 0)
        def _():
            along_y(k).start()

    def start_x(k):
        keep(k).start()

        @pl.when(row > 0)
        def _():
            along_x(k).start()

    def take_y(k):
        @pl.when(me < columns - 1)
        def _():
            along_y(k).wait_recv()

    for h in range(2):
        boxes_out.start(0, h)
    start_x(2)
    notes = [
        remote(table.at[target], places.at[me], table_send.at[k], table_recv.at[k], "gy", target)
        for k, target in enumerate(others)
    ]
    for note in notes:
        note.start()
    note = pltpu.make_async_copy(table.at[me], places.at[me], own.at[5])
    note.start()
    for h in range(2):
        boxes_out.forward(0, h)
    start_y(0)
    for h in range(2):
        boxes_out.arrive(0, h)
        boxes_out.start(1, h)
    take_y(0)
    start_x(0)
    for h in range(2):
        boxes_out.forward(1, h)
    start_y(1)
    for h in range(2):
        boxes_out.arrive(1, h)
    take_y(1)
    start_x(1)
    for k, sender in enumerate(senders):
        remote(
            table.at[me], places.at[sender], table_send.at[k], table_recv.at[k], "gy", sender
        ).wait_recv()
    for copy in notes:
        copy.wait_send()
    note.wait()
    for k in range(3):
        keep(k).wait()

        @pl.when(row > 0)
        def _():
            along_x(k).wait_send()

        @pl.when(row < rows - 1)
        def _():
            along_x(k).wait_recv()

    for k in range(2):

        @pl.when(me > 0)
        def _():
            along_y(k).wait_send()

    boxes_out.finish()


def rim_kernel(own, crowd, from_x, full, from_y, x_send, x_recv, y_send, y_recv):
    me, row = lax.axis_index("gy"), lax.axis_index("gx")
    columns, rows = lax.axis_size("gy"), lax.axis_size("gx")
    edge = own.shape[1] // 2
    part = edge // 2
    sides = (
        (row < rows - 1, row + 1, slice(edge, 2 * edge), 0),
        (row > 0, row - 1, slice(0, edge), 1),
    )
    count = 0
    for axis, at, size in (("gx", row, rows), ("gy", me, columns)):
        for there, target in ((at > 0, at - 1), (at < size - 1, at + 1)):
            count += there.astype(jnp.int32)

            @pl.when(there)
            def _():
                signal(axis, target)

    pl.semaphore_wait(pltpu.get_barrier_semaphore(), count)
    chunks = [slice(p, p + part) for p in (0, edge, part, edge + part)]

    def along_x(c, side):
        _, target, half, k = sides[side]
        return remote(
            own.at[chunks[c], half],
            from_x.at[k, chunks[c]],
            x_send.at[k, c],
            x_recv.at[k, c],
            "gx",
            target,
        )

    def along_y(c):
        start = chunks[c].start
        up = start >= edge
        target = me + 1 if up else me - 1
        rest = slice(start % edge, start % edge + part)
        copy = remote(
            full.at[chunks[c]], from_y.at[int(up), rest], y_send.at[c], y_recv.at[c], "gy", target
        )
        sends = me < columns - 1 if up else me > 0
        takes = me > 0 if up else me < columns - 1
        return copy, sends, takes

    for c in range(len(chunks)):
        for side in range(2):

            @pl.when(sides[side][0])
            def _():
                along_x(c, side).start()

    for c, rest in enumerate(chunks):
        for side in range(2):
            takes, half = sides[1 - side][0], slice(edge, 2 * edge) if side else slice(0, edge)

            @pl.when(takes)
            def _():
                along_x(c, side).wait_recv()
                full[rest, half] = own[rest, half] + from_x[side, rest]

            @pl.when(jnp.logical_not(takes))
            def _():
                full[rest, half] = own[rest, half]

        copy, sends, _ = along_y(c)

        @pl.when(sends)
        def _():
            copy.start()

    for c in range(len(chunks)):
        copy, sends, takes = along_y(c)
        up = chunks[c].start >= edge
        start = chunks[c].start % edge
        rest = slice(start, start + part)
        rows_in = slice(start, start + part) if up else slice(edge + start, edge + start + part)

        @pl.when(takes)
        def _():
            copy.wait_recv()
            crowd[rows_in] = full[rows_in].astype(jnp.float32) + from_y[int(up), rest].astype(jnp.float32)

        @pl.when(jnp.logical_not(takes))
        def _():
            crowd[rows_in] = full[rows_in].astype(jnp.float32)

        @pl.when(sends)
        def _():
            copy.wait_send()

        for side in range(2):

            @pl.when(sides[side][0])
            def _():
                along_x(c, side).wait_send()


def return_kernel(
    settled, wide, returned, deposit, stage, relay, from_x, outgoing, from_y,
    send, recv, x_send, x_recv, y_send, y_recv, own,
):
    me, row = lax.axis_index("gy"), lax.axis_index("gx")
    columns, rows = lax.axis_size("gy"), lax.axis_size("gx")
    edge = wide.shape[1] // 2
    count = greet()
    boxes_back = Exchange(settled, returned, stage, relay, send, recv, own, 1)
    boxes_back.prepare()
    pl.semaphore_wait(pltpu.get_barrier_semaphore(), count)
    halves = (slice(edge, 2 * edge), slice(0, edge))

    def along_x(k):
        return remote(
            wide.at[halves[k], pl.ds(edge, edge)], from_x.at[k], x_send.at[k], x_recv.at[k], "gx", row + 1
        )

    for h in range(2):
        boxes_back.start(0, h)

    @pl.when(row < rows - 1)
    def _():
        for k in range(2):
            along_x(k).start()

    for h in range(2):
        boxes_back.forward(0, h)

    @pl.when(row > 0)
    def _():
        along_x(0).wait_recv()
        outgoing[...] = wide[edge:, :edge] + from_x[0]

    @pl.when(row == 0)
    def _():
        outgoing[...] = wide[edge:, :edge]

    part = edge // 2

    def along_y(k):
        rest = pl.ds(k * part, part)
        return remote(
            outgoing.at[rest], from_y.at[rest], y_send.at[k], y_recv.at[k], "gy", me + 1
        )

    @pl.when(me < columns - 1)
    def _():
        along_y(0).start()

    for h in range(2):
        boxes_back.arrive(0, h)
        boxes_back.start(1, h)

    @pl.when(row > 0)
    def _():
        along_x(1).wait_recv()
        deposit[...] = wide[:edge, :edge].astype(jnp.float32) + from_x[1].astype(jnp.float32)

    @pl.when(row == 0)
    def _():
        deposit[...] = wide[:edge, :edge].astype(jnp.float32)

    for h in range(2):
        boxes_back.forward(1, h)

    @pl.when(me < columns - 1)
    def _():
        along_y(1).start()

    for h in range(2):
        boxes_back.arrive(1, h)

    @pl.when(me > 0)
    def _():
        for k in range(2):
            along_y(k).wait_recv()
        deposit[...] = deposit[...] + from_y[...].astype(jnp.float32)

    boxes_back.finish()

    @pl.when(me < columns - 1)
    def _():
        for k in range(2):
            along_y(k).wait_send()

    @pl.when(row < rows - 1)
    def _():
        for k in range(2):
            along_x(k).wait_send()


def fetch_places(table, places, sem):
    copy = pltpu.make_async_copy(table.at[:, 0], places, sem)
    copy.start()
    copy.wait()


def spread_base(base):
    row = lax.broadcasted_iota(jnp.int32, base.shape, 0)
    lane = lax.broadcasted_iota(jnp.int32, base.shape, 1)
    base[...] = jnp.where(row // LANES == lane // B, lax.rem(row, LANES) - lax.rem(lane, B), -1)


def stacked(boxes, s):
    return jnp.concatenate(
        [boxes[s, :, j * LANES : (j + 1) * LANES] for j in range(B // GROUP)], 0
    )


def add_box(wide, v, spread, lx, ly):
    placed = lax.dot_general(
        v, spread, (((1,), (1,)), ((), ())), preferred_element_type=jnp.float32
    )
    for j in range(B // GROUP):
        for i in range(GROUP):
            at = (ly + (GROUP * j + i), pl.ds(lx, B), slice(None))
            wide[at] = wide[at] + placed[j * B : (j + 1) * B, i * LANES : (i + 1) * LANES]


def take_box(field, spread, lx, ly):
    rows = []
    for j in range(B // GROUP):
        parts = [field[ly + (GROUP * j + i), pl.ds(lx, B), :] for i in range(GROUP)]
        rows.append(jnp.concatenate([p.astype(jnp.bfloat16) for p in parts], 1))
    return jnp.dot(jnp.concatenate(rows, 0), spread, preferred_element_type=jnp.float32)


def crowd_kernel(table, boxes, out, wide, base, places, sem):
    fetch_places(table, places, sem)
    wide[...] = jnp.zeros_like(wide)
    spread_base(base)

    def one(s, carry):
        @pl.when(places[s, 3] > 0)
        def _():
            lx, ly, lz = places[s, 0], places[s, 1], places[s, 2]
            spread = jnp.where(base[...] == lz, 1.0, 0.0).astype(jnp.bfloat16)
            v = stacked(boxes, s).astype(jnp.float32)
            add_box(wide, (v * v).astype(jnp.bfloat16), spread, lx, ly)

        return carry

    lax.fori_loop(0, boxes.shape[0], one, 0)
    out[...] = wide[...].astype(out.dtype)


def update_kernel(
    table, boxes, crowd, low, settled, out, density, wide, base, taps, places, sem
):
    fetch_places(table, places, sem)
    density[...] = low[...].astype(jnp.float32)
    wide[...] = jnp.zeros_like(wide)
    spread_base(base)
    from_b = lax.broadcasted_iota(jnp.int32, taps.shape, 0) - LANES
    to_b = lax.broadcasted_iota(jnp.int32, taps.shape, 1)
    gap = from_b - to_b
    beside = (gap == B) | (gap == -B)
    same = (from_b >= 0) & (from_b < LANES) & (lax.rem(from_b + LANES, LANES) // B == to_b // B)
    along = same & ((gap == 1) | (gap == -1))
    taps[...] = jnp.where(gap == 0, -6.0, jnp.where(beside | along, 1.0, 0.0)).astype(taps.dtype)
    step = lax.rem(lax.broadcasted_iota(jnp.int32, (B * B // GROUP, LANES), 0), B)
    edge = jnp.zeros((B, LANES), jnp.bfloat16)
    total = B * B // GROUP

    def one(s, carry):
        @pl.when(places[s, 3] > 0)
        def _():
            lx, ly, lz = places[s, 0], places[s, 1], places[s, 2]
            spread = jnp.where(base[...] == lz, 1.0, 0.0).astype(jnp.bfloat16)
            cr = take_box(crowd, spread, lx, ly)
            dn = take_box(density, spread, lx, ly)
            v = stacked(boxes, s)
            near = jnp.concatenate(
                [
                    jnp.concatenate([edge, v[: total - B]], 0),
                    v,
                    jnp.concatenate([v[B:], edge], 0),
                ],
                1,
            )
            lap = jnp.dot(near, taps[...], preferred_element_type=jnp.float32)
            p = v.astype(jnp.float32)
            across = jnp.where(step < B - 1, pltpu.roll(p, total - 1, 0), 0.0) + jnp.where(
                step > 0, pltpu.roll(p, 1, 0), 0.0
            )
            others = cr - p * p
            reaction = 4.0 * p * (1.0 - p) * (p - 0.5 + (dn - 0.5))
            fresh = p + 0.1 * (lap + across + reaction - 2.0 * p * others)
            fresh = fresh.astype(jnp.bfloat16)
            for j in range(B // GROUP):
                settled[s, :, j * LANES : (j + 1) * LANES] = fresh[j * B : (j + 1) * B]
            add_box(wide, fresh, spread, lx, ly)

        @pl.when(places[s, 3] <= 0)
        def _():
            settled[s] = jnp.zeros(settled.shape[1:], settled.dtype)

        return carry

    lax.fori_loop(0, boxes.shape[0], one, 0)
    out[...] = wide[...].astype(out.dtype)


VMEM = pl.BlockSpec(memory_space=pltpu.VMEM)
ANY = pl.BlockSpec(memory_space=pl.ANY)
SMEM = pl.BlockSpec(memory_space=pltpu.SMEM)
LIMIT = 24 * 2**20


def like(shape, dtype):
    return jax.ShapeDtypeStruct(shape, dtype)


def dma(*shape):
    return pltpu.SemaphoreType.DMA(shape)


def linked(number):
    return pltpu.CompilerParams(
        collective_id=number, has_side_effects=True, vmem_limit_bytes=LIMIT
    )


def per_device(phase_box, matrix_density, box_corner):
    slab_rows, slab_cols, grid_depth = matrix_density.shape
    peers = lax.axis_size("gy")
    cells = phase_box.shape[0]
    home = box_corner[1] // slab_cols
    local = jnp.stack(
        [
            box_corner[0] - lax.axis_index("gx") * slab_rows,
            box_corner[1] - home * slab_cols,
            box_corner[2],
            jnp.ones_like(home),
        ],
        1,
    )
    match = (home[None, :] == jnp.arange(peers, dtype=jnp.int32)[:, None]).astype(jnp.int32)
    source = jnp.sum(match * jnp.arange(cells, dtype=jnp.int32)[None, :], 1)
    table = jnp.sum(match[:, :, None] * local[None], 1)
    table = jnp.pad(jnp.broadcast_to(table[:, None], (peers, 8, 4)), ((0, 0), (0, 0), (0, LANES - 4)))
    low = jnp.swapaxes(matrix_density, 0, 1).astype(jnp.bfloat16)

    bf16, f32 = jnp.bfloat16, jnp.float32
    slots = (peers,) + phase_box.shape[1:]
    torus = (SIDE, SIDE) + phase_box.shape[1:]
    rows = (phase_box.shape[1] // 2,) + phase_box.shape[2:]
    moving = [pltpu.VMEM((2, SIDE, SIDE) + rows, bf16), pltpu.VMEM((2, 2, 2, SIDE - 1) + rows, bf16)]
    wide = (2 * slab_cols, 2 * slab_rows, grid_depth)
    half = (2 * slab_cols, slab_rows, grid_depth)
    quarter = (slab_cols, slab_rows, grid_depth)
    boxes, places, density = pl.pallas_call(
        gather_kernel,
        out_shape=(like(torus, bf16), like(table.shape, jnp.int32), like(wide, bf16)),
        in_specs=[SMEM, VMEM, VMEM, VMEM],
        out_specs=(ANY, ANY, ANY),
        scratch_shapes=[pltpu.VMEM(torus, bf16)]
        + moving
        + [
            pltpu.VMEM(quarter, bf16),
            dma(2, 2, 6), dma(2, 2, 6), dma(peers - 1), dma(peers - 1),
            dma(2), dma(2), dma(3), dma(3), dma(6),
        ],
        compiler_params=linked(0),
        name="gather",
    )(source, phase_box, table, low)
    boxes = boxes.reshape(slots)

    spread = pltpu.VMEM((GROUP * LANES, LANES), jnp.int32)
    taps = pltpu.VMEM((3 * LANES, LANES), bf16)
    spots = [pltpu.SMEM((peers, LANES), jnp.int32), dma()]
    quiet = pltpu.CompilerParams(vmem_limit_bytes=LIMIT)
    crowd = pl.pallas_call(
        crowd_kernel,
        out_shape=like(wide, bf16),
        in_specs=[ANY, VMEM],
        out_specs=VMEM,
        scratch_shapes=[pltpu.VMEM(wide, f32), spread] + spots,
        compiler_params=quiet,
        name="crowd",
    )(places, boxes)

    crowd = pl.pallas_call(
        rim_kernel,
        out_shape=like(wide, f32),
        in_specs=[VMEM],
        out_specs=VMEM,
        scratch_shapes=[
            pltpu.VMEM((2,) + half, bf16),
            pltpu.VMEM(wide, bf16),
            pltpu.VMEM((2, slab_cols) + wide[1:], bf16),
            dma(2, 4), dma(2, 4), dma(4), dma(4),
        ],
        compiler_params=linked(1),
        name="rim",
    )(crowd)

    settled, deposit = pl.pallas_call(
        update_kernel,
        out_shape=(like(slots, bf16), like(wide, bf16)),
        in_specs=[ANY, VMEM, VMEM, VMEM],
        out_specs=(VMEM, VMEM),
        scratch_shapes=[pltpu.VMEM(wide, f32), pltpu.VMEM(wide, f32), spread, taps] + spots,
        compiler_params=quiet,
        name="update",
    )(places, boxes, crowd, density)

    returned, deposit = pl.pallas_call(
        return_kernel,
        out_shape=(like(torus, bf16), like(quarter, f32)),
        in_specs=[VMEM, VMEM],
        out_specs=(ANY, VMEM),
        scratch_shapes=moving
        + [
            pltpu.VMEM((2,) + quarter, bf16),
            pltpu.VMEM(quarter, bf16),
            pltpu.VMEM(quarter, bf16),
            dma(2, 2, 6), dma(2, 2, 6), dma(2), dma(2), dma(2), dma(2), dma(2),
        ],
        compiler_params=linked(2),
        name="return",
    )(settled.reshape(torus), deposit)
    returned = returned.reshape(slots)

    phase_next = returned[home]
    matrix_next = matrix_density - 0.5 * matrix_density * jnp.swapaxes(deposit, 0, 1)
    return phase_next, matrix_next


def solution(mesh):
    return jax.shard_map(
        per_device,
        mesh=mesh,
        in_specs=(P(("gx", "gy"), None, None), P("gx", "gy", None), P(None, ("gx", "gy"))),
        out_specs=(P(("gx", "gy"), None, None), P("gx", "gy", None)),
        check_vma=False,
    )
```

```python
import jax
import jax.numpy as jnp
from jax import lax
from jax.experimental import pallas as pl
from jax.experimental.pallas import tpu as pltpu
from jax.sharding import PartitionSpec as P

B = 32
LANES = 128
GROUP = LANES // B
SIDE = 4

def signal(axis, target):
    pl.semaphore_signal(
        pltpu.get_barrier_semaphore(),
        inc=1,
        device_id={axis: target},
        device_id_type=pl.DeviceIdType.MESH,
    )


def remote(src, dst, send, recv, axis, target):
    return pltpu.make_async_remote_copy(
        src_ref=src,
        dst_ref=dst,
        send_sem=send,
        recv_sem=recv,
        device_id={axis: target},
        device_id_type=pl.DeviceIdType.MESH,
    )


def greet():
    me, row = lax.axis_index("gy"), lax.axis_index("gx")
    columns, rows = lax.axis_size("gy"), lax.axis_size("gx")
    high, low = me // SIDE, lax.rem(me, SIDE)
    count = 0
    for step in (1, SIDE - 1):
        signal("gy", lax.rem(high + step, SIDE) * SIDE + low)
        signal("gy", high * SIDE + lax.rem(low + step, SIDE))
        count += 2
    for axis, at, size, step in (("gx", row, rows, 1), ("gx", row, rows, -1)):
        there = (at < size - 1) if step > 0 else (at > 0)
        count += there.astype(jnp.int32)

        @pl.when(there)
        def _():
            signal(axis, at + step)

    for step in (1, -1):
        far = (low == (SIDE - 1 if step > 0 else 0)) & (
            (me < columns - 1) if step > 0 else (me > 0)
        )
        count += far.astype(jnp.int32)

        @pl.when(far)
        def _():
            signal("gy", me + step)

    return count


class Exchange:
    def __init__(self, src, dst, stage, relay, send, recv, own, share_y):
        self.src, self.dst, self.stage, self.relay = src, dst, stage, relay
        self.send, self.recv, self.own = send, recv, own
        me = lax.axis_index("gy")
        self.at = (me // SIDE, lax.rem(me, SIDE))
        self.share = (SIDE // 2, share_y)
        self.rows = src.shape[2] // 2

    def turn(self, axis, step):
        return lax.rem(self.at[axis] + SIDE + step, SIDE)

    def device(self, axis, step):
        other, moved = self.at[1 - axis], self.turn(axis, step)
        return moved * SIDE + other if axis == 0 else other * SIDE + moved

    def whole(self, ref, half, first, second):
        rest = pl.ds(half * self.rows, self.rows)
        return ref.at[first, second, rest]

    def block(self, half, stage, goal, part):
        if stage == 1:
            return self.stage.at[half, part, goal]
        return self.whole(self.src, half, *((goal, part) if half == 0 else (part, goal)))

    def place(self, half, stage, origin, part):
        if stage == 0:
            return self.stage.at[half, origin, part]
        return self.whole(self.dst, half, *((part, origin) if half == 0 else (origin, part)))

    def copies(self, half, stage):
        axis = (half + stage) % 2
        share = self.share[axis]
        parts = (pl.ds(0, share), pl.ds(share, SIDE - share))
        sizes = (share, SIDE - share)
        every = pl.ds(0, SIDE)
        out = []
        for kind in ("relay", "direct", "forward"):
            for side in range(2):
                step = 1 if side == 0 else -1
                if kind == "direct":
                    src = self.block(half, stage, self.turn(axis, step), every)
                    dst = self.place(half, stage, self.at[axis], every)
                else:
                    hold = self.relay.at[half, stage, side, pl.ds(0, sizes[side])]
                    if kind == "relay":
                        src, dst = self.block(half, stage, self.turn(axis, 2), parts[side]), hold
                    else:
                        src = hold
                        dst = self.place(half, stage, self.turn(axis, -step), parts[side])
                at = (half, stage, len(out))
                out.append(
                    remote(src, dst, self.send.at[at], self.recv.at[at], "gy", self.device(axis, step))
                )
        return out

    def prepare(self):
        x, y = self.at
        self.stage[0, x] = self.src[x, :, : self.rows]
        self.stage[1, y] = self.src[:, y, self.rows :]

    def start(self, stage, half):
        copies = self.copies(half, stage)
        for copy in copies[:4]:
            copy.start()
        if stage == 1:
            self.kept(half).start()

    def forward(self, stage, half):
        copies = self.copies(half, stage)
        for side in range(2):
            copies[side].wait_recv()
            copies[4 + side].start()

    def arrive(self, stage, half):
        for copy in self.copies(half, stage)[2:]:
            copy.wait_recv()

    def kept(self, half):
        axis = (half + 1) % 2
        every = pl.ds(0, SIDE)
        return pltpu.make_async_copy(
            self.block(half, 1, self.at[axis], every),
            self.place(half, 1, self.at[axis], every),
            self.own.at[half],
        )

    def finish(self):
        for half in range(2):
            for stage in range(2):
                for copy in self.copies(half, stage):
                    copy.wait_send()
            self.kept(half).wait()


def gather_kernel(
    corner_in, phase_in, density_in, boxes, places, density,
    corner, phase, matrix, table, low, outbox, stage, relay, half, send, recv, table_send, table_recv,
    y_send, y_recv, x_send, x_recv, own, fetch,
):
    me, row = lax.axis_index("gy"), lax.axis_index("gx")
    columns, rows = lax.axis_size("gy"), lax.axis_size("gx")
    edge = low.shape[0]
    loads = [
        pltpu.make_async_copy(phase_in, phase, fetch.at[0]),
        pltpu.make_async_copy(density_in, matrix, fetch.at[1]),
        pltpu.make_async_copy(corner_in, corner, fetch.at[2]),
    ]
    for load in loads:
        load.start()
    part = edge // 2
    barrier = pltpu.get_barrier_semaphore()
    others = [lax.rem(me + k, columns) for k in range(1, columns)]
    senders = [lax.rem(me + columns - k, columns) for k in range(1, columns)]
    for target in others:
        signal("gy", target)

    @pl.when(row > 0)
    def _():
        signal("gx", row - 1)

    @pl.when(row < rows - 1)
    def _():
        signal("gx", row + 1)

    cells = range(phase.shape[0])
    loads[2].wait()
    home = [lax.div(corner[1, c], edge) for c in cells]
    lane = lax.broadcasted_iota(jnp.int32, table.shape[1:], 1)
    loads[0].wait()

    def fill(s, carry):
        source, found = jnp.int32(0), jnp.int32(0)
        for c in cells:
            source = jnp.where(home[c] == s, c, source)
            found = jnp.where(home[c] == s, 1, found)
        note = (
            corner[0, source] - row * edge,
            corner[1, source] - s * edge,
            corner[2, source],
            found,
        )
        line = jnp.zeros_like(lane)
        for k, value in enumerate(note):
            line = jnp.where(lane == k, value, line)
        table[s] = line
        outbox[s // SIDE, lax.rem(s, SIDE)] = phase[source]
        return carry

    lax.fori_loop(0, columns, fill, 0)
    loads[1].wait()
    low[...] = jnp.swapaxes(matrix[...], 0, 1).astype(low.dtype)

    @pl.when(me == columns - 1)
    def _():
        half[...] = jnp.zeros_like(half)

    boxes_out = Exchange(outbox, boxes, stage, relay, send, recv, own, 3)
    boxes_out.prepare()

    neighbours = (row > 0).astype(jnp.int32) + (row < rows - 1).astype(jnp.int32)
    pl.semaphore_wait(barrier, columns - 1 + neighbours)

    def along_y(k):
        rest = pl.ds(k * part, part)
        return remote(low.at[rest], half.at[rest], y_send.at[k], y_recv.at[k], "gy", me - 1)

    def along_x(k):
        src = low if k == 2 else half.at[pl.ds(k * part, part)]
        rest = pl.ds(0, edge) if k == 2 else pl.ds(edge + k * part, part)
        dst = density.at[rest, pl.ds(edge, edge)]
        return remote(src, dst, x_send.at[k], x_recv.at[k], "gx", row - 1)

    def keep(k):
        src = low if k == 2 else half.at[pl.ds(k * part, part)]
        rest = pl.ds(0, edge) if k == 2 else pl.ds(edge + k * part, part)
        return pltpu.make_async_copy(src, density.at[rest, pl.ds(0, edge)], own.at[2 + k])

    def start_y(k):
        @pl.when(me > 0)
        def _():
            along_y(k).start()

    def start_x(k):
        keep(k).start()

        @pl.when(row > 0)
        def _():
            along_x(k).start()

    def take_y(k):
        @pl.when(me < columns - 1)
        def _():
            along_y(k).wait_recv()

    for h in range(2):
        boxes_out.start(0, h)
    start_x(2)
    notes = [
        remote(table.at[target], places.at[me], table_send.at[k], table_recv.at[k], "gy", target)
        for k, target in enumerate(others)
    ]
    for note in notes:
        note.start()
    note = pltpu.make_async_copy(table.at[me], places.at[me], own.at[5])
    note.start()
    for h in range(2):
        boxes_out.forward(0, h)
    start_y(0)
    start_y(1)
    for h in range(2):
        boxes_out.arrive(0, h)
        boxes_out.start(1, h)
    take_y(0)
    start_x(0)
    for h in range(2):
        boxes_out.forward(1, h)
    take_y(1)
    start_x(1)
    for h in range(2):
        boxes_out.arrive(1, h)
    for k, sender in enumerate(senders):
        remote(
            table.at[me], places.at[sender], table_send.at[k], table_recv.at[k], "gy", sender
        ).wait_recv()
    for copy in notes:
        copy.wait_send()
    note.wait()
    for k in range(3):
        keep(k).wait()

        @pl.when(row > 0)
        def _():
            along_x(k).wait_send()

        @pl.when(row < rows - 1)
        def _():
            along_x(k).wait_recv()

    for k in range(2):

        @pl.when(me > 0)
        def _():
            along_y(k).wait_send()

    boxes_out.finish()


def rim_kernel(own, crowd, from_x, full, from_y, x_send, x_recv, y_send, y_recv):
    me, row = lax.axis_index("gy"), lax.axis_index("gx")
    columns, rows = lax.axis_size("gy"), lax.axis_size("gx")
    edge = own.shape[1] // 2
    part = edge // 2
    sides = (
        (row < rows - 1, row + 1, slice(edge, 2 * edge), 0),
        (row > 0, row - 1, slice(0, edge), 1),
    )
    count = 0
    for axis, at, size in (("gx", row, rows), ("gy", me, columns)):
        for there, target in ((at > 0, at - 1), (at < size - 1, at + 1)):
            count += there.astype(jnp.int32)

            @pl.when(there)
            def _():
                signal(axis, target)

    pl.semaphore_wait(pltpu.get_barrier_semaphore(), count)
    chunks = [slice(p, p + part) for p in (0, edge, part, edge + part)]

    def along_x(c, side):
        _, target, half, k = sides[side]
        return remote(
            own.at[chunks[c], half],
            from_x.at[k, chunks[c]],
            x_send.at[k, c],
            x_recv.at[k, c],
            "gx",
            target,
        )

    def along_y(c):
        start = chunks[c].start
        up = start >= edge
        target = me + 1 if up else me - 1
        rest = slice(start % edge, start % edge + part)
        copy = remote(
            full.at[chunks[c]], from_y.at[int(up), rest], y_send.at[c], y_recv.at[c], "gy", target
        )
        sends = me < columns - 1 if up else me > 0
        takes = me > 0 if up else me < columns - 1
        return copy, sends, takes

    for c in range(len(chunks)):
        for side in range(2):

            @pl.when(sides[side][0])
            def _():
                along_x(c, side).start()

    for c, rest in enumerate(chunks):
        for side in range(2):
            takes, half = sides[1 - side][0], slice(edge, 2 * edge) if side else slice(0, edge)

            @pl.when(takes)
            def _():
                along_x(c, side).wait_recv()
                full[rest, half] = own[rest, half] + from_x[side, rest]

            @pl.when(jnp.logical_not(takes))
            def _():
                full[rest, half] = own[rest, half]

        copy, sends, _ = along_y(c)

        @pl.when(sends)
        def _():
            copy.start()

    for c in range(len(chunks)):
        copy, sends, takes = along_y(c)
        up = chunks[c].start >= edge
        start = chunks[c].start % edge
        rest = slice(start, start + part)
        rows_in = slice(start, start + part) if up else slice(edge + start, edge + start + part)

        @pl.when(takes)
        def _():
            copy.wait_recv()
            crowd[rows_in] = full[rows_in].astype(jnp.float32) + from_y[int(up), rest].astype(jnp.float32)

        @pl.when(jnp.logical_not(takes))
        def _():
            crowd[rows_in] = full[rows_in].astype(jnp.float32)

        @pl.when(sends)
        def _():
            copy.wait_send()

        for side in range(2):

            @pl.when(sides[side][0])
            def _():
                along_x(c, side).wait_send()


def return_kernel(
    settled, wide, returned, deposit, stage, relay, from_x, outgoing, from_y,
    send, recv, x_send, x_recv, y_send, y_recv, own,
):
    me, row = lax.axis_index("gy"), lax.axis_index("gx")
    columns, rows = lax.axis_size("gy"), lax.axis_size("gx")
    edge = wide.shape[1] // 2
    count = greet()
    boxes_back = Exchange(settled, returned, stage, relay, send, recv, own, 1)
    boxes_back.prepare()
    pl.semaphore_wait(pltpu.get_barrier_semaphore(), count)
    halves = (slice(edge, 2 * edge), slice(0, edge))

    def along_x(k):
        return remote(
            wide.at[halves[k], pl.ds(edge, edge)], from_x.at[k], x_send.at[k], x_recv.at[k], "gx", row + 1
        )

    for h in range(2):
        boxes_back.start(0, h)

    @pl.when(row < rows - 1)
    def _():
        for k in range(2):
            along_x(k).start()

    for h in range(2):
        boxes_back.forward(0, h)

    @pl.when(row > 0)
    def _():
        along_x(0).wait_recv()
        outgoing[...] = wide[edge:, :edge] + from_x[0]

    @pl.when(row == 0)
    def _():
        outgoing[...] = wide[edge:, :edge]

    part = edge // 2

    def along_y(k):
        rest = pl.ds(k * part, part)
        return remote(
            outgoing.at[rest], from_y.at[rest], y_send.at[k], y_recv.at[k], "gy", me + 1
        )

    @pl.when(me < columns - 1)
    def _():
        for k in range(2):
            along_y(k).start()

    for h in range(2):
        boxes_back.arrive(0, h)
        boxes_back.start(1, h)

    @pl.when(row > 0)
    def _():
        along_x(1).wait_recv()
        deposit[...] = wide[:edge, :edge].astype(jnp.float32) + from_x[1].astype(jnp.float32)

    @pl.when(row == 0)
    def _():
        deposit[...] = wide[:edge, :edge].astype(jnp.float32)

    for h in range(2):
        boxes_back.forward(1, h)

    @pl.when(me > 0)
    def _():
        for k in range(2):
            along_y(k).wait_recv()
        deposit[...] = deposit[...] + from_y[...].astype(jnp.float32)

    for h in range(2):
        boxes_back.arrive(1, h)

    boxes_back.finish()

    @pl.when(me < columns - 1)
    def _():
        for k in range(2):
            along_y(k).wait_send()

    @pl.when(row < rows - 1)
    def _():
        for k in range(2):
            along_x(k).wait_send()


def fetch_places(table, places, sem):
    copy = pltpu.make_async_copy(table.at[:, 0], places, sem)
    copy.start()
    copy.wait()


def spread_base(base):
    row = lax.broadcasted_iota(jnp.int32, base.shape, 0)
    lane = lax.broadcasted_iota(jnp.int32, base.shape, 1)
    base[...] = jnp.where(row // LANES == lane // B, lax.rem(row, LANES) - lax.rem(lane, B), -1)


def stacked(boxes, s):
    return jnp.concatenate(
        [boxes[s, :, j * LANES : (j + 1) * LANES] for j in range(B // GROUP)], 0
    )


def add_box(wide, v, spread, lx, ly):
    placed = lax.dot_general(
        v, spread, (((1,), (1,)), ((), ())), preferred_element_type=jnp.float32
    )
    for j in range(B // GROUP):
        for i in range(GROUP):
            at = (ly + (GROUP * j + i), pl.ds(lx, B), slice(None))
            wide[at] = wide[at] + placed[j * B : (j + 1) * B, i * LANES : (i + 1) * LANES]


def take_box(field, spread, lx, ly):
    rows = []
    for j in range(B // GROUP):
        parts = [field[ly + (GROUP * j + i), pl.ds(lx, B), :] for i in range(GROUP)]
        rows.append(jnp.concatenate([p.astype(jnp.bfloat16) for p in parts], 1))
    return jnp.dot(jnp.concatenate(rows, 0), spread, preferred_element_type=jnp.float32)


def crowd_kernel(table, boxes, out, wide, base, places, sem):
    fetch_places(table, places, sem)
    wide[...] = jnp.zeros_like(wide)
    spread_base(base)

    def one(s, carry):
        @pl.when(places[s, 3] > 0)
        def _():
            lx, ly, lz = places[s, 0], places[s, 1], places[s, 2]
            spread = jnp.where(base[...] == lz, 1.0, 0.0).astype(jnp.bfloat16)
            v = stacked(boxes, s).astype(jnp.float32)
            add_box(wide, (v * v).astype(jnp.bfloat16), spread, lx, ly)

        return carry

    lax.fori_loop(0, boxes.shape[0], one, 0)
    out[...] = wide[...].astype(out.dtype)


def update_kernel(
    table, boxes, crowd, low, settled, out, density, wide, base, taps, places, sem
):
    fetch_places(table, places, sem)
    density[...] = low[...].astype(jnp.float32)
    wide[...] = jnp.zeros_like(wide)
    spread_base(base)
    from_b = lax.broadcasted_iota(jnp.int32, taps.shape, 0) - LANES
    to_b = lax.broadcasted_iota(jnp.int32, taps.shape, 1)
    gap = from_b - to_b
    beside = (gap == B) | (gap == -B)
    same = (from_b >= 0) & (from_b < LANES) & (lax.rem(from_b + LANES, LANES) // B == to_b // B)
    along = same & ((gap == 1) | (gap == -1))
    taps[...] = jnp.where(gap == 0, -6.0, jnp.where(beside | along, 1.0, 0.0)).astype(taps.dtype)
    step = lax.rem(lax.broadcasted_iota(jnp.int32, (B * B // GROUP, LANES), 0), B)
    edge = jnp.zeros((B, LANES), jnp.bfloat16)
    total = B * B // GROUP

    def one(s, carry):
        @pl.when(places[s, 3] > 0)
        def _():
            lx, ly, lz = places[s, 0], places[s, 1], places[s, 2]
            spread = jnp.where(base[...] == lz, 1.0, 0.0).astype(jnp.bfloat16)
            cr = take_box(crowd, spread, lx, ly)
            dn = take_box(density, spread, lx, ly)
            v = stacked(boxes, s)
            near = jnp.concatenate(
                [
                    jnp.concatenate([edge, v[: total - B]], 0),
                    v,
                    jnp.concatenate([v[B:], edge], 0),
                ],
                1,
            )
            lap = jnp.dot(near, taps[...], preferred_element_type=jnp.float32)
            p = v.astype(jnp.float32)
            across = jnp.where(step < B - 1, pltpu.roll(p, total - 1, 0), 0.0) + jnp.where(
                step > 0, pltpu.roll(p, 1, 0), 0.0
            )
            others = cr - p * p
            reaction = 4.0 * p * (1.0 - p) * (p - 0.5 + (dn - 0.5))
            fresh = p + 0.1 * (lap + across + reaction - 2.0 * p * others)
            fresh = fresh.astype(jnp.bfloat16)
            for j in range(B // GROUP):
                settled[s, :, j * LANES : (j + 1) * LANES] = fresh[j * B : (j + 1) * B]
            add_box(wide, fresh, spread, lx, ly)

        @pl.when(places[s, 3] <= 0)
        def _():
            settled[s] = jnp.zeros(settled.shape[1:], settled.dtype)

        return carry

    lax.fori_loop(0, boxes.shape[0], one, 0)
    out[...] = wide[...].astype(out.dtype)


def finish_kernel(
    corner_in, returned, deposit, matrix, phase_next, matrix_next, corner, sem, fetch
):
    edge = matrix.shape[1]
    load = pltpu.make_async_copy(corner_in, corner, fetch)
    load.start()
    load.wait()
    copies = [
        pltpu.make_async_copy(
            returned.at[lax.div(corner[1, c], edge)], phase_next.at[c], sem.at[c]
        )
        for c in range(phase_next.shape[0])
    ]
    for copy in copies:
        copy.start()
    now = matrix[...]
    matrix_next[...] = now - 0.5 * now * jnp.swapaxes(deposit[...], 0, 1)
    for copy in copies:
        copy.wait()


VMEM = pl.BlockSpec(memory_space=pltpu.VMEM)
ANY = pl.BlockSpec(memory_space=pl.ANY)
HBM = pl.BlockSpec(memory_space=pltpu.HBM)
LIMIT = 24 * 2**20


def like(shape, dtype):
    return jax.ShapeDtypeStruct(shape, dtype)


def dma(*shape):
    return pltpu.SemaphoreType.DMA(shape)


def linked(number):
    return pltpu.CompilerParams(
        collective_id=number, has_side_effects=True, vmem_limit_bytes=LIMIT
    )


def per_device(phase_box, matrix_density, box_corner):
    slab_rows, slab_cols, grid_depth = matrix_density.shape
    peers = lax.axis_size("gy")
    bf16, f32 = jnp.bfloat16, jnp.float32
    slots = (peers,) + phase_box.shape[1:]
    notes = (peers, 8, LANES)
    torus = (SIDE, SIDE) + phase_box.shape[1:]
    rows = (phase_box.shape[1] // 2,) + phase_box.shape[2:]
    moving = [pltpu.VMEM((2, SIDE, SIDE) + rows, bf16), pltpu.VMEM((2, 2, 2, SIDE - 1) + rows, bf16)]
    wide = (2 * slab_cols, 2 * slab_rows, grid_depth)
    half = (2 * slab_cols, slab_rows, grid_depth)
    quarter = (slab_cols, slab_rows, grid_depth)
    boxes, places, density = pl.pallas_call(
        gather_kernel,
        out_shape=(like(torus, bf16), like(notes, jnp.int32), like(wide, bf16)),
        in_specs=[HBM, HBM, HBM],
        out_specs=(ANY, ANY, ANY),
        scratch_shapes=[
            pltpu.SMEM(box_corner.shape, jnp.int32),
            pltpu.VMEM(phase_box.shape, bf16),
            pltpu.VMEM(matrix_density.shape, f32),
            pltpu.VMEM(notes, jnp.int32),
            pltpu.VMEM(quarter, bf16),
            pltpu.VMEM(torus, bf16),
        ]
        + moving
        + [
            pltpu.VMEM(quarter, bf16),
            dma(2, 2, 6), dma(2, 2, 6), dma(peers - 1), dma(peers - 1),
            dma(2), dma(2), dma(3), dma(3), dma(6), dma(3),
        ],
        compiler_params=linked(0),
        name="gather",
    )(box_corner, phase_box, matrix_density)
    boxes = boxes.reshape(slots)

    spread = pltpu.VMEM((GROUP * LANES, LANES), jnp.int32)
    taps = pltpu.VMEM((3 * LANES, LANES), bf16)
    spots = [pltpu.SMEM((peers, LANES), jnp.int32), dma()]
    quiet = pltpu.CompilerParams(vmem_limit_bytes=LIMIT)
    crowd = pl.pallas_call(
        crowd_kernel,
        out_shape=like(wide, bf16),
        in_specs=[ANY, VMEM],
        out_specs=VMEM,
        scratch_shapes=[pltpu.VMEM(wide, f32), spread] + spots,
        compiler_params=quiet,
        name="crowd",
    )(places, boxes)

    crowd = pl.pallas_call(
        rim_kernel,
        out_shape=like(wide, f32),
        in_specs=[VMEM],
        out_specs=VMEM,
        scratch_shapes=[
            pltpu.VMEM((2,) + half, bf16),
            pltpu.VMEM(wide, bf16),
            pltpu.VMEM((2, slab_cols) + wide[1:], bf16),
            dma(2, 4), dma(2, 4), dma(4), dma(4),
        ],
        compiler_params=linked(1),
        name="rim",
    )(crowd)

    settled, deposit = pl.pallas_call(
        update_kernel,
        out_shape=(like(slots, bf16), like(wide, bf16)),
        in_specs=[ANY, VMEM, VMEM, VMEM],
        out_specs=(VMEM, VMEM),
        scratch_shapes=[pltpu.VMEM(wide, f32), pltpu.VMEM(wide, f32), spread, taps] + spots,
        compiler_params=quiet,
        name="update",
    )(places, boxes, crowd, density)

    returned, deposit = pl.pallas_call(
        return_kernel,
        out_shape=(like(torus, bf16), like(quarter, f32)),
        in_specs=[VMEM, VMEM],
        out_specs=(ANY, VMEM),
        scratch_shapes=moving
        + [
            pltpu.VMEM((2,) + quarter, bf16),
            pltpu.VMEM(quarter, bf16),
            pltpu.VMEM(quarter, bf16),
            dma(2, 2, 6), dma(2, 2, 6), dma(2), dma(2), dma(2), dma(2), dma(2),
        ],
        compiler_params=linked(2),
        name="return",
    )(settled.reshape(torus), deposit)
    returned = returned.reshape(slots)

    return pl.pallas_call(
        finish_kernel,
        out_shape=(like(phase_box.shape, bf16), like(matrix_density.shape, f32)),
        in_specs=[HBM, VMEM, VMEM, VMEM],
        out_specs=(ANY, VMEM),
        scratch_shapes=[
            pltpu.SMEM(box_corner.shape, jnp.int32),
            dma(phase_box.shape[0]),
            dma(),
        ],
        compiler_params=quiet,
        name="finish",
    )(box_corner, returned, deposit, matrix_density)


def solution(mesh):
    return jax.shard_map(
        per_device,
        mesh=mesh,
        in_specs=(P(("gx", "gy"), None, None), P("gx", "gy", None), P(None, ("gx", "gy"))),
        out_specs=(P(("gx", "gy"), None, None), P("gx", "gy", None)),
        check_vma=False,
    )
```

```python
import jax
import jax.numpy as jnp
from jax import lax
from jax.experimental import pallas as pl
from jax.experimental.pallas import tpu as pltpu
from jax.sharding import PartitionSpec as P

B = 32
LANES = 128
GROUP = LANES // B
SIDE = 4

def signal(axis, target):
    pl.semaphore_signal(
        pltpu.get_barrier_semaphore(),
        inc=1,
        device_id={axis: target},
        device_id_type=pl.DeviceIdType.MESH,
    )


def remote(src, dst, send, recv, axis, target):
    return pltpu.make_async_remote_copy(
        src_ref=src,
        dst_ref=dst,
        send_sem=send,
        recv_sem=recv,
        device_id={axis: target},
        device_id_type=pl.DeviceIdType.MESH,
    )


def greet():
    me, row = lax.axis_index("gy"), lax.axis_index("gx")
    columns, rows = lax.axis_size("gy"), lax.axis_size("gx")
    high, low = me // SIDE, lax.rem(me, SIDE)
    count = 0
    for step in (1, SIDE - 1):
        signal("gy", lax.rem(high + step, SIDE) * SIDE + low)
        signal("gy", high * SIDE + lax.rem(low + step, SIDE))
        count += 2
    for axis, at, size, step in (("gx", row, rows, 1), ("gx", row, rows, -1)):
        there = (at < size - 1) if step > 0 else (at > 0)
        count += there.astype(jnp.int32)

        @pl.when(there)
        def _():
            signal(axis, at + step)

    for step in (1, -1):
        far = (low == (SIDE - 1 if step > 0 else 0)) & (
            (me < columns - 1) if step > 0 else (me > 0)
        )
        count += far.astype(jnp.int32)

        @pl.when(far)
        def _():
            signal("gy", me + step)

    return count


class Exchange:
    def __init__(self, src, dst, stage, relay, send, recv, own, share_y):
        self.src, self.dst, self.stage, self.relay = src, dst, stage, relay
        self.send, self.recv, self.own = send, recv, own
        me = lax.axis_index("gy")
        self.at = (me // SIDE, lax.rem(me, SIDE))
        self.share = (SIDE // 2, share_y)
        self.rows = src.shape[2] // 2

    def turn(self, axis, step):
        return lax.rem(self.at[axis] + SIDE + step, SIDE)

    def device(self, axis, step):
        other, moved = self.at[1 - axis], self.turn(axis, step)
        return moved * SIDE + other if axis == 0 else other * SIDE + moved

    def whole(self, ref, half, first, second):
        rest = pl.ds(half * self.rows, self.rows)
        return ref.at[first, second, rest]

    def block(self, half, stage, goal, part):
        if stage == 1:
            return self.stage.at[half, part, goal]
        return self.whole(self.src, half, *((goal, part) if half == 0 else (part, goal)))

    def place(self, half, stage, origin, part):
        if stage == 0:
            return self.stage.at[half, origin, part]
        return self.whole(self.dst, half, *((part, origin) if half == 0 else (origin, part)))

    def copies(self, half, stage):
        axis = (half + stage) % 2
        share = self.share[axis]
        parts = (pl.ds(0, share), pl.ds(share, SIDE - share))
        sizes = (share, SIDE - share)
        every = pl.ds(0, SIDE)
        out = []
        for kind in ("relay", "direct", "forward"):
            for side in range(2):
                step = 1 if side == 0 else -1
                if kind == "direct":
                    src = self.block(half, stage, self.turn(axis, step), every)
                    dst = self.place(half, stage, self.at[axis], every)
                else:
                    hold = self.relay.at[half, stage, side, pl.ds(0, sizes[side])]
                    if kind == "relay":
                        src, dst = self.block(half, stage, self.turn(axis, 2), parts[side]), hold
                    else:
                        src = hold
                        dst = self.place(half, stage, self.turn(axis, -step), parts[side])
                at = (half, stage, len(out))
                out.append(
                    remote(src, dst, self.send.at[at], self.recv.at[at], "gy", self.device(axis, step))
                )
        return out

    def prepare(self):
        x, y = self.at
        self.stage[0, x] = self.src[x, :, : self.rows]
        self.stage[1, y] = self.src[:, y, self.rows :]

    def start(self, stage, half):
        copies = self.copies(half, stage)
        for copy in copies[:4]:
            copy.start()
        if stage == 1:
            self.kept(half).start()

    def forward(self, stage, half):
        copies = self.copies(half, stage)
        for side in range(2):
            copies[side].wait_recv()
            copies[4 + side].start()

    def arrive(self, stage, half):
        for copy in self.copies(half, stage)[2:]:
            copy.wait_recv()

    def kept(self, half):
        axis = (half + 1) % 2
        every = pl.ds(0, SIDE)
        return pltpu.make_async_copy(
            self.block(half, 1, self.at[axis], every),
            self.place(half, 1, self.at[axis], every),
            self.own.at[half],
        )

    def finish(self):
        for half in range(2):
            for stage in range(2):
                for copy in self.copies(half, stage):
                    copy.wait_send()
            self.kept(half).wait()


def gather_kernel(
    corner_in, phase_in, density_in, boxes, places, density,
    corner, phase, matrix, table, low, outbox, stage, relay, half, send, recv, table_send, table_recv,
    y_send, y_recv, x_send, x_recv, own, fetch,
):
    me, row = lax.axis_index("gy"), lax.axis_index("gx")
    columns, rows = lax.axis_size("gy"), lax.axis_size("gx")
    edge = low.shape[0]
    loads = [
        pltpu.make_async_copy(phase_in, phase, fetch.at[0]),
        pltpu.make_async_copy(density_in, matrix, fetch.at[1]),
        pltpu.make_async_copy(corner_in, corner, fetch.at[2]),
    ]
    for load in loads:
        load.start()
    part = edge // 2
    barrier = pltpu.get_barrier_semaphore()
    others = [lax.rem(me + k, columns) for k in range(1, columns)]
    senders = [lax.rem(me + columns - k, columns) for k in range(1, columns)]
    for target in others:
        signal("gy", target)

    @pl.when(row > 0)
    def _():
        signal("gx", row - 1)

    @pl.when(row < rows - 1)
    def _():
        signal("gx", row + 1)

    cells = range(phase.shape[0])
    loads[2].wait()
    home = [lax.div(corner[1, c], edge) for c in cells]
    lane = lax.broadcasted_iota(jnp.int32, table.shape[1:], 1)
    loads[0].wait()

    def fill(s, carry):
        source, found = jnp.int32(0), jnp.int32(0)
        for c in cells:
            source = jnp.where(home[c] == s, c, source)
            found = jnp.where(home[c] == s, 1, found)
        note = (
            corner[0, source] - row * edge,
            corner[1, source] - s * edge,
            corner[2, source],
            found,
        )
        line = jnp.zeros_like(lane)
        for k, value in enumerate(note):
            line = jnp.where(lane == k, value, line)
        table[s] = line
        outbox[s // SIDE, lax.rem(s, SIDE)] = phase[source]
        return carry

    lax.fori_loop(0, columns, fill, 0)
    loads[1].wait()
    low[...] = jnp.swapaxes(matrix[...], 0, 1).astype(low.dtype)

    @pl.when(me == columns - 1)
    def _():
        half[...] = jnp.zeros_like(half)

    boxes_out = Exchange(outbox, boxes, stage, relay, send, recv, own, 3)
    boxes_out.prepare()

    neighbours = (row > 0).astype(jnp.int32) + (row < rows - 1).astype(jnp.int32)
    pl.semaphore_wait(barrier, columns - 1 + neighbours)

    def along_y(k):
        rest = pl.ds(k * part, part)
        return remote(low.at[rest], half.at[rest], y_send.at[k], y_recv.at[k], "gy", me - 1)

    def along_x(k):
        src = low if k == 2 else half.at[pl.ds(k * part, part)]
        rest = pl.ds(0, edge) if k == 2 else pl.ds(edge + k * part, part)
        dst = density.at[rest, pl.ds(edge, edge)]
        return remote(src, dst, x_send.at[k], x_recv.at[k], "gx", row - 1)

    def keep(k):
        src = low if k == 2 else half.at[pl.ds(k * part, part)]
        rest = pl.ds(0, edge) if k == 2 else pl.ds(edge + k * part, part)
        return pltpu.make_async_copy(src, density.at[rest, pl.ds(0, edge)], own.at[2 + k])

    def start_y(k):
        @pl.when(me > 0)
        def _():
            along_y(k).start()

    def start_x(k):
        keep(k).start()

        @pl.when(row > 0)
        def _():
            along_x(k).start()

    def take_y(k):
        @pl.when(me < columns - 1)
        def _():
            along_y(k).wait_recv()

    for h in range(2):
        boxes_out.start(0, h)
    start_x(2)
    notes = [
        remote(table.at[target], places.at[me], table_send.at[k], table_recv.at[k], "gy", target)
        for k, target in enumerate(others)
    ]
    for note in notes:
        note.start()
    note = pltpu.make_async_copy(table.at[me], places.at[me], own.at[5])
    note.start()
    for h in range(2):
        boxes_out.forward(0, h)
    start_y(0)
    start_y(1)
    for h in range(2):
        boxes_out.arrive(0, h)
        boxes_out.start(1, h)
    take_y(0)
    start_x(0)
    for h in range(2):
        boxes_out.forward(1, h)
    take_y(1)
    start_x(1)
    for h in range(2):
        boxes_out.arrive(1, h)
    for k, sender in enumerate(senders):
        remote(
            table.at[me], places.at[sender], table_send.at[k], table_recv.at[k], "gy", sender
        ).wait_recv()
    for copy in notes:
        copy.wait_send()
    note.wait()
    for k in range(3):
        keep(k).wait()

        @pl.when(row > 0)
        def _():
            along_x(k).wait_send()

        @pl.when(row < rows - 1)
        def _():
            along_x(k).wait_recv()

    for k in range(2):

        @pl.when(me > 0)
        def _():
            along_y(k).wait_send()

    boxes_out.finish()


def rim_kernel(own, crowd, from_x, full, from_y, x_send, x_recv, y_send, y_recv):
    me, row = lax.axis_index("gy"), lax.axis_index("gx")
    columns, rows = lax.axis_size("gy"), lax.axis_size("gx")
    edge = own.shape[1] // 2
    part = edge // 2
    sides = (
        (row < rows - 1, row + 1, slice(edge, 2 * edge), 0),
        (row > 0, row - 1, slice(0, edge), 1),
    )
    count = 0
    for axis, at, size in (("gx", row, rows), ("gy", me, columns)):
        for there, target in ((at > 0, at - 1), (at < size - 1, at + 1)):
            count += there.astype(jnp.int32)

            @pl.when(there)
            def _():
                signal(axis, target)

    pl.semaphore_wait(pltpu.get_barrier_semaphore(), count)
    chunks = [slice(p, p + part) for p in (0, edge, part, edge + part)]

    def along_x(c, side):
        _, target, half, k = sides[side]
        return remote(
            own.at[chunks[c], half],
            from_x.at[k, chunks[c]],
            x_send.at[k, c],
            x_recv.at[k, c],
            "gx",
            target,
        )

    def along_y(c):
        start = chunks[c].start
        up = start >= edge
        target = me + 1 if up else me - 1
        rest = slice(start % edge, start % edge + part)
        copy = remote(
            full.at[chunks[c]], from_y.at[int(up), rest], y_send.at[c], y_recv.at[c], "gy", target
        )
        sends = me < columns - 1 if up else me > 0
        takes = me > 0 if up else me < columns - 1
        return copy, sends, takes

    for c in range(len(chunks)):
        for side in range(2):

            @pl.when(sides[side][0])
            def _():
                along_x(c, side).start()

    for c, rest in enumerate(chunks):
        for side in range(2):
            takes, half = sides[1 - side][0], slice(edge, 2 * edge) if side else slice(0, edge)

            @pl.when(takes)
            def _():
                along_x(c, side).wait_recv()
                full[rest, half] = own[rest, half] + from_x[side, rest]

            @pl.when(jnp.logical_not(takes))
            def _():
                full[rest, half] = own[rest, half]

        copy, sends, _ = along_y(c)

        @pl.when(sends)
        def _():
            copy.start()

    for c in range(len(chunks)):
        copy, sends, takes = along_y(c)
        up = chunks[c].start >= edge
        start = chunks[c].start % edge
        rest = slice(start, start + part)
        rows_in = slice(start, start + part) if up else slice(edge + start, edge + start + part)

        @pl.when(takes)
        def _():
            copy.wait_recv()
            crowd[rows_in] = full[rows_in].astype(jnp.float32) + from_y[int(up), rest].astype(jnp.float32)

        @pl.when(jnp.logical_not(takes))
        def _():
            crowd[rows_in] = full[rows_in].astype(jnp.float32)

        @pl.when(sends)
        def _():
            copy.wait_send()

        for side in range(2):

            @pl.when(sides[side][0])
            def _():
                along_x(c, side).wait_send()


def return_kernel(
    settled, wide, returned, deposit, stage, relay, from_x, outgoing, from_y,
    send, recv, x_send, x_recv, y_send, y_recv, own,
):
    me, row = lax.axis_index("gy"), lax.axis_index("gx")
    columns, rows = lax.axis_size("gy"), lax.axis_size("gx")
    edge = wide.shape[1] // 2
    count = greet()
    boxes_back = Exchange(settled, returned, stage, relay, send, recv, own, 1)
    boxes_back.prepare()
    pl.semaphore_wait(pltpu.get_barrier_semaphore(), count)
    halves = (slice(edge, 2 * edge), slice(0, edge))

    def along_x(k):
        return remote(
            wide.at[halves[k], pl.ds(edge, edge)], from_x.at[k], x_send.at[k], x_recv.at[k], "gx", row + 1
        )

    for h in range(2):
        boxes_back.start(0, h)

    @pl.when(row < rows - 1)
    def _():
        for k in range(2):
            along_x(k).start()

    for h in range(2):
        boxes_back.forward(0, h)

    @pl.when(row > 0)
    def _():
        along_x(0).wait_recv()
        outgoing[...] = wide[edge:, :edge] + from_x[0]

    @pl.when(row == 0)
    def _():
        outgoing[...] = wide[edge:, :edge]

    part = edge // 2

    def along_y(k):
        rest = pl.ds(k * part, part)
        return remote(
            outgoing.at[rest], from_y.at[rest], y_send.at[k], y_recv.at[k], "gy", me + 1
        )

    @pl.when(me < columns - 1)
    def _():
        for k in range(2):
            along_y(k).start()

    for h in range(2):
        boxes_back.arrive(0, h)
        boxes_back.start(1, h)

    @pl.when(row > 0)
    def _():
        along_x(1).wait_recv()
        deposit[...] = wide[:edge, :edge].astype(jnp.float32) + from_x[1].astype(jnp.float32)

    @pl.when(row == 0)
    def _():
        deposit[...] = wide[:edge, :edge].astype(jnp.float32)

    for h in range(2):
        boxes_back.forward(1, h)

    @pl.when(me > 0)
    def _():
        for k in range(2):
            along_y(k).wait_recv()
        deposit[...] = deposit[...] + from_y[...].astype(jnp.float32)

    for h in range(2):
        boxes_back.arrive(1, h)

    boxes_back.finish()

    @pl.when(me < columns - 1)
    def _():
        for k in range(2):
            along_y(k).wait_send()

    @pl.when(row < rows - 1)
    def _():
        for k in range(2):
            along_x(k).wait_send()


def fetch_places(table, places, sem):
    copy = pltpu.make_async_copy(table.at[:, 0], places, sem)
    copy.start()
    copy.wait()


def spread_base(base):
    row = lax.broadcasted_iota(jnp.int32, base.shape, 0)
    lane = lax.broadcasted_iota(jnp.int32, base.shape, 1)
    base[...] = jnp.where(row // LANES == lane // B, lax.rem(row, LANES) - lax.rem(lane, B), -1)


def stacked(boxes, s):
    return jnp.concatenate(
        [boxes[s, :, j * LANES : (j + 1) * LANES] for j in range(B // GROUP)], 0
    )


def add_box(wide, v, spread, lx, ly):
    placed = lax.dot_general(
        v, spread, (((1,), (1,)), ((), ())), preferred_element_type=jnp.float32
    )
    for j in range(B // GROUP):
        for i in range(GROUP):
            at = (ly + (GROUP * j + i), pl.ds(lx, B), slice(None))
            wide[at] = wide[at] + placed[j * B : (j + 1) * B, i * LANES : (i + 1) * LANES]


def take_box(field, spread, lx, ly):
    rows = []
    for j in range(B // GROUP):
        parts = [field[ly + (GROUP * j + i), pl.ds(lx, B), :] for i in range(GROUP)]
        rows.append(jnp.concatenate([p.astype(jnp.bfloat16) for p in parts], 1))
    return jnp.dot(jnp.concatenate(rows, 0), spread, preferred_element_type=jnp.float32)


def crowd_kernel(table, boxes, out, wide, base, places, sem):
    fetch_places(table, places, sem)
    wide[...] = jnp.zeros_like(wide)
    spread_base(base)

    def one(s, carry):
        @pl.when(places[s, 3] > 0)
        def _():
            lx, ly, lz = places[s, 0], places[s, 1], places[s, 2]
            spread = jnp.where(base[...] == lz, 1.0, 0.0).astype(jnp.bfloat16)
            v = stacked(boxes, s).astype(jnp.float32)
            add_box(wide, (v * v).astype(jnp.bfloat16), spread, lx, ly)

        return carry

    lax.fori_loop(0, boxes.shape[0], one, 0)
    out[...] = wide[...].astype(out.dtype)


def update_kernel(
    table, boxes, crowd, low, settled, out, density, wide, base, taps, places, sem
):
    fetch_places(table, places, sem)
    density[...] = low[...].astype(jnp.float32)
    wide[...] = jnp.zeros_like(wide)
    spread_base(base)
    from_b = lax.broadcasted_iota(jnp.int32, taps.shape, 0) - LANES
    to_b = lax.broadcasted_iota(jnp.int32, taps.shape, 1)
    gap = from_b - to_b
    beside = (gap == B) | (gap == -B)
    same = (from_b >= 0) & (from_b < LANES) & (lax.rem(from_b + LANES, LANES) // B == to_b // B)
    along = same & ((gap == 1) | (gap == -1))
    taps[...] = jnp.where(gap == 0, -6.0, jnp.where(beside | along, 1.0, 0.0)).astype(taps.dtype)
    step = lax.rem(lax.broadcasted_iota(jnp.int32, (B * B // GROUP, LANES), 0), B)
    edge = jnp.zeros((B, LANES), jnp.bfloat16)
    total = B * B // GROUP

    def one(s, carry):
        @pl.when(places[s, 3] > 0)
        def _():
            lx, ly, lz = places[s, 0], places[s, 1], places[s, 2]
            spread = jnp.where(base[...] == lz, 1.0, 0.0).astype(jnp.bfloat16)
            cr = take_box(crowd, spread, lx, ly)
            dn = take_box(density, spread, lx, ly)
            v = stacked(boxes, s)
            near = jnp.concatenate(
                [
                    jnp.concatenate([edge, v[: total - B]], 0),
                    v,
                    jnp.concatenate([v[B:], edge], 0),
                ],
                1,
            )
            lap = jnp.dot(near, taps[...], preferred_element_type=jnp.float32)
            p = v.astype(jnp.float32)
            across = jnp.where(step < B - 1, pltpu.roll(p, total - 1, 0), 0.0) + jnp.where(
                step > 0, pltpu.roll(p, 1, 0), 0.0
            )
            others = cr - p * p
            reaction = 4.0 * p * (1.0 - p) * (p - 0.5 + (dn - 0.5))
            fresh = p + 0.1 * (lap + across + reaction - 2.0 * p * others)
            fresh = fresh.astype(jnp.bfloat16)
            for j in range(B // GROUP):
                settled[s, :, j * LANES : (j + 1) * LANES] = fresh[j * B : (j + 1) * B]
            add_box(wide, fresh, spread, lx, ly)

        @pl.when(places[s, 3] <= 0)
        def _():
            settled[s] = jnp.zeros(settled.shape[1:], settled.dtype)

        return carry

    lax.fori_loop(0, boxes.shape[0], one, 0)
    out[...] = wide[...].astype(out.dtype)


def finish_kernel(
    corner_in, returned, deposit, matrix, phase_next, matrix_next, corner, turned, sem, fetch
):
    edge = matrix.shape[1]
    load = pltpu.make_async_copy(corner_in, corner, fetch.at[0])
    load.start()
    now = matrix[...]
    turned[...] = now - 0.5 * now * jnp.swapaxes(deposit[...], 0, 1)
    store = pltpu.make_async_copy(turned, matrix_next, fetch.at[1])
    store.start()
    load.wait()
    copies = [
        pltpu.make_async_copy(
            returned.at[lax.div(corner[1, c], edge)], phase_next.at[c], sem.at[c]
        )
        for c in range(phase_next.shape[0])
    ]
    for copy in copies:
        copy.start()
    store.wait()
    for copy in copies:
        copy.wait()


VMEM = pl.BlockSpec(memory_space=pltpu.VMEM)
ANY = pl.BlockSpec(memory_space=pl.ANY)
HBM = pl.BlockSpec(memory_space=pltpu.HBM)
LIMIT = 24 * 2**20


def like(shape, dtype):
    return jax.ShapeDtypeStruct(shape, dtype)


def dma(*shape):
    return pltpu.SemaphoreType.DMA(shape)


def linked(number):
    return pltpu.CompilerParams(
        collective_id=number, has_side_effects=True, vmem_limit_bytes=LIMIT
    )


def per_device(phase_box, matrix_density, box_corner):
    slab_rows, slab_cols, grid_depth = matrix_density.shape
    peers = lax.axis_size("gy")
    bf16, f32 = jnp.bfloat16, jnp.float32
    slots = (peers,) + phase_box.shape[1:]
    notes = (peers, 8, LANES)
    torus = (SIDE, SIDE) + phase_box.shape[1:]
    rows = (phase_box.shape[1] // 2,) + phase_box.shape[2:]
    moving = [pltpu.VMEM((2, SIDE, SIDE) + rows, bf16), pltpu.VMEM((2, 2, 2, SIDE - 1) + rows, bf16)]
    wide = (2 * slab_cols, 2 * slab_rows, grid_depth)
    half = (2 * slab_cols, slab_rows, grid_depth)
    quarter = (slab_cols, slab_rows, grid_depth)
    boxes, places, density = pl.pallas_call(
        gather_kernel,
        out_shape=(like(torus, bf16), like(notes, jnp.int32), like(wide, bf16)),
        in_specs=[HBM, HBM, HBM],
        out_specs=(ANY, ANY, ANY),
        scratch_shapes=[
            pltpu.SMEM(box_corner.shape, jnp.int32),
            pltpu.VMEM(phase_box.shape, bf16),
            pltpu.VMEM(matrix_density.shape, f32),
            pltpu.VMEM(notes, jnp.int32),
            pltpu.VMEM(quarter, bf16),
            pltpu.VMEM(torus, bf16),
        ]
        + moving
        + [
            pltpu.VMEM(quarter, bf16),
            dma(2, 2, 6), dma(2, 2, 6), dma(peers - 1), dma(peers - 1),
            dma(2), dma(2), dma(3), dma(3), dma(6), dma(3),
        ],
        compiler_params=linked(0),
        name="gather",
    )(
        *(pltpu.with_memory_space_constraint(a, pltpu.HBM) for a in (box_corner, phase_box, matrix_density))
    )
    boxes = boxes.reshape(slots)

    spread = pltpu.VMEM((GROUP * LANES, LANES), jnp.int32)
    taps = pltpu.VMEM((3 * LANES, LANES), bf16)
    spots = [pltpu.SMEM((peers, LANES), jnp.int32), dma()]
    quiet = pltpu.CompilerParams(vmem_limit_bytes=LIMIT)
    crowd = pl.pallas_call(
        crowd_kernel,
        out_shape=like(wide, bf16),
        in_specs=[ANY, VMEM],
        out_specs=VMEM,
        scratch_shapes=[pltpu.VMEM(wide, f32), spread] + spots,
        compiler_params=quiet,
        name="crowd",
    )(places, boxes)

    crowd = pl.pallas_call(
        rim_kernel,
        out_shape=like(wide, f32),
        in_specs=[VMEM],
        out_specs=VMEM,
        scratch_shapes=[
            pltpu.VMEM((2,) + half, bf16),
            pltpu.VMEM(wide, bf16),
            pltpu.VMEM((2, slab_cols) + wide[1:], bf16),
            dma(2, 4), dma(2, 4), dma(4), dma(4),
        ],
        compiler_params=linked(1),
        name="rim",
    )(crowd)

    settled, deposit = pl.pallas_call(
        update_kernel,
        out_shape=(like(slots, bf16), like(wide, bf16)),
        in_specs=[ANY, VMEM, VMEM, VMEM],
        out_specs=(VMEM, VMEM),
        scratch_shapes=[pltpu.VMEM(wide, f32), pltpu.VMEM(wide, f32), spread, taps] + spots,
        compiler_params=quiet,
        name="update",
    )(places, boxes, crowd, density)

    returned, deposit = pl.pallas_call(
        return_kernel,
        out_shape=(like(torus, bf16), like(quarter, f32)),
        in_specs=[VMEM, VMEM],
        out_specs=(ANY, VMEM),
        scratch_shapes=moving
        + [
            pltpu.VMEM((2,) + quarter, bf16),
            pltpu.VMEM(quarter, bf16),
            pltpu.VMEM(quarter, bf16),
            dma(2, 2, 6), dma(2, 2, 6), dma(2), dma(2), dma(2), dma(2), dma(2),
        ],
        compiler_params=linked(2),
        name="return",
    )(settled.reshape(torus), deposit)
    returned = returned.reshape(slots)

    return pl.pallas_call(
        finish_kernel,
        out_shape=(like(phase_box.shape, bf16), like(matrix_density.shape, f32)),
        in_specs=[HBM, VMEM, VMEM, VMEM],
        out_specs=(ANY, ANY),
        scratch_shapes=[
            pltpu.SMEM(box_corner.shape, jnp.int32),
            pltpu.VMEM(matrix_density.shape, f32),
            dma(phase_box.shape[0]),
            dma(2),
        ],
        compiler_params=quiet,
        name="finish",
    )(
        pltpu.with_memory_space_constraint(box_corner, pltpu.HBM), returned, deposit, matrix_density
    )


def solution(mesh):
    return jax.shard_map(
        per_device,
        mesh=mesh,
        in_specs=(P(("gx", "gy"), None, None), P("gx", "gy", None), P(None, ("gx", "gy"))),
        out_specs=(P(("gx", "gy"), None, None), P("gx", "gy", None)),
        check_vma=False,
    )
```

```python
import jax
import jax.numpy as jnp
from jax import lax
from jax.experimental import pallas as pl
from jax.experimental.pallas import tpu as pltpu
from jax.sharding import PartitionSpec as P

B = 32
LANES = 128
GROUP = LANES // B
SIDE = 4
RIM_CHUNKS = 4

def signal(axis, target):
    pl.semaphore_signal(
        pltpu.get_barrier_semaphore(),
        inc=1,
        device_id={axis: target},
        device_id_type=pl.DeviceIdType.MESH,
    )


def remote(src, dst, send, recv, axis, target):
    return pltpu.make_async_remote_copy(
        src_ref=src,
        dst_ref=dst,
        send_sem=send,
        recv_sem=recv,
        device_id={axis: target},
        device_id_type=pl.DeviceIdType.MESH,
    )


def greet():
    me, row = lax.axis_index("gy"), lax.axis_index("gx")
    columns, rows = lax.axis_size("gy"), lax.axis_size("gx")
    high, low = me // SIDE, lax.rem(me, SIDE)
    count = 0
    for step in (1, SIDE - 1):
        signal("gy", lax.rem(high + step, SIDE) * SIDE + low)
        signal("gy", high * SIDE + lax.rem(low + step, SIDE))
        count += 2
    for axis, at, size, step in (("gx", row, rows, 1), ("gx", row, rows, -1)):
        there = (at < size - 1) if step > 0 else (at > 0)
        count += there.astype(jnp.int32)

        @pl.when(there)
        def _():
            signal(axis, at + step)

    for step in (1, -1):
        far = (low == (SIDE - 1 if step > 0 else 0)) & (
            (me < columns - 1) if step > 0 else (me > 0)
        )
        count += far.astype(jnp.int32)

        @pl.when(far)
        def _():
            signal("gy", me + step)

    return count


class Exchange:
    def __init__(self, src, dst, stage, relay, send, recv, own, share_y):
        self.src, self.dst, self.stage, self.relay = src, dst, stage, relay
        self.send, self.recv, self.own = send, recv, own
        me = lax.axis_index("gy")
        self.at = (me // SIDE, lax.rem(me, SIDE))
        self.share = (SIDE // 2, share_y)
        self.rows = src.shape[2] // 2

    def turn(self, axis, step):
        return lax.rem(self.at[axis] + SIDE + step, SIDE)

    def device(self, axis, step):
        other, moved = self.at[1 - axis], self.turn(axis, step)
        return moved * SIDE + other if axis == 0 else other * SIDE + moved

    def whole(self, ref, half, first, second):
        rest = pl.ds(half * self.rows, self.rows)
        return ref.at[first, second, rest]

    def block(self, half, stage, goal, part):
        if stage == 1:
            return self.stage.at[half, part, goal]
        return self.whole(self.src, half, *((goal, part) if half == 0 else (part, goal)))

    def place(self, half, stage, origin, part):
        if stage == 0:
            return self.stage.at[half, origin, part]
        return self.whole(self.dst, half, *((part, origin) if half == 0 else (origin, part)))

    def copies(self, half, stage):
        axis = (half + stage) % 2
        share = self.share[axis]
        parts = (pl.ds(0, share), pl.ds(share, SIDE - share))
        sizes = (share, SIDE - share)
        every = pl.ds(0, SIDE)
        out = []
        for kind in ("relay", "direct", "forward"):
            for side in range(2):
                step = 1 if side == 0 else -1
                if kind == "direct":
                    src = self.block(half, stage, self.turn(axis, step), every)
                    dst = self.place(half, stage, self.at[axis], every)
                else:
                    hold = self.relay.at[half, stage, side, pl.ds(0, sizes[side])]
                    if kind == "relay":
                        src, dst = self.block(half, stage, self.turn(axis, 2), parts[side]), hold
                    else:
                        src = hold
                        dst = self.place(half, stage, self.turn(axis, -step), parts[side])
                at = (half, stage, len(out))
                out.append(
                    remote(src, dst, self.send.at[at], self.recv.at[at], "gy", self.device(axis, step))
                )
        return out

    def prepare(self):
        x, y = self.at
        self.stage[0, x] = self.src[x, :, : self.rows]
        self.stage[1, y] = self.src[:, y, self.rows :]

    def start(self, stage, half):
        copies = self.copies(half, stage)
        for copy in copies[:4]:
            copy.start()
        if stage == 1:
            self.kept(half).start()

    def forward(self, stage, half):
        copies = self.copies(half, stage)
        for side in range(2):
            copies[side].wait_recv()
            copies[4 + side].start()

    def arrive(self, stage, half):
        for copy in self.copies(half, stage)[2:]:
            copy.wait_recv()

    def kept(self, half):
        axis = (half + 1) % 2
        every = pl.ds(0, SIDE)
        return pltpu.make_async_copy(
            self.block(half, 1, self.at[axis], every),
            self.place(half, 1, self.at[axis], every),
            self.own.at[half],
        )

    def finish(self):
        for half in range(2):
            for stage in range(2):
                for copy in self.copies(half, stage):
                    copy.wait_send()
            self.kept(half).wait()


def gather_kernel(
    corner_in, phase_in, density_in, boxes, places, density,
    corner, phase, matrix, table, low, outbox, stage, relay, half, send, recv, table_send, table_recv,
    y_send, y_recv, x_send, x_recv, own, fetch,
):
    me, row = lax.axis_index("gy"), lax.axis_index("gx")
    columns, rows = lax.axis_size("gy"), lax.axis_size("gx")
    edge = low.shape[0]
    loads = [
        pltpu.make_async_copy(phase_in, phase, fetch.at[0]),
        pltpu.make_async_copy(density_in, matrix, fetch.at[1]),
        pltpu.make_async_copy(corner_in, corner, fetch.at[2]),
    ]
    for load in loads:
        load.start()
    part = edge // 2
    barrier = pltpu.get_barrier_semaphore()
    others = [lax.rem(me + k, columns) for k in range(1, columns)]
    senders = [lax.rem(me + columns - k, columns) for k in range(1, columns)]
    for target in others:
        signal("gy", target)

    @pl.when(row > 0)
    def _():
        signal("gx", row - 1)

    @pl.when(row < rows - 1)
    def _():
        signal("gx", row + 1)

    cells = range(phase.shape[0])
    loads[2].wait()
    home = [lax.div(corner[1, c], edge) for c in cells]
    lane = lax.broadcasted_iota(jnp.int32, table.shape[1:], 1)
    loads[0].wait()

    def fill(s, carry):
        source, found = jnp.int32(0), jnp.int32(0)
        for c in cells:
            source = jnp.where(home[c] == s, c, source)
            found = jnp.where(home[c] == s, 1, found)
        note = (
            corner[0, source] - row * edge,
            corner[1, source] - s * edge,
            corner[2, source],
            found,
        )
        line = jnp.zeros_like(lane)
        for k, value in enumerate(note):
            line = jnp.where(lane == k, value, line)
        table[s] = line
        outbox[s // SIDE, lax.rem(s, SIDE)] = phase[source]
        return carry

    lax.fori_loop(0, columns, fill, 0)
    loads[1].wait()
    low[...] = jnp.swapaxes(matrix[...], 0, 1).astype(low.dtype)

    @pl.when(me == columns - 1)
    def _():
        half[...] = jnp.zeros_like(half)

    boxes_out = Exchange(outbox, boxes, stage, relay, send, recv, own, 3)
    boxes_out.prepare()

    neighbours = (row > 0).astype(jnp.int32) + (row < rows - 1).astype(jnp.int32)
    pl.semaphore_wait(barrier, columns - 1 + neighbours)

    def along_y(k):
        rest = pl.ds(k * part, part)
        return remote(low.at[rest], half.at[rest], y_send.at[k], y_recv.at[k], "gy", me - 1)

    def along_x(k):
        src = low if k == 2 else half.at[pl.ds(k * part, part)]
        rest = pl.ds(0, edge) if k == 2 else pl.ds(edge + k * part, part)
        dst = density.at[rest, pl.ds(edge, edge)]
        return remote(src, dst, x_send.at[k], x_recv.at[k], "gx", row - 1)

    def keep(k):
        src = low if k == 2 else half.at[pl.ds(k * part, part)]
        rest = pl.ds(0, edge) if k == 2 else pl.ds(edge + k * part, part)
        return pltpu.make_async_copy(src, density.at[rest, pl.ds(0, edge)], own.at[2 + k])

    def start_y(k):
        @pl.when(me > 0)
        def _():
            along_y(k).start()

    def start_x(k):
        keep(k).start()

        @pl.when(row > 0)
        def _():
            along_x(k).start()

    def take_y(k):
        @pl.when(me < columns - 1)
        def _():
            along_y(k).wait_recv()

    for h in range(2):
        boxes_out.start(0, h)
    start_x(2)
    notes = [
        remote(table.at[target], places.at[me], table_send.at[k], table_recv.at[k], "gy", target)
        for k, target in enumerate(others)
    ]
    for note in notes:
        note.start()
    note = pltpu.make_async_copy(table.at[me], places.at[me], own.at[5])
    note.start()
    for h in range(2):
        boxes_out.forward(0, h)
    start_y(0)
    start_y(1)
    for h in range(2):
        boxes_out.arrive(0, h)
        boxes_out.start(1, h)
    take_y(0)
    start_x(0)
    for h in range(2):
        boxes_out.forward(1, h)
    take_y(1)
    start_x(1)
    for h in range(2):
        boxes_out.arrive(1, h)
    for k, sender in enumerate(senders):
        remote(
            table.at[me], places.at[sender], table_send.at[k], table_recv.at[k], "gy", sender
        ).wait_recv()
    for copy in notes:
        copy.wait_send()
    note.wait()
    for k in range(3):
        keep(k).wait()

        @pl.when(row > 0)
        def _():
            along_x(k).wait_send()

        @pl.when(row < rows - 1)
        def _():
            along_x(k).wait_recv()

    for k in range(2):

        @pl.when(me > 0)
        def _():
            along_y(k).wait_send()

    boxes_out.finish()


def rim_kernel(
    own, crowd, from_x, full, from_y, done, back,
    x_send, x_recv, y_send, y_recv, b_send, b_recv,
):
    me, row = lax.axis_index("gy"), lax.axis_index("gx")
    columns, rows = lax.axis_size("gy"), lax.axis_size("gx")
    edge = own.shape[1] // 2
    chunks, _, part, _ = full.shape
    count = 0
    for axis, at, size in (("gx", row, rows), ("gy", me, columns)):
        for there, target in ((at > 0, at - 1), (at < size - 1, at + 1)):
            count += there.astype(jnp.int32)

            @pl.when(there)
            def _():
                signal(axis, target)

    pl.semaphore_wait(pltpu.get_barrier_semaphore(), count)
    low, high = slice(0, edge), slice(edge, 2 * edge)
    ups = ((me < columns - 1, me > 0, me + 1, high, low), (me > 0, me < columns - 1, me - 1, low, high))

    def spill(c):
        src = own.at[:, pl.ds(edge + c * part, part)]
        return remote(src, from_x.at[c], x_send.at[c], x_recv.at[c], "gx", row + 1)

    def exchange(c, k):
        _, _, target, sent, _ = ups[k]
        return remote(
            full.at[c, sent], from_y.at[k, c], y_send.at[k, c], y_recv.at[k, c], "gy", target
        )

    def give(c):
        return remote(done.at[c], back.at[c], b_send.at[c], b_recv.at[c], "gx", row - 1)

    @pl.when(row < rows - 1)
    def _():
        for c in range(chunks):
            spill(c).start()

    for c in range(chunks):
        mine = slice(c * part, (c + 1) * part)

        @pl.when(row > 0)
        def _():
            spill(c).wait_recv()
            full[c] = own[:, mine] + from_x[c]

        @pl.when(row == 0)
        def _():
            full[c] = own[:, mine]

        for k in range(2):

            @pl.when(ups[k][0])
            def _():
                exchange(c, k).start()

    for c in range(chunks):
        for k in range(2):
            _, takes, _, _, into = ups[k]

            @pl.when(takes)
            def _():
                exchange(c, k).wait_recv()
                done[c, into] = full[c, into] + from_y[k, c]

            @pl.when(jnp.logical_not(takes))
            def _():
                done[c, into] = full[c, into]

        @pl.when(row > 0)
        def _():
            give(c).start()

        crowd[:, c * part : (c + 1) * part] = done[c].astype(jnp.float32)

    @pl.when(row == rows - 1)
    def _():
        crowd[:, edge:] = jnp.zeros((crowd.shape[0], edge, crowd.shape[2]), jnp.float32)

    @pl.when(row < rows - 1)
    def _():
        for c in range(chunks):
            give(c).wait_recv()
            crowd[:, edge + c * part : edge + (c + 1) * part] = back[c].astype(jnp.float32)

    for c in range(chunks):

        @pl.when(row < rows - 1)
        def _():
            spill(c).wait_send()

        for k in range(2):

            @pl.when(ups[k][0])
            def _():
                exchange(c, k).wait_send()

        @pl.when(row > 0)
        def _():
            give(c).wait_send()


def return_kernel(
    settled, wide, returned, deposit, stage, relay, from_x, outgoing, from_y,
    send, recv, x_send, x_recv, y_send, y_recv, own,
):
    me, row = lax.axis_index("gy"), lax.axis_index("gx")
    columns, rows = lax.axis_size("gy"), lax.axis_size("gx")
    edge = wide.shape[1] // 2
    count = greet()
    boxes_back = Exchange(settled, returned, stage, relay, send, recv, own, 1)
    boxes_back.prepare()
    pl.semaphore_wait(pltpu.get_barrier_semaphore(), count)
    halves = (slice(edge, 2 * edge), slice(0, edge))

    def along_x(k):
        return remote(
            wide.at[halves[k], pl.ds(edge, edge)], from_x.at[k], x_send.at[k], x_recv.at[k], "gx", row + 1
        )

    for h in range(2):
        boxes_back.start(0, h)

    @pl.when(row < rows - 1)
    def _():
        for k in range(2):
            along_x(k).start()

    for h in range(2):
        boxes_back.forward(0, h)

    @pl.when(row > 0)
    def _():
        along_x(0).wait_recv()
        outgoing[...] = wide[edge:, :edge] + from_x[0]

    @pl.when(row == 0)
    def _():
        outgoing[...] = wide[edge:, :edge]

    part = edge // 2

    def along_y(k):
        rest = pl.ds(k * part, part)
        return remote(
            outgoing.at[rest], from_y.at[rest], y_send.at[k], y_recv.at[k], "gy", me + 1
        )

    @pl.when(me < columns - 1)
    def _():
        for k in range(2):
            along_y(k).start()

    for h in range(2):
        boxes_back.arrive(0, h)
        boxes_back.start(1, h)

    @pl.when(row > 0)
    def _():
        along_x(1).wait_recv()
        deposit[...] = wide[:edge, :edge].astype(jnp.float32) + from_x[1].astype(jnp.float32)

    @pl.when(row == 0)
    def _():
        deposit[...] = wide[:edge, :edge].astype(jnp.float32)

    for h in range(2):
        boxes_back.forward(1, h)

    @pl.when(me > 0)
    def _():
        for k in range(2):
            along_y(k).wait_recv()
        deposit[...] = deposit[...] + from_y[...].astype(jnp.float32)

    for h in range(2):
        boxes_back.arrive(1, h)

    boxes_back.finish()

    @pl.when(me < columns - 1)
    def _():
        for k in range(2):
            along_y(k).wait_send()

    @pl.when(row < rows - 1)
    def _():
        for k in range(2):
            along_x(k).wait_send()


def fetch_places(table, places, sem):
    copy = pltpu.make_async_copy(table.at[:, 0], places, sem)
    copy.start()
    copy.wait()


def spread_base(base):
    row = lax.broadcasted_iota(jnp.int32, base.shape, 0)
    lane = lax.broadcasted_iota(jnp.int32, base.shape, 1)
    base[...] = jnp.where(row // LANES == lane // B, lax.rem(row, LANES) - lax.rem(lane, B), -1)


def stacked(boxes, s):
    return jnp.concatenate(
        [boxes[s, :, j * LANES : (j + 1) * LANES] for j in range(B // GROUP)], 0
    )


def add_box(wide, v, spread, lx, ly):
    placed = lax.dot_general(
        v, spread, (((1,), (1,)), ((), ())), preferred_element_type=jnp.float32
    )
    for j in range(B // GROUP):
        for i in range(GROUP):
            at = (ly + (GROUP * j + i), pl.ds(lx, B), slice(None))
            wide[at] = wide[at] + placed[j * B : (j + 1) * B, i * LANES : (i + 1) * LANES]


def take_box(field, spread, lx, ly):
    rows = []
    for j in range(B // GROUP):
        parts = [field[ly + (GROUP * j + i), pl.ds(lx, B), :] for i in range(GROUP)]
        rows.append(jnp.concatenate([p.astype(jnp.bfloat16) for p in parts], 1))
    return jnp.dot(jnp.concatenate(rows, 0), spread, preferred_element_type=jnp.float32)


def crowd_kernel(table, boxes, out, wide, base, places, sem):
    fetch_places(table, places, sem)
    wide[...] = jnp.zeros_like(wide)
    spread_base(base)

    def one(s, carry):
        @pl.when(places[s, 3] > 0)
        def _():
            lx, ly, lz = places[s, 0], places[s, 1], places[s, 2]
            spread = jnp.where(base[...] == lz, 1.0, 0.0).astype(jnp.bfloat16)
            v = stacked(boxes, s).astype(jnp.float32)
            add_box(wide, (v * v).astype(jnp.bfloat16), spread, lx, ly)

        return carry

    lax.fori_loop(0, boxes.shape[0], one, 0)
    out[...] = wide[...].astype(out.dtype)


def update_kernel(
    table, boxes, crowd, low, settled, out, density, wide, base, taps, places, sem
):
    fetch_places(table, places, sem)
    density[...] = low[...].astype(jnp.float32)
    wide[...] = jnp.zeros_like(wide)
    spread_base(base)
    from_b = lax.broadcasted_iota(jnp.int32, taps.shape, 0) - LANES
    to_b = lax.broadcasted_iota(jnp.int32, taps.shape, 1)
    gap = from_b - to_b
    beside = (gap == B) | (gap == -B)
    same = (from_b >= 0) & (from_b < LANES) & (lax.rem(from_b + LANES, LANES) // B == to_b // B)
    along = same & ((gap == 1) | (gap == -1))
    taps[...] = jnp.where(gap == 0, -6.0, jnp.where(beside | along, 1.0, 0.0)).astype(taps.dtype)
    step = lax.rem(lax.broadcasted_iota(jnp.int32, (B * B // GROUP, LANES), 0), B)
    edge = jnp.zeros((B, LANES), jnp.bfloat16)
    total = B * B // GROUP

    def one(s, carry):
        @pl.when(places[s, 3] > 0)
        def _():
            lx, ly, lz = places[s, 0], places[s, 1], places[s, 2]
            spread = jnp.where(base[...] == lz, 1.0, 0.0).astype(jnp.bfloat16)
            cr = take_box(crowd, spread, lx, ly)
            dn = take_box(density, spread, lx, ly)
            v = stacked(boxes, s)
            near = jnp.concatenate(
                [
                    jnp.concatenate([edge, v[: total - B]], 0),
                    v,
                    jnp.concatenate([v[B:], edge], 0),
                ],
                1,
            )
            lap = jnp.dot(near, taps[...], preferred_element_type=jnp.float32)
            p = v.astype(jnp.float32)
            across = jnp.where(step < B - 1, pltpu.roll(p, total - 1, 0), 0.0) + jnp.where(
                step > 0, pltpu.roll(p, 1, 0), 0.0
            )
            others = cr - p * p
            reaction = 4.0 * p * (1.0 - p) * (p - 0.5 + (dn - 0.5))
            fresh = p + 0.1 * (lap + across + reaction - 2.0 * p * others)
            fresh = fresh.astype(jnp.bfloat16)
            for j in range(B // GROUP):
                settled[s, :, j * LANES : (j + 1) * LANES] = fresh[j * B : (j + 1) * B]
            add_box(wide, fresh, spread, lx, ly)

        @pl.when(places[s, 3] <= 0)
        def _():
            settled[s] = jnp.zeros(settled.shape[1:], settled.dtype)

        return carry

    lax.fori_loop(0, boxes.shape[0], one, 0)
    out[...] = wide[...].astype(out.dtype)


def finish_kernel(
    corner_in, returned, deposit, matrix, phase_next, matrix_next, corner, turned, sem, fetch
):
    edge = matrix.shape[1]
    load = pltpu.make_async_copy(corner_in, corner, fetch.at[0])
    load.start()
    now = matrix[...]
    turned[...] = now - 0.5 * now * jnp.swapaxes(deposit[...], 0, 1)
    store = pltpu.make_async_copy(turned, matrix_next, fetch.at[1])
    store.start()
    load.wait()
    copies = [
        pltpu.make_async_copy(
            returned.at[lax.div(corner[1, c], edge)], phase_next.at[c], sem.at[c]
        )
        for c in range(phase_next.shape[0])
    ]
    for copy in copies:
        copy.start()
    store.wait()
    for copy in copies:
        copy.wait()


VMEM = pl.BlockSpec(memory_space=pltpu.VMEM)
ANY = pl.BlockSpec(memory_space=pl.ANY)
HBM = pl.BlockSpec(memory_space=pltpu.HBM)
LIMIT = 24 * 2**20


def like(shape, dtype):
    return jax.ShapeDtypeStruct(shape, dtype)


def dma(*shape):
    return pltpu.SemaphoreType.DMA(shape)


def linked(number):
    return pltpu.CompilerParams(
        collective_id=number, has_side_effects=True, vmem_limit_bytes=LIMIT
    )


def per_device(phase_box, matrix_density, box_corner):
    slab_rows, slab_cols, grid_depth = matrix_density.shape
    peers = lax.axis_size("gy")
    bf16, f32 = jnp.bfloat16, jnp.float32
    slots = (peers,) + phase_box.shape[1:]
    notes = (peers, 8, LANES)
    torus = (SIDE, SIDE) + phase_box.shape[1:]
    rows = (phase_box.shape[1] // 2,) + phase_box.shape[2:]
    moving = [pltpu.VMEM((2, SIDE, SIDE) + rows, bf16), pltpu.VMEM((2, 2, 2, SIDE - 1) + rows, bf16)]
    wide = (2 * slab_cols, 2 * slab_rows, grid_depth)
    strips = (RIM_CHUNKS, 2 * slab_cols, slab_rows // RIM_CHUNKS, grid_depth)
    quarter = (slab_cols, slab_rows, grid_depth)
    boxes, places, density = pl.pallas_call(
        gather_kernel,
        out_shape=(like(torus, bf16), like(notes, jnp.int32), like(wide, bf16)),
        in_specs=[HBM, HBM, HBM],
        out_specs=(ANY, ANY, ANY),
        scratch_shapes=[
            pltpu.SMEM(box_corner.shape, jnp.int32),
            pltpu.VMEM(phase_box.shape, bf16),
            pltpu.VMEM(matrix_density.shape, f32),
            pltpu.VMEM(notes, jnp.int32),
            pltpu.VMEM(quarter, bf16),
            pltpu.VMEM(torus, bf16),
        ]
        + moving
        + [
            pltpu.VMEM(quarter, bf16),
            dma(2, 2, 6), dma(2, 2, 6), dma(peers - 1), dma(peers - 1),
            dma(2), dma(2), dma(3), dma(3), dma(6), dma(3),
        ],
        compiler_params=linked(0),
        name="gather",
    )(
        *(pltpu.with_memory_space_constraint(a, pltpu.HBM) for a in (box_corner, phase_box, matrix_density))
    )
    boxes = boxes.reshape(slots)

    spread = pltpu.VMEM((GROUP * LANES, LANES), jnp.int32)
    taps = pltpu.VMEM((3 * LANES, LANES), bf16)
    spots = [pltpu.SMEM((peers, LANES), jnp.int32), dma()]
    quiet = pltpu.CompilerParams(vmem_limit_bytes=LIMIT)
    crowd = pl.pallas_call(
        crowd_kernel,
        out_shape=like(wide, bf16),
        in_specs=[ANY, VMEM],
        out_specs=VMEM,
        scratch_shapes=[pltpu.VMEM(wide, f32), spread] + spots,
        compiler_params=quiet,
        name="crowd",
    )(places, boxes)

    crowd = pl.pallas_call(
        rim_kernel,
        out_shape=like(wide, f32),
        in_specs=[VMEM],
        out_specs=VMEM,
        scratch_shapes=[
            pltpu.VMEM(strips, bf16),
            pltpu.VMEM(strips, bf16),
            pltpu.VMEM((2, RIM_CHUNKS, slab_cols) + strips[2:], bf16),
            pltpu.VMEM(strips, bf16),
            pltpu.VMEM(strips, bf16),
            dma(RIM_CHUNKS), dma(RIM_CHUNKS), dma(2, RIM_CHUNKS), dma(2, RIM_CHUNKS),
            dma(RIM_CHUNKS), dma(RIM_CHUNKS),
        ],
        compiler_params=linked(1),
        name="rim",
    )(crowd)

    settled, deposit = pl.pallas_call(
        update_kernel,
        out_shape=(like(slots, bf16), like(wide, bf16)),
        in_specs=[ANY, VMEM, VMEM, VMEM],
        out_specs=(VMEM, VMEM),
        scratch_shapes=[pltpu.VMEM(wide, f32), pltpu.VMEM(wide, f32), spread, taps] + spots,
        compiler_params=quiet,
        name="update",
    )(places, boxes, crowd, density)

    returned, deposit = pl.pallas_call(
        return_kernel,
        out_shape=(like(torus, bf16), like(quarter, f32)),
        in_specs=[VMEM, VMEM],
        out_specs=(ANY, VMEM),
        scratch_shapes=moving
        + [
            pltpu.VMEM((2,) + quarter, bf16),
            pltpu.VMEM(quarter, bf16),
            pltpu.VMEM(quarter, bf16),
            dma(2, 2, 6), dma(2, 2, 6), dma(2), dma(2), dma(2), dma(2), dma(2),
        ],
        compiler_params=linked(2),
        name="return",
    )(settled.reshape(torus), deposit)
    returned = returned.reshape(slots)

    return pl.pallas_call(
        finish_kernel,
        out_shape=(like(phase_box.shape, bf16), like(matrix_density.shape, f32)),
        in_specs=[HBM, VMEM, VMEM, VMEM],
        out_specs=(ANY, ANY),
        scratch_shapes=[
            pltpu.SMEM(box_corner.shape, jnp.int32),
            pltpu.VMEM(matrix_density.shape, f32),
            dma(phase_box.shape[0]),
            dma(2),
        ],
        compiler_params=quiet,
        name="finish",
    )(
        pltpu.with_memory_space_constraint(box_corner, pltpu.HBM), returned, deposit, matrix_density
    )


def solution(mesh):
    return jax.shard_map(
        per_device,
        mesh=mesh,
        in_specs=(P(("gx", "gy"), None, None), P("gx", "gy", None), P(None, ("gx", "gy"))),
        out_specs=(P(("gx", "gy"), None, None), P("gx", "gy", None)),
        check_vma=False,
    )
```

```python
import jax
import jax.numpy as jnp
from jax import lax
from jax.experimental import pallas as pl
from jax.experimental.pallas import tpu as pltpu
from jax.sharding import PartitionSpec as P

B = 32
LANES = 128
GROUP = LANES // B
SIDE = 4
TOGETHER = 2
RIM_CHUNKS = 4

def signal(axis, target):
    pl.semaphore_signal(
        pltpu.get_barrier_semaphore(),
        inc=1,
        device_id={axis: target},
        device_id_type=pl.DeviceIdType.MESH,
    )


def remote(src, dst, send, recv, axis, target):
    return pltpu.make_async_remote_copy(
        src_ref=src,
        dst_ref=dst,
        send_sem=send,
        recv_sem=recv,
        device_id={axis: target},
        device_id_type=pl.DeviceIdType.MESH,
    )


def greet():
    me, row = lax.axis_index("gy"), lax.axis_index("gx")
    columns, rows = lax.axis_size("gy"), lax.axis_size("gx")
    high, low = me // SIDE, lax.rem(me, SIDE)
    count = 0
    for step in (1, SIDE - 1):
        signal("gy", lax.rem(high + step, SIDE) * SIDE + low)
        signal("gy", high * SIDE + lax.rem(low + step, SIDE))
        count += 2
    for axis, at, size, step in (("gx", row, rows, 1), ("gx", row, rows, -1)):
        there = (at < size - 1) if step > 0 else (at > 0)
        count += there.astype(jnp.int32)

        @pl.when(there)
        def _():
            signal(axis, at + step)

    for step in (1, -1):
        far = (low == (SIDE - 1 if step > 0 else 0)) & (
            (me < columns - 1) if step > 0 else (me > 0)
        )
        count += far.astype(jnp.int32)

        @pl.when(far)
        def _():
            signal("gy", me + step)

    return count


class Exchange:
    def __init__(self, src, dst, stage, relay, send, recv, own, share_y):
        self.src, self.dst, self.stage, self.relay = src, dst, stage, relay
        self.send, self.recv, self.own = send, recv, own
        me = lax.axis_index("gy")
        self.at = (me // SIDE, lax.rem(me, SIDE))
        self.share = (SIDE // 2, share_y)
        self.rows = src.shape[2] // 2

    def turn(self, axis, step):
        return lax.rem(self.at[axis] + SIDE + step, SIDE)

    def device(self, axis, step):
        other, moved = self.at[1 - axis], self.turn(axis, step)
        return moved * SIDE + other if axis == 0 else other * SIDE + moved

    def whole(self, ref, half, first, second):
        rest = pl.ds(half * self.rows, self.rows)
        return ref.at[first, second, rest]

    def block(self, half, stage, goal, part):
        if stage == 1:
            return self.stage.at[half, part, goal]
        return self.whole(self.src, half, *((goal, part) if half == 0 else (part, goal)))

    def place(self, half, stage, origin, part):
        if stage == 0:
            return self.stage.at[half, origin, part]
        return self.whole(self.dst, half, *((part, origin) if half == 0 else (origin, part)))

    def copies(self, half, stage):
        axis = (half + stage) % 2
        share = self.share[axis]
        parts = (pl.ds(0, share), pl.ds(share, SIDE - share))
        sizes = (share, SIDE - share)
        every = pl.ds(0, SIDE)
        out = []
        for kind in ("relay", "direct", "forward"):
            for side in range(2):
                step = 1 if side == 0 else -1
                if kind == "direct":
                    src = self.block(half, stage, self.turn(axis, step), every)
                    dst = self.place(half, stage, self.at[axis], every)
                else:
                    hold = self.relay.at[half, stage, side, pl.ds(0, sizes[side])]
                    if kind == "relay":
                        src, dst = self.block(half, stage, self.turn(axis, 2), parts[side]), hold
                    else:
                        src = hold
                        dst = self.place(half, stage, self.turn(axis, -step), parts[side])
                at = (half, stage, len(out))
                out.append(
                    remote(src, dst, self.send.at[at], self.recv.at[at], "gy", self.device(axis, step))
                )
        return out

    def prepare(self):
        x, y = self.at
        self.stage[0, x] = self.src[x, :, : self.rows]
        self.stage[1, y] = self.src[:, y, self.rows :]

    def start(self, stage, half):
        copies = self.copies(half, stage)
        for copy in copies[:4]:
            copy.start()
        if stage == 1:
            self.kept(half).start()

    def forward(self, stage, half):
        copies = self.copies(half, stage)
        for side in range(2):
            copies[side].wait_recv()
            copies[4 + side].start()

    def arrive(self, stage, half):
        for copy in self.copies(half, stage)[2:]:
            copy.wait_recv()

    def kept(self, half):
        axis = (half + 1) % 2
        every = pl.ds(0, SIDE)
        return pltpu.make_async_copy(
            self.block(half, 1, self.at[axis], every),
            self.place(half, 1, self.at[axis], every),
            self.own.at[half],
        )

    def finish(self):
        for half in range(2):
            for stage in range(2):
                for copy in self.copies(half, stage):
                    copy.wait_send()
            self.kept(half).wait()


def gather_kernel(
    corner_in, phase_in, density_in, boxes, places, density,
    corner, phase, matrix, table, low, outbox, stage, relay, half, send, recv, table_send, table_recv,
    y_send, y_recv, x_send, x_recv, own, fetch,
):
    me, row = lax.axis_index("gy"), lax.axis_index("gx")
    columns, rows = lax.axis_size("gy"), lax.axis_size("gx")
    edge = low.shape[0]
    loads = [
        pltpu.make_async_copy(phase_in, phase, fetch.at[0]),
        pltpu.make_async_copy(density_in, matrix, fetch.at[1]),
        pltpu.make_async_copy(corner_in, corner, fetch.at[2]),
    ]
    for load in loads:
        load.start()
    part = edge // 2
    barrier = pltpu.get_barrier_semaphore()
    others = [lax.rem(me + k, columns) for k in range(1, columns)]
    senders = [lax.rem(me + columns - k, columns) for k in range(1, columns)]
    for target in others:
        signal("gy", target)

    @pl.when(row > 0)
    def _():
        signal("gx", row - 1)

    @pl.when(row < rows - 1)
    def _():
        signal("gx", row + 1)

    cells = range(phase.shape[0])
    loads[2].wait()
    home = [lax.div(corner[1, c], edge) for c in cells]
    lane = lax.broadcasted_iota(jnp.int32, table.shape[1:], 1)
    loads[0].wait()

    def fill(s, carry):
        source, found = jnp.int32(0), jnp.int32(0)
        for c in cells:
            source = jnp.where(home[c] == s, c, source)
            found = jnp.where(home[c] == s, 1, found)
        note = (
            corner[0, source] - row * edge,
            jnp.where(found > 0, corner[1, source] - s * edge, 0),
            corner[2, source],
            found,
        )
        line = jnp.zeros_like(lane)
        for k, value in enumerate(note):
            line = jnp.where(lane == k, value, line)
        table[s] = line
        outbox[s // SIDE, lax.rem(s, SIDE)] = phase[source]
        return carry

    lax.fori_loop(0, columns, fill, 0)
    loads[1].wait()
    low[...] = jnp.swapaxes(matrix[...], 0, 1).astype(low.dtype)

    @pl.when(me == columns - 1)
    def _():
        half[...] = jnp.zeros_like(half)

    boxes_out = Exchange(outbox, boxes, stage, relay, send, recv, own, 3)
    boxes_out.prepare()

    neighbours = (row > 0).astype(jnp.int32) + (row < rows - 1).astype(jnp.int32)
    pl.semaphore_wait(barrier, columns - 1 + neighbours)

    def along_y(k):
        rest = pl.ds(k * part, part)
        return remote(low.at[rest], half.at[rest], y_send.at[k], y_recv.at[k], "gy", me - 1)

    def along_x(k):
        src = low if k == 2 else half.at[pl.ds(k * part, part)]
        rest = pl.ds(0, edge) if k == 2 else pl.ds(edge + k * part, part)
        dst = density.at[rest, pl.ds(edge, edge)]
        return remote(src, dst, x_send.at[k], x_recv.at[k], "gx", row - 1)

    def keep(k):
        src = low if k == 2 else half.at[pl.ds(k * part, part)]
        rest = pl.ds(0, edge) if k == 2 else pl.ds(edge + k * part, part)
        return pltpu.make_async_copy(src, density.at[rest, pl.ds(0, edge)], own.at[2 + k])

    def start_y(k):
        @pl.when(me > 0)
        def _():
            along_y(k).start()

    def start_x(k):
        keep(k).start()

        @pl.when(row > 0)
        def _():
            along_x(k).start()

    def take_y(k):
        @pl.when(me < columns - 1)
        def _():
            along_y(k).wait_recv()

    for h in range(2):
        boxes_out.start(0, h)
    start_x(2)
    notes = [
        remote(table.at[target], places.at[me], table_send.at[k], table_recv.at[k], "gy", target)
        for k, target in enumerate(others)
    ]
    for note in notes:
        note.start()
    note = pltpu.make_async_copy(table.at[me], places.at[me], own.at[5])
    note.start()
    for h in range(2):
        boxes_out.forward(0, h)
    start_y(0)
    start_y(1)
    for h in range(2):
        boxes_out.arrive(0, h)
        boxes_out.start(1, h)
    take_y(0)
    start_x(0)
    for h in range(2):
        boxes_out.forward(1, h)
    take_y(1)
    start_x(1)
    for h in range(2):
        boxes_out.arrive(1, h)
    for k, sender in enumerate(senders):
        remote(
            table.at[me], places.at[sender], table_send.at[k], table_recv.at[k], "gy", sender
        ).wait_recv()
    for copy in notes:
        copy.wait_send()
    note.wait()
    for k in range(3):
        keep(k).wait()

        @pl.when(row > 0)
        def _():
            along_x(k).wait_send()

        @pl.when(row < rows - 1)
        def _():
            along_x(k).wait_recv()

    for k in range(2):

        @pl.when(me > 0)
        def _():
            along_y(k).wait_send()

    boxes_out.finish()


def rim_kernel(
    own, crowd, from_x, full, from_y, done, back,
    x_send, x_recv, y_send, y_recv, b_send, b_recv,
):
    me, row = lax.axis_index("gy"), lax.axis_index("gx")
    columns, rows = lax.axis_size("gy"), lax.axis_size("gx")
    edge = own.shape[1] // 2
    chunks, _, part, _ = full.shape
    count = 0
    for axis, at, size in (("gx", row, rows), ("gy", me, columns)):
        for there, target in ((at > 0, at - 1), (at < size - 1, at + 1)):
            count += there.astype(jnp.int32)

            @pl.when(there)
            def _():
                signal(axis, target)

    pl.semaphore_wait(pltpu.get_barrier_semaphore(), count)
    low, high = slice(0, edge), slice(edge, 2 * edge)
    ups = ((me < columns - 1, me > 0, me + 1, high, low), (me > 0, me < columns - 1, me - 1, low, high))

    def spill(c):
        src = own.at[:, pl.ds(edge + c * part, part)]
        return remote(src, from_x.at[c], x_send.at[c], x_recv.at[c], "gx", row + 1)

    def exchange(c, k):
        _, _, target, sent, _ = ups[k]
        return remote(
            full.at[c, sent], from_y.at[k, c], y_send.at[k, c], y_recv.at[k, c], "gy", target
        )

    def give(c):
        return remote(done.at[c], back.at[c], b_send.at[c], b_recv.at[c], "gx", row - 1)

    @pl.when(row < rows - 1)
    def _():
        for c in range(chunks):
            spill(c).start()

    for c in range(chunks):
        mine = slice(c * part, (c + 1) * part)

        @pl.when(row > 0)
        def _():
            spill(c).wait_recv()
            full[c] = own[:, mine] + from_x[c]

        @pl.when(row == 0)
        def _():
            full[c] = own[:, mine]

        for k in range(2):

            @pl.when(ups[k][0])
            def _():
                exchange(c, k).start()

    for c in range(chunks):
        for k in range(2):
            _, takes, _, _, into = ups[k]

            @pl.when(takes)
            def _():
                exchange(c, k).wait_recv()
                done[c, into] = full[c, into] + from_y[k, c]

            @pl.when(jnp.logical_not(takes))
            def _():
                done[c, into] = full[c, into]

        @pl.when(row > 0)
        def _():
            give(c).start()

        crowd[:, c * part : (c + 1) * part] = done[c].astype(jnp.float32)

    @pl.when(row == rows - 1)
    def _():
        crowd[:, edge:] = jnp.zeros((crowd.shape[0], edge, crowd.shape[2]), jnp.float32)

    @pl.when(row < rows - 1)
    def _():
        for c in range(chunks):
            give(c).wait_recv()
            crowd[:, edge + c * part : edge + (c + 1) * part] = back[c].astype(jnp.float32)

    for c in range(chunks):

        @pl.when(row < rows - 1)
        def _():
            spill(c).wait_send()

        for k in range(2):

            @pl.when(ups[k][0])
            def _():
                exchange(c, k).wait_send()

        @pl.when(row > 0)
        def _():
            give(c).wait_send()


def return_kernel(
    settled, wide, returned, deposit, stage, relay, from_x, outgoing, from_y,
    send, recv, x_send, x_recv, y_send, y_recv, own,
):
    me, row = lax.axis_index("gy"), lax.axis_index("gx")
    columns, rows = lax.axis_size("gy"), lax.axis_size("gx")
    edge = wide.shape[1] // 2
    count = greet()
    boxes_back = Exchange(settled, returned, stage, relay, send, recv, own, 1)
    boxes_back.prepare()
    pl.semaphore_wait(pltpu.get_barrier_semaphore(), count)
    halves = (slice(edge, 2 * edge), slice(0, edge))

    def along_x(k):
        return remote(
            wide.at[halves[k], pl.ds(edge, edge)], from_x.at[k], x_send.at[k], x_recv.at[k], "gx", row + 1
        )

    for h in range(2):
        boxes_back.start(0, h)

    @pl.when(row < rows - 1)
    def _():
        for k in range(2):
            along_x(k).start()

    for h in range(2):
        boxes_back.forward(0, h)

    @pl.when(row > 0)
    def _():
        along_x(0).wait_recv()
        outgoing[...] = wide[edge:, :edge] + from_x[0]

    @pl.when(row == 0)
    def _():
        outgoing[...] = wide[edge:, :edge]

    part = edge // 2

    def along_y(k):
        rest = pl.ds(k * part, part)
        return remote(
            outgoing.at[rest], from_y.at[rest], y_send.at[k], y_recv.at[k], "gy", me + 1
        )

    @pl.when(me < columns - 1)
    def _():
        for k in range(2):
            along_y(k).start()

    for h in range(2):
        boxes_back.arrive(0, h)
        boxes_back.start(1, h)

    @pl.when(row > 0)
    def _():
        along_x(1).wait_recv()
        deposit[...] = wide[:edge, :edge].astype(jnp.float32) + from_x[1].astype(jnp.float32)

    @pl.when(row == 0)
    def _():
        deposit[...] = wide[:edge, :edge].astype(jnp.float32)

    for h in range(2):
        boxes_back.forward(1, h)

    @pl.when(me > 0)
    def _():
        for k in range(2):
            along_y(k).wait_recv()
        deposit[...] = deposit[...] + from_y[...].astype(jnp.float32)

    for h in range(2):
        boxes_back.arrive(1, h)

    boxes_back.finish()

    @pl.when(me < columns - 1)
    def _():
        for k in range(2):
            along_y(k).wait_send()

    @pl.when(row < rows - 1)
    def _():
        for k in range(2):
            along_x(k).wait_send()


def fetch_places(table, places, sem):
    copy = pltpu.make_async_copy(table.at[:, 0], places, sem)
    copy.start()
    copy.wait()


def spread_base(base):
    row = lax.broadcasted_iota(jnp.int32, base.shape, 0)
    lane = lax.broadcasted_iota(jnp.int32, base.shape, 1)
    base[...] = jnp.where(row // LANES == lane // B, lax.rem(row, LANES) - lax.rem(lane, B), -1)


def stacked(boxes, s, here):
    v = jnp.concatenate(
        [boxes[s, :, j * LANES : (j + 1) * LANES] for j in range(B // GROUP)], 0
    )
    return jnp.where(here, v, jnp.zeros_like(v))


def add_box(wide, v, spread, lx, ly):
    placed = lax.dot_general(
        v, spread, (((1,), (1,)), ((), ())), preferred_element_type=jnp.float32
    )
    for j in range(B // GROUP):
        for i in range(GROUP):
            at = (ly + (GROUP * j + i), pl.ds(lx, B), slice(None))
            wide[at] = wide[at] + placed[j * B : (j + 1) * B, i * LANES : (i + 1) * LANES]


def take_box(field, spread, lx, ly):
    rows = []
    for j in range(B // GROUP):
        parts = [field[ly + (GROUP * j + i), pl.ds(lx, B), :] for i in range(GROUP)]
        rows.append(jnp.concatenate([p.astype(jnp.bfloat16) for p in parts], 1))
    return jnp.dot(jnp.concatenate(rows, 0), spread, preferred_element_type=jnp.float32)


def crowd_kernel(table, boxes, out, wide, base, places, sem):
    fetch_places(table, places, sem)
    wide[...] = jnp.zeros_like(wide)
    spread_base(base)

    def one(t, carry):
        slots = [t * TOGETHER + k for k in range(TOGETHER)]

        @pl.when(sum(places[s, 3] for s in slots) > 0)
        def _():
            squares, spreads = [], []
            for s in slots:
                v = stacked(boxes, s, places[s, 3] > 0).astype(jnp.float32)
                squares.append((v * v).astype(jnp.bfloat16))
                spreads.append(jnp.where(base[...] == places[s, 2], 1.0, 0.0).astype(jnp.bfloat16))
            for s, square, spread in zip(slots, squares, spreads):
                add_box(wide, square, spread, places[s, 0], places[s, 1])

        return carry

    lax.fori_loop(0, boxes.shape[0] // TOGETHER, one, 0)
    out[...] = wide[...].astype(out.dtype)


def update_kernel(
    table, boxes, crowd, low, settled, out, density, wide, base, taps, places, sem
):
    fetch_places(table, places, sem)
    density[...] = low[...].astype(jnp.float32)
    wide[...] = jnp.zeros_like(wide)
    spread_base(base)
    from_b = lax.broadcasted_iota(jnp.int32, taps.shape, 0) - LANES
    to_b = lax.broadcasted_iota(jnp.int32, taps.shape, 1)
    gap = from_b - to_b
    beside = (gap == B) | (gap == -B)
    same = (from_b >= 0) & (from_b < LANES) & (lax.rem(from_b + LANES, LANES) // B == to_b // B)
    along = same & ((gap == 1) | (gap == -1))
    taps[...] = jnp.where(gap == 0, -6.0, jnp.where(beside | along, 1.0, 0.0)).astype(taps.dtype)
    step = lax.rem(lax.broadcasted_iota(jnp.int32, (B * B // GROUP, LANES), 0), B)
    edge = jnp.zeros((B, LANES), jnp.bfloat16)
    total = B * B // GROUP

    def one(t, carry):
        slots = [t * TOGETHER + k for k in range(TOGETHER)]
        busy = sum(places[s, 3] for s in slots) > 0

        @pl.when(busy)
        def _():
            spreads, results = [], []
            for s in slots:
                lx, ly, lz = places[s, 0], places[s, 1], places[s, 2]
                spread = jnp.where(base[...] == lz, 1.0, 0.0).astype(jnp.bfloat16)
                cr = take_box(crowd, spread, lx, ly)
                dn = take_box(density, spread, lx, ly)
                v = stacked(boxes, s, places[s, 3] > 0)
                near = jnp.concatenate(
                    [
                        jnp.concatenate([edge, v[: total - B]], 0),
                        v,
                        jnp.concatenate([v[B:], edge], 0),
                    ],
                    1,
                )
                lap = jnp.dot(near, taps[...], preferred_element_type=jnp.float32)
                p = v.astype(jnp.float32)
                across = jnp.where(step < B - 1, pltpu.roll(p, total - 1, 0), 0.0) + jnp.where(
                    step > 0, pltpu.roll(p, 1, 0), 0.0
                )
                others = cr - p * p
                reaction = 4.0 * p * (1.0 - p) * (p - 0.5 + (dn - 0.5))
                fresh = p + 0.1 * (lap + across + reaction - 2.0 * p * others)
                fresh = fresh.astype(jnp.bfloat16)
                for j in range(B // GROUP):
                    settled[s, :, j * LANES : (j + 1) * LANES] = fresh[j * B : (j + 1) * B]
                spreads.append(spread)
                results.append(fresh)
            for s, fresh, spread in zip(slots, results, spreads):
                add_box(wide, fresh, spread, places[s, 0], places[s, 1])

        @pl.when(jnp.logical_not(busy))
        def _():
            for s in slots:
                settled[s] = jnp.zeros(settled.shape[1:], settled.dtype)

        return carry

    lax.fori_loop(0, boxes.shape[0] // TOGETHER, one, 0)
    out[...] = wide[...].astype(out.dtype)


def finish_kernel(
    corner_in, returned, deposit, matrix, phase_next, matrix_next, corner, turned, sem, fetch
):
    edge = matrix.shape[1]
    load = pltpu.make_async_copy(corner_in, corner, fetch.at[0])
    load.start()
    now = matrix[...]
    turned[...] = now - 0.5 * now * jnp.swapaxes(deposit[...], 0, 1)
    store = pltpu.make_async_copy(turned, matrix_next, fetch.at[1])
    store.start()
    load.wait()
    copies = [
        pltpu.make_async_copy(
            returned.at[lax.div(corner[1, c], edge)], phase_next.at[c], sem.at[c]
        )
        for c in range(phase_next.shape[0])
    ]
    for copy in copies:
        copy.start()
    store.wait()
    for copy in copies:
        copy.wait()


VMEM = pl.BlockSpec(memory_space=pltpu.VMEM)
ANY = pl.BlockSpec(memory_space=pl.ANY)
HBM = pl.BlockSpec(memory_space=pltpu.HBM)
LIMIT = 24 * 2**20


def like(shape, dtype):
    return jax.ShapeDtypeStruct(shape, dtype)


def dma(*shape):
    return pltpu.SemaphoreType.DMA(shape)


def linked(number):
    return pltpu.CompilerParams(
        collective_id=number, has_side_effects=True, vmem_limit_bytes=LIMIT
    )


def per_device(phase_box, matrix_density, box_corner):
    slab_rows, slab_cols, grid_depth = matrix_density.shape
    peers = lax.axis_size("gy")
    bf16, f32 = jnp.bfloat16, jnp.float32
    slots = (peers,) + phase_box.shape[1:]
    notes = (peers, 8, LANES)
    torus = (SIDE, SIDE) + phase_box.shape[1:]
    rows = (phase_box.shape[1] // 2,) + phase_box.shape[2:]
    moving = [pltpu.VMEM((2, SIDE, SIDE) + rows, bf16), pltpu.VMEM((2, 2, 2, SIDE - 1) + rows, bf16)]
    wide = (2 * slab_cols, 2 * slab_rows, grid_depth)
    strips = (RIM_CHUNKS, 2 * slab_cols, slab_rows // RIM_CHUNKS, grid_depth)
    quarter = (slab_cols, slab_rows, grid_depth)
    boxes, places, density = pl.pallas_call(
        gather_kernel,
        out_shape=(like(torus, bf16), like(notes, jnp.int32), like(wide, bf16)),
        in_specs=[HBM, HBM, HBM],
        out_specs=(ANY, ANY, ANY),
        scratch_shapes=[
            pltpu.SMEM(box_corner.shape, jnp.int32),
            pltpu.VMEM(phase_box.shape, bf16),
            pltpu.VMEM(matrix_density.shape, f32),
            pltpu.VMEM(notes, jnp.int32),
            pltpu.VMEM(quarter, bf16),
            pltpu.VMEM(torus, bf16),
        ]
        + moving
        + [
            pltpu.VMEM(quarter, bf16),
            dma(2, 2, 6), dma(2, 2, 6), dma(peers - 1), dma(peers - 1),
            dma(2), dma(2), dma(3), dma(3), dma(6), dma(3),
        ],
        compiler_params=linked(0),
        name="gather",
    )(
        *(pltpu.with_memory_space_constraint(a, pltpu.HBM) for a in (box_corner, phase_box, matrix_density))
    )
    boxes = boxes.reshape(slots)

    spread = pltpu.VMEM((GROUP * LANES, LANES), jnp.int32)
    taps = pltpu.VMEM((3 * LANES, LANES), bf16)
    spots = [pltpu.SMEM((peers, LANES), jnp.int32), dma()]
    quiet = pltpu.CompilerParams(vmem_limit_bytes=LIMIT)
    crowd = pl.pallas_call(
        crowd_kernel,
        out_shape=like(wide, bf16),
        in_specs=[ANY, VMEM],
        out_specs=VMEM,
        scratch_shapes=[pltpu.VMEM(wide, f32), spread] + spots,
        compiler_params=quiet,
        name="crowd",
    )(places, boxes)

    crowd = pl.pallas_call(
        rim_kernel,
        out_shape=like(wide, f32),
        in_specs=[VMEM],
        out_specs=VMEM,
        scratch_shapes=[
            pltpu.VMEM(strips, bf16),
            pltpu.VMEM(strips, bf16),
            pltpu.VMEM((2, RIM_CHUNKS, slab_cols) + strips[2:], bf16),
            pltpu.VMEM(strips, bf16),
            pltpu.VMEM(strips, bf16),
            dma(RIM_CHUNKS), dma(RIM_CHUNKS), dma(2, RIM_CHUNKS), dma(2, RIM_CHUNKS),
            dma(RIM_CHUNKS), dma(RIM_CHUNKS),
        ],
        compiler_params=linked(1),
        name="rim",
    )(crowd)

    settled, deposit = pl.pallas_call(
        update_kernel,
        out_shape=(like(slots, bf16), like(wide, bf16)),
        in_specs=[ANY, VMEM, VMEM, VMEM],
        out_specs=(VMEM, VMEM),
        scratch_shapes=[pltpu.VMEM(wide, f32), pltpu.VMEM(wide, f32), spread, taps] + spots,
        compiler_params=quiet,
        name="update",
    )(places, boxes, crowd, density)

    returned, deposit = pl.pallas_call(
        return_kernel,
        out_shape=(like(torus, bf16), like(quarter, f32)),
        in_specs=[VMEM, VMEM],
        out_specs=(ANY, VMEM),
        scratch_shapes=moving
        + [
            pltpu.VMEM((2,) + quarter, bf16),
            pltpu.VMEM(quarter, bf16),
            pltpu.VMEM(quarter, bf16),
            dma(2, 2, 6), dma(2, 2, 6), dma(2), dma(2), dma(2), dma(2), dma(2),
        ],
        compiler_params=linked(2),
        name="return",
    )(settled.reshape(torus), deposit)
    returned = returned.reshape(slots)

    return pl.pallas_call(
        finish_kernel,
        out_shape=(like(phase_box.shape, bf16), like(matrix_density.shape, f32)),
        in_specs=[HBM, VMEM, VMEM, VMEM],
        out_specs=(ANY, ANY),
        scratch_shapes=[
            pltpu.SMEM(box_corner.shape, jnp.int32),
            pltpu.VMEM(matrix_density.shape, f32),
            dma(phase_box.shape[0]),
            dma(2),
        ],
        compiler_params=quiet,
        name="finish",
    )(
        pltpu.with_memory_space_constraint(box_corner, pltpu.HBM), returned, deposit, matrix_density
    )


def solution(mesh):
    return jax.shard_map(
        per_device,
        mesh=mesh,
        in_specs=(P(("gx", "gy"), None, None), P("gx", "gy", None), P(None, ("gx", "gy"))),
        out_specs=(P(("gx", "gy"), None, None), P("gx", "gy", None)),
        check_vma=False,
    )
```

```python
import jax
import jax.numpy as jnp
from jax import lax
from jax.experimental import pallas as pl
from jax.experimental.pallas import tpu as pltpu
from jax.sharding import PartitionSpec as P

B = 32
LANES = 128
GROUP = LANES // B
SIDE = 4
TOGETHER = 4
RIM_CHUNKS = 4

def signal(axis, target):
    pl.semaphore_signal(
        pltpu.get_barrier_semaphore(),
        inc=1,
        device_id={axis: target},
        device_id_type=pl.DeviceIdType.MESH,
    )


def remote(src, dst, send, recv, axis, target):
    return pltpu.make_async_remote_copy(
        src_ref=src,
        dst_ref=dst,
        send_sem=send,
        recv_sem=recv,
        device_id={axis: target},
        device_id_type=pl.DeviceIdType.MESH,
    )


def greet():
    me, row = lax.axis_index("gy"), lax.axis_index("gx")
    columns, rows = lax.axis_size("gy"), lax.axis_size("gx")
    high, low = me // SIDE, lax.rem(me, SIDE)
    count = 0
    for step in (1, SIDE - 1):
        signal("gy", lax.rem(high + step, SIDE) * SIDE + low)
        signal("gy", high * SIDE + lax.rem(low + step, SIDE))
        count += 2
    for axis, at, size, step in (("gx", row, rows, 1), ("gx", row, rows, -1)):
        there = (at < size - 1) if step > 0 else (at > 0)
        count += there.astype(jnp.int32)

        @pl.when(there)
        def _():
            signal(axis, at + step)

    for step in (1, -1):
        far = (low == (SIDE - 1 if step > 0 else 0)) & (
            (me < columns - 1) if step > 0 else (me > 0)
        )
        count += far.astype(jnp.int32)

        @pl.when(far)
        def _():
            signal("gy", me + step)

    return count


class Exchange:
    def __init__(self, src, dst, stage, relay, send, recv, own, share_y):
        self.src, self.dst, self.stage, self.relay = src, dst, stage, relay
        self.send, self.recv, self.own = send, recv, own
        me = lax.axis_index("gy")
        self.at = (me // SIDE, lax.rem(me, SIDE))
        self.share = (SIDE // 2, share_y)
        self.rows = src.shape[2] // 2

    def turn(self, axis, step):
        return lax.rem(self.at[axis] + SIDE + step, SIDE)

    def device(self, axis, step):
        other, moved = self.at[1 - axis], self.turn(axis, step)
        return moved * SIDE + other if axis == 0 else other * SIDE + moved

    def whole(self, ref, half, first, second):
        rest = pl.ds(half * self.rows, self.rows)
        return ref.at[first, second, rest]

    def block(self, half, stage, goal, part):
        if stage == 1:
            return self.stage.at[half, part, goal]
        return self.whole(self.src, half, *((goal, part) if half == 0 else (part, goal)))

    def place(self, half, stage, origin, part):
        if stage == 0:
            return self.stage.at[half, origin, part]
        return self.whole(self.dst, half, *((part, origin) if half == 0 else (origin, part)))

    def copies(self, half, stage):
        axis = (half + stage) % 2
        share = self.share[axis]
        parts = (pl.ds(0, share), pl.ds(share, SIDE - share))
        sizes = (share, SIDE - share)
        every = pl.ds(0, SIDE)
        out = []
        for kind in ("relay", "direct", "forward"):
            for side in range(2):
                step = 1 if side == 0 else -1
                if kind == "direct":
                    src = self.block(half, stage, self.turn(axis, step), every)
                    dst = self.place(half, stage, self.at[axis], every)
                else:
                    hold = self.relay.at[half, stage, side, pl.ds(0, sizes[side])]
                    if kind == "relay":
                        src, dst = self.block(half, stage, self.turn(axis, 2), parts[side]), hold
                    else:
                        src = hold
                        dst = self.place(half, stage, self.turn(axis, -step), parts[side])
                at = (half, stage, len(out))
                out.append(
                    remote(src, dst, self.send.at[at], self.recv.at[at], "gy", self.device(axis, step))
                )
        return out

    def prepare(self):
        x, y = self.at
        self.stage[0, x] = self.src[x, :, : self.rows]
        self.stage[1, y] = self.src[:, y, self.rows :]

    def start(self, stage, half):
        copies = self.copies(half, stage)
        for copy in copies[:4]:
            copy.start()
        if stage == 1:
            self.kept(half).start()

    def forward(self, stage, half):
        copies = self.copies(half, stage)
        for side in range(2):
            copies[side].wait_recv()
            copies[4 + side].start()

    def arrive(self, stage, half):
        for copy in self.copies(half, stage)[2:]:
            copy.wait_recv()

    def kept(self, half):
        axis = (half + 1) % 2
        every = pl.ds(0, SIDE)
        return pltpu.make_async_copy(
            self.block(half, 1, self.at[axis], every),
            self.place(half, 1, self.at[axis], every),
            self.own.at[half],
        )

    def finish(self):
        for half in range(2):
            for stage in range(2):
                for copy in self.copies(half, stage):
                    copy.wait_send()
            self.kept(half).wait()


def gather_kernel(
    corner_in, phase_in, density_in, boxes, places, density,
    corner, phase, matrix, table, low, outbox, stage, relay, half, send, recv, table_send, table_recv,
    y_send, y_recv, x_send, x_recv, own, fetch,
):
    me, row = lax.axis_index("gy"), lax.axis_index("gx")
    columns, rows = lax.axis_size("gy"), lax.axis_size("gx")
    edge = low.shape[0]
    loads = [
        pltpu.make_async_copy(phase_in, phase, fetch.at[0]),
        pltpu.make_async_copy(density_in, matrix, fetch.at[1]),
        pltpu.make_async_copy(corner_in, corner, fetch.at[2]),
    ]
    for load in loads:
        load.start()
    part = edge // 2
    barrier = pltpu.get_barrier_semaphore()
    others = [lax.rem(me + k, columns) for k in range(1, columns)]
    senders = [lax.rem(me + columns - k, columns) for k in range(1, columns)]
    for target in others:
        signal("gy", target)

    @pl.when(row > 0)
    def _():
        signal("gx", row - 1)

    @pl.when(row < rows - 1)
    def _():
        signal("gx", row + 1)

    cells = range(phase.shape[0])
    loads[2].wait()
    home = [lax.div(corner[1, c], edge) for c in cells]
    lane = lax.broadcasted_iota(jnp.int32, table.shape[1:], 1)
    loads[0].wait()

    def fill(s, carry):
        source, found = jnp.int32(0), jnp.int32(0)
        for c in cells:
            source = jnp.where(home[c] == s, c, source)
            found = jnp.where(home[c] == s, 1, found)
        note = (
            corner[0, source] - row * edge,
            jnp.where(found > 0, corner[1, source] - s * edge, 0),
            corner[2, source],
            found,
        )
        line = jnp.zeros_like(lane)
        for k, value in enumerate(note):
            line = jnp.where(lane == k, value, line)
        table[s] = line
        outbox[s // SIDE, lax.rem(s, SIDE)] = phase[source]
        return carry

    lax.fori_loop(0, columns, fill, 0)
    loads[1].wait()
    low[...] = jnp.swapaxes(matrix[...], 0, 1).astype(low.dtype)

    @pl.when(me == columns - 1)
    def _():
        half[...] = jnp.zeros_like(half)

    boxes_out = Exchange(outbox, boxes, stage, relay, send, recv, own, 3)
    boxes_out.prepare()

    neighbours = (row > 0).astype(jnp.int32) + (row < rows - 1).astype(jnp.int32)
    pl.semaphore_wait(barrier, columns - 1 + neighbours)

    def along_y(k):
        rest = pl.ds(k * part, part)
        return remote(low.at[rest], half.at[rest], y_send.at[k], y_recv.at[k], "gy", me - 1)

    def along_x(k):
        src = low if k == 2 else half.at[pl.ds(k * part, part)]
        rest = pl.ds(0, edge) if k == 2 else pl.ds(edge + k * part, part)
        dst = density.at[rest, pl.ds(edge, edge)]
        return remote(src, dst, x_send.at[k], x_recv.at[k], "gx", row - 1)

    def keep(k):
        src = low if k == 2 else half.at[pl.ds(k * part, part)]
        rest = pl.ds(0, edge) if k == 2 else pl.ds(edge + k * part, part)
        return pltpu.make_async_copy(src, density.at[rest, pl.ds(0, edge)], own.at[2 + k])

    def start_y(k):
        @pl.when(me > 0)
        def _():
            along_y(k).start()

    def start_x(k):
        keep(k).start()

        @pl.when(row > 0)
        def _():
            along_x(k).start()

    def take_y(k):
        @pl.when(me < columns - 1)
        def _():
            along_y(k).wait_recv()

    for h in range(2):
        boxes_out.start(0, h)
    start_x(2)
    notes = [
        remote(table.at[target], places.at[me], table_send.at[k], table_recv.at[k], "gy", target)
        for k, target in enumerate(others)
    ]
    for note in notes:
        note.start()
    note = pltpu.make_async_copy(table.at[me], places.at[me], own.at[5])
    note.start()
    for h in range(2):
        boxes_out.forward(0, h)
    start_y(0)
    start_y(1)
    for h in range(2):
        boxes_out.arrive(0, h)
        boxes_out.start(1, h)
    take_y(0)
    start_x(0)
    for h in range(2):
        boxes_out.forward(1, h)
    take_y(1)
    start_x(1)
    for h in range(2):
        boxes_out.arrive(1, h)
    for k, sender in enumerate(senders):
        remote(
            table.at[me], places.at[sender], table_send.at[k], table_recv.at[k], "gy", sender
        ).wait_recv()
    for copy in notes:
        copy.wait_send()
    note.wait()
    for k in range(3):
        keep(k).wait()

        @pl.when(row > 0)
        def _():
            along_x(k).wait_send()

        @pl.when(row < rows - 1)
        def _():
            along_x(k).wait_recv()

    for k in range(2):

        @pl.when(me > 0)
        def _():
            along_y(k).wait_send()

    boxes_out.finish()


def rim_kernel(
    own, crowd, from_x, full, from_y, done, back,
    x_send, x_recv, y_send, y_recv, b_send, b_recv,
):
    me, row = lax.axis_index("gy"), lax.axis_index("gx")
    columns, rows = lax.axis_size("gy"), lax.axis_size("gx")
    edge = own.shape[1] // 2
    chunks, _, part, _ = full.shape
    count = 0
    for axis, at, size in (("gx", row, rows), ("gy", me, columns)):
        for there, target in ((at > 0, at - 1), (at < size - 1, at + 1)):
            count += there.astype(jnp.int32)

            @pl.when(there)
            def _():
                signal(axis, target)

    pl.semaphore_wait(pltpu.get_barrier_semaphore(), count)
    low, high = slice(0, edge), slice(edge, 2 * edge)
    ups = ((me < columns - 1, me > 0, me + 1, high, low), (me > 0, me < columns - 1, me - 1, low, high))

    def spill(c):
        src = own.at[:, pl.ds(edge + c * part, part)]
        return remote(src, from_x.at[c], x_send.at[c], x_recv.at[c], "gx", row + 1)

    def exchange(c, k):
        _, _, target, sent, _ = ups[k]
        return remote(
            full.at[c, sent], from_y.at[k, c], y_send.at[k, c], y_recv.at[k, c], "gy", target
        )

    def give(c):
        return remote(done.at[c], back.at[c], b_send.at[c], b_recv.at[c], "gx", row - 1)

    @pl.when(row < rows - 1)
    def _():
        for c in range(chunks):
            spill(c).start()

    for c in range(chunks):
        mine = slice(c * part, (c + 1) * part)

        @pl.when(row > 0)
        def _():
            spill(c).wait_recv()
            full[c] = own[:, mine] + from_x[c]

        @pl.when(row == 0)
        def _():
            full[c] = own[:, mine]

        for k in range(2):

            @pl.when(ups[k][0])
            def _():
                exchange(c, k).start()

    for c in range(chunks):
        for k in range(2):
            _, takes, _, _, into = ups[k]

            @pl.when(takes)
            def _():
                exchange(c, k).wait_recv()
                done[c, into] = full[c, into] + from_y[k, c]

            @pl.when(jnp.logical_not(takes))
            def _():
                done[c, into] = full[c, into]

        @pl.when(row > 0)
        def _():
            give(c).start()

        crowd[:, c * part : (c + 1) * part] = done[c].astype(jnp.float32)

    @pl.when(row == rows - 1)
    def _():
        crowd[:, edge:] = jnp.zeros((crowd.shape[0], edge, crowd.shape[2]), jnp.float32)

    @pl.when(row < rows - 1)
    def _():
        for c in range(chunks):
            give(c).wait_recv()
            crowd[:, edge + c * part : edge + (c + 1) * part] = back[c].astype(jnp.float32)

    for c in range(chunks):

        @pl.when(row < rows - 1)
        def _():
            spill(c).wait_send()

        for k in range(2):

            @pl.when(ups[k][0])
            def _():
                exchange(c, k).wait_send()

        @pl.when(row > 0)
        def _():
            give(c).wait_send()


def return_kernel(
    settled, wide, returned, deposit, stage, relay, from_x, outgoing, from_y,
    send, recv, x_send, x_recv, y_send, y_recv, own,
):
    me, row = lax.axis_index("gy"), lax.axis_index("gx")
    columns, rows = lax.axis_size("gy"), lax.axis_size("gx")
    edge = wide.shape[1] // 2
    count = greet()
    boxes_back = Exchange(settled, returned, stage, relay, send, recv, own, 1)
    boxes_back.prepare()
    pl.semaphore_wait(pltpu.get_barrier_semaphore(), count)
    halves = (slice(edge, 2 * edge), slice(0, edge))

    def along_x(k):
        return remote(
            wide.at[halves[k], pl.ds(edge, edge)], from_x.at[k], x_send.at[k], x_recv.at[k], "gx", row + 1
        )

    for h in range(2):
        boxes_back.start(0, h)

    @pl.when(row < rows - 1)
    def _():
        for k in range(2):
            along_x(k).start()

    for h in range(2):
        boxes_back.forward(0, h)

    @pl.when(row > 0)
    def _():
        along_x(0).wait_recv()
        outgoing[...] = wide[edge:, :edge] + from_x[0]

    @pl.when(row == 0)
    def _():
        outgoing[...] = wide[edge:, :edge]

    part = edge // 2

    def along_y(k):
        rest = pl.ds(k * part, part)
        return remote(
            outgoing.at[rest], from_y.at[rest], y_send.at[k], y_recv.at[k], "gy", me + 1
        )

    @pl.when(me < columns - 1)
    def _():
        for k in range(2):
            along_y(k).start()

    for h in range(2):
        boxes_back.arrive(0, h)
        boxes_back.start(1, h)

    @pl.when(row > 0)
    def _():
        along_x(1).wait_recv()
        deposit[...] = wide[:edge, :edge].astype(jnp.float32) + from_x[1].astype(jnp.float32)

    @pl.when(row == 0)
    def _():
        deposit[...] = wide[:edge, :edge].astype(jnp.float32)

    for h in range(2):
        boxes_back.forward(1, h)

    @pl.when(me > 0)
    def _():
        for k in range(2):
            along_y(k).wait_recv()
        deposit[...] = deposit[...] + from_y[...].astype(jnp.float32)

    for h in range(2):
        boxes_back.arrive(1, h)

    boxes_back.finish()

    @pl.when(me < columns - 1)
    def _():
        for k in range(2):
            along_y(k).wait_send()

    @pl.when(row < rows - 1)
    def _():
        for k in range(2):
            along_x(k).wait_send()


def fetch_places(table, places, sem):
    copy = pltpu.make_async_copy(table.at[:, 0], places, sem)
    copy.start()
    copy.wait()


def spread_base(base):
    row = lax.broadcasted_iota(jnp.int32, base.shape, 0)
    lane = lax.broadcasted_iota(jnp.int32, base.shape, 1)
    base[...] = jnp.where(row // LANES == lane // B, lax.rem(row, LANES) - lax.rem(lane, B), -1)


def stacked(boxes, s, here):
    v = jnp.concatenate(
        [boxes[s, :, j * LANES : (j + 1) * LANES] for j in range(B // GROUP)], 0
    )
    return jnp.where(here, v, jnp.zeros_like(v))


def add_box(wide, v, spread, lx, ly):
    placed = lax.dot_general(
        v, spread, (((1,), (1,)), ((), ())), preferred_element_type=jnp.float32
    )
    for j in range(B // GROUP):
        for i in range(GROUP):
            at = (ly + (GROUP * j + i), pl.ds(lx, B), slice(None))
            wide[at] = wide[at] + placed[j * B : (j + 1) * B, i * LANES : (i + 1) * LANES]


def take_box(field, spread, lx, ly):
    rows = []
    for j in range(B // GROUP):
        parts = [field[ly + (GROUP * j + i), pl.ds(lx, B), :] for i in range(GROUP)]
        rows.append(jnp.concatenate([p.astype(jnp.bfloat16) for p in parts], 1))
    return jnp.dot(jnp.concatenate(rows, 0), spread, preferred_element_type=jnp.float32)


def crowd_kernel(table, boxes, out, wide, base, places, sem):
    fetch_places(table, places, sem)
    wide[...] = jnp.zeros_like(wide)
    spread_base(base)

    def one(t, carry):
        slots = [t * TOGETHER + k for k in range(TOGETHER)]

        @pl.when(sum(places[s, 3] for s in slots) > 0)
        def _():
            squares, spreads = [], []
            for s in slots:
                v = stacked(boxes, s, places[s, 3] > 0).astype(jnp.float32)
                squares.append((v * v).astype(jnp.bfloat16))
                spreads.append(jnp.where(base[...] == places[s, 2], 1.0, 0.0).astype(jnp.bfloat16))
            for s, square, spread in zip(slots, squares, spreads):
                add_box(wide, square, spread, places[s, 0], places[s, 1])

        return carry

    lax.fori_loop(0, boxes.shape[0] // TOGETHER, one, 0)
    out[...] = wide[...].astype(out.dtype)


def update_kernel(
    table, boxes, crowd, low, settled, out, density, wide, base, taps, places, sem
):
    fetch_places(table, places, sem)
    density[...] = low[...].astype(jnp.float32)
    wide[...] = jnp.zeros_like(wide)
    spread_base(base)
    from_b = lax.broadcasted_iota(jnp.int32, taps.shape, 0) - LANES
    to_b = lax.broadcasted_iota(jnp.int32, taps.shape, 1)
    gap = from_b - to_b
    beside = (gap == B) | (gap == -B)
    same = (from_b >= 0) & (from_b < LANES) & (lax.rem(from_b + LANES, LANES) // B == to_b // B)
    along = same & ((gap == 1) | (gap == -1))
    taps[...] = jnp.where(gap == 0, -6.0, jnp.where(beside | along, 1.0, 0.0)).astype(taps.dtype)
    step = lax.rem(lax.broadcasted_iota(jnp.int32, (B * B // GROUP, LANES), 0), B)
    edge = jnp.zeros((B, LANES), jnp.bfloat16)
    total = B * B // GROUP

    def one(t, carry):
        slots = [t * TOGETHER + k for k in range(TOGETHER)]
        busy = sum(places[s, 3] for s in slots) > 0

        @pl.when(busy)
        def _():
            spreads, results = [], []
            for s in slots:
                lx, ly, lz = places[s, 0], places[s, 1], places[s, 2]
                spread = jnp.where(base[...] == lz, 1.0, 0.0).astype(jnp.bfloat16)
                cr = take_box(crowd, spread, lx, ly)
                dn = take_box(density, spread, lx, ly)
                v = stacked(boxes, s, places[s, 3] > 0)
                near = jnp.concatenate(
                    [
                        jnp.concatenate([edge, v[: total - B]], 0),
                        v,
                        jnp.concatenate([v[B:], edge], 0),
                    ],
                    1,
                )
                lap = jnp.dot(near, taps[...], preferred_element_type=jnp.float32)
                p = v.astype(jnp.float32)
                across = jnp.where(step < B - 1, pltpu.roll(p, total - 1, 0), 0.0) + jnp.where(
                    step > 0, pltpu.roll(p, 1, 0), 0.0
                )
                others = cr - p * p
                reaction = 4.0 * p * (1.0 - p) * (p - 0.5 + (dn - 0.5))
                fresh = p + 0.1 * (lap + across + reaction - 2.0 * p * others)
                fresh = fresh.astype(jnp.bfloat16)
                for j in range(B // GROUP):
                    settled[s, :, j * LANES : (j + 1) * LANES] = fresh[j * B : (j + 1) * B]
                spreads.append(spread)
                results.append(fresh)
            for s, fresh, spread in zip(slots, results, spreads):
                add_box(wide, fresh, spread, places[s, 0], places[s, 1])

        @pl.when(jnp.logical_not(busy))
        def _():
            for s in slots:
                settled[s] = jnp.zeros(settled.shape[1:], settled.dtype)

        return carry

    lax.fori_loop(0, boxes.shape[0] // TOGETHER, one, 0)
    out[...] = wide[...].astype(out.dtype)


def finish_kernel(
    corner_in, returned, deposit, matrix, phase_next, matrix_next, corner, turned, sem, fetch
):
    edge = matrix.shape[1]
    load = pltpu.make_async_copy(corner_in, corner, fetch.at[0])
    load.start()
    now = matrix[...]
    turned[...] = now - 0.5 * now * jnp.swapaxes(deposit[...], 0, 1)
    store = pltpu.make_async_copy(turned, matrix_next, fetch.at[1])
    store.start()
    load.wait()
    copies = [
        pltpu.make_async_copy(
            returned.at[lax.div(corner[1, c], edge)], phase_next.at[c], sem.at[c]
        )
        for c in range(phase_next.shape[0])
    ]
    for copy in copies:
        copy.start()
    store.wait()
    for copy in copies:
        copy.wait()


VMEM = pl.BlockSpec(memory_space=pltpu.VMEM)
ANY = pl.BlockSpec(memory_space=pl.ANY)
HBM = pl.BlockSpec(memory_space=pltpu.HBM)
LIMIT = 24 * 2**20


def like(shape, dtype):
    return jax.ShapeDtypeStruct(shape, dtype)


def dma(*shape):
    return pltpu.SemaphoreType.DMA(shape)


def linked(number):
    return pltpu.CompilerParams(
        collective_id=number, has_side_effects=True, vmem_limit_bytes=LIMIT
    )


def per_device(phase_box, matrix_density, box_corner):
    slab_rows, slab_cols, grid_depth = matrix_density.shape
    peers = lax.axis_size("gy")
    bf16, f32 = jnp.bfloat16, jnp.float32
    slots = (peers,) + phase_box.shape[1:]
    notes = (peers, 8, LANES)
    torus = (SIDE, SIDE) + phase_box.shape[1:]
    rows = (phase_box.shape[1] // 2,) + phase_box.shape[2:]
    moving = [pltpu.VMEM((2, SIDE, SIDE) + rows, bf16), pltpu.VMEM((2, 2, 2, SIDE - 1) + rows, bf16)]
    wide = (2 * slab_cols, 2 * slab_rows, grid_depth)
    strips = (RIM_CHUNKS, 2 * slab_cols, slab_rows // RIM_CHUNKS, grid_depth)
    quarter = (slab_cols, slab_rows, grid_depth)
    boxes, places, density = pl.pallas_call(
        gather_kernel,
        out_shape=(like(torus, bf16), like(notes, jnp.int32), like(wide, bf16)),
        in_specs=[HBM, HBM, HBM],
        out_specs=(ANY, ANY, ANY),
        scratch_shapes=[
            pltpu.SMEM(box_corner.shape, jnp.int32),
            pltpu.VMEM(phase_box.shape, bf16),
            pltpu.VMEM(matrix_density.shape, f32),
            pltpu.VMEM(notes, jnp.int32),
            pltpu.VMEM(quarter, bf16),
            pltpu.VMEM(torus, bf16),
        ]
        + moving
        + [
            pltpu.VMEM(quarter, bf16),
            dma(2, 2, 6), dma(2, 2, 6), dma(peers - 1), dma(peers - 1),
            dma(2), dma(2), dma(3), dma(3), dma(6), dma(3),
        ],
        compiler_params=linked(0),
        name="gather",
    )(
        *(pltpu.with_memory_space_constraint(a, pltpu.HBM) for a in (box_corner, phase_box, matrix_density))
    )
    boxes = boxes.reshape(slots)

    spread = pltpu.VMEM((GROUP * LANES, LANES), jnp.int32)
    taps = pltpu.VMEM((3 * LANES, LANES), bf16)
    spots = [pltpu.SMEM((peers, LANES), jnp.int32), dma()]
    quiet = pltpu.CompilerParams(vmem_limit_bytes=LIMIT)
    crowd = pl.pallas_call(
        crowd_kernel,
        out_shape=like(wide, bf16),
        in_specs=[ANY, VMEM],
        out_specs=VMEM,
        scratch_shapes=[pltpu.VMEM(wide, f32), spread] + spots,
        compiler_params=quiet,
        name="crowd",
    )(places, boxes)

    crowd = pl.pallas_call(
        rim_kernel,
        out_shape=like(wide, f32),
        in_specs=[VMEM],
        out_specs=VMEM,
        scratch_shapes=[
            pltpu.VMEM(strips, bf16),
            pltpu.VMEM(strips, bf16),
            pltpu.VMEM((2, RIM_CHUNKS, slab_cols) + strips[2:], bf16),
            pltpu.VMEM(strips, bf16),
            pltpu.VMEM(strips, bf16),
            dma(RIM_CHUNKS), dma(RIM_CHUNKS), dma(2, RIM_CHUNKS), dma(2, RIM_CHUNKS),
            dma(RIM_CHUNKS), dma(RIM_CHUNKS),
        ],
        compiler_params=linked(1),
        name="rim",
    )(crowd)

    settled, deposit = pl.pallas_call(
        update_kernel,
        out_shape=(like(slots, bf16), like(wide, bf16)),
        in_specs=[ANY, VMEM, VMEM, VMEM],
        out_specs=(VMEM, VMEM),
        scratch_shapes=[pltpu.VMEM(wide, f32), pltpu.VMEM(wide, f32), spread, taps] + spots,
        compiler_params=quiet,
        name="update",
    )(places, boxes, crowd, density)

    returned, deposit = pl.pallas_call(
        return_kernel,
        out_shape=(like(torus, bf16), like(quarter, f32)),
        in_specs=[VMEM, VMEM],
        out_specs=(ANY, VMEM),
        scratch_shapes=moving
        + [
            pltpu.VMEM((2,) + quarter, bf16),
            pltpu.VMEM(quarter, bf16),
            pltpu.VMEM(quarter, bf16),
            dma(2, 2, 6), dma(2, 2, 6), dma(2), dma(2), dma(2), dma(2), dma(2),
        ],
        compiler_params=linked(2),
        name="return",
    )(settled.reshape(torus), deposit)
    returned = returned.reshape(slots)

    return pl.pallas_call(
        finish_kernel,
        out_shape=(like(phase_box.shape, bf16), like(matrix_density.shape, f32)),
        in_specs=[HBM, VMEM, VMEM, VMEM],
        out_specs=(ANY, ANY),
        scratch_shapes=[
            pltpu.SMEM(box_corner.shape, jnp.int32),
            pltpu.VMEM(matrix_density.shape, f32),
            dma(phase_box.shape[0]),
            dma(2),
        ],
        compiler_params=quiet,
        name="finish",
    )(
        pltpu.with_memory_space_constraint(box_corner, pltpu.HBM), returned, deposit, matrix_density
    )


def solution(mesh):
    return jax.shard_map(
        per_device,
        mesh=mesh,
        in_specs=(P(("gx", "gy"), None, None), P("gx", "gy", None), P(None, ("gx", "gy"))),
        out_specs=(P(("gx", "gy"), None, None), P("gx", "gy", None)),
        check_vma=False,
    )
```

```python
import jax
import jax.numpy as jnp
from jax import lax
from jax.experimental import pallas as pl
from jax.experimental.pallas import tpu as pltpu
from jax.sharding import PartitionSpec as P

B = 32
LANES = 128
GROUP = LANES // B
SIDE = 4
TOGETHER = 8
RIM_CHUNKS = 4

def signal(axis, target):
    pl.semaphore_signal(
        pltpu.get_barrier_semaphore(),
        inc=1,
        device_id={axis: target},
        device_id_type=pl.DeviceIdType.MESH,
    )


def remote(src, dst, send, recv, axis, target):
    return pltpu.make_async_remote_copy(
        src_ref=src,
        dst_ref=dst,
        send_sem=send,
        recv_sem=recv,
        device_id={axis: target},
        device_id_type=pl.DeviceIdType.MESH,
    )


def greet():
    me, row = lax.axis_index("gy"), lax.axis_index("gx")
    columns, rows = lax.axis_size("gy"), lax.axis_size("gx")
    high, low = me // SIDE, lax.rem(me, SIDE)
    count = 0
    for step in (1, SIDE - 1):
        signal("gy", lax.rem(high + step, SIDE) * SIDE + low)
        signal("gy", high * SIDE + lax.rem(low + step, SIDE))
        count += 2
    for axis, at, size, step in (("gx", row, rows, 1), ("gx", row, rows, -1)):
        there = (at < size - 1) if step > 0 else (at > 0)
        count += there.astype(jnp.int32)

        @pl.when(there)
        def _():
            signal(axis, at + step)

    for step in (1, -1):
        far = (low == (SIDE - 1 if step > 0 else 0)) & (
            (me < columns - 1) if step > 0 else (me > 0)
        )
        count += far.astype(jnp.int32)

        @pl.when(far)
        def _():
            signal("gy", me + step)

    return count


class Exchange:
    def __init__(self, src, dst, stage, relay, send, recv, own, share_y):
        self.src, self.dst, self.stage, self.relay = src, dst, stage, relay
        self.send, self.recv, self.own = send, recv, own
        me = lax.axis_index("gy")
        self.at = (me // SIDE, lax.rem(me, SIDE))
        self.share = (SIDE // 2, share_y)
        self.rows = src.shape[2] // 2

    def turn(self, axis, step):
        return lax.rem(self.at[axis] + SIDE + step, SIDE)

    def device(self, axis, step):
        other, moved = self.at[1 - axis], self.turn(axis, step)
        return moved * SIDE + other if axis == 0 else other * SIDE + moved

    def whole(self, ref, half, first, second):
        rest = pl.ds(half * self.rows, self.rows)
        return ref.at[first, second, rest]

    def block(self, half, stage, goal, part):
        if stage == 1:
            return self.stage.at[half, part, goal]
        return self.whole(self.src, half, *((goal, part) if half == 0 else (part, goal)))

    def place(self, half, stage, origin, part):
        if stage == 0:
            return self.stage.at[half, origin, part]
        return self.whole(self.dst, half, *((part, origin) if half == 0 else (origin, part)))

    def copies(self, half, stage):
        axis = (half + stage) % 2
        share = self.share[axis]
        parts = (pl.ds(0, share), pl.ds(share, SIDE - share))
        sizes = (share, SIDE - share)
        every = pl.ds(0, SIDE)
        out = []
        for kind in ("relay", "direct", "forward"):
            for side in range(2):
                step = 1 if side == 0 else -1
                if kind == "direct":
                    src = self.block(half, stage, self.turn(axis, step), every)
                    dst = self.place(half, stage, self.at[axis], every)
                else:
                    hold = self.relay.at[half, stage, side, pl.ds(0, sizes[side])]
                    if kind == "relay":
                        src, dst = self.block(half, stage, self.turn(axis, 2), parts[side]), hold
                    else:
                        src = hold
                        dst = self.place(half, stage, self.turn(axis, -step), parts[side])
                at = (half, stage, len(out))
                out.append(
                    remote(src, dst, self.send.at[at], self.recv.at[at], "gy", self.device(axis, step))
                )
        return out

    def prepare(self):
        x, y = self.at
        self.stage[0, x] = self.src[x, :, : self.rows]
        self.stage[1, y] = self.src[:, y, self.rows :]

    def start(self, stage, half):
        copies = self.copies(half, stage)
        for copy in copies[:4]:
            copy.start()
        if stage == 1:
            self.kept(half).start()

    def forward(self, stage, half):
        copies = self.copies(half, stage)
        for side in range(2):
            copies[side].wait_recv()
            copies[4 + side].start()

    def arrive(self, stage, half):
        for copy in self.copies(half, stage)[2:]:
            copy.wait_recv()

    def kept(self, half):
        axis = (half + 1) % 2
        every = pl.ds(0, SIDE)
        return pltpu.make_async_copy(
            self.block(half, 1, self.at[axis], every),
            self.place(half, 1, self.at[axis], every),
            self.own.at[half],
        )

    def finish(self):
        for half in range(2):
            for stage in range(2):
                for copy in self.copies(half, stage):
                    copy.wait_send()
            self.kept(half).wait()


def gather_kernel(
    corner_in, phase_in, density_in, boxes, places, density,
    corner, phase, matrix, table, low, outbox, stage, relay, half, send, recv, table_send, table_recv,
    y_send, y_recv, x_send, x_recv, own, fetch,
):
    me, row = lax.axis_index("gy"), lax.axis_index("gx")
    columns, rows = lax.axis_size("gy"), lax.axis_size("gx")
    edge = low.shape[0]
    loads = [
        pltpu.make_async_copy(phase_in, phase, fetch.at[0]),
        pltpu.make_async_copy(density_in, matrix, fetch.at[1]),
        pltpu.make_async_copy(corner_in, corner, fetch.at[2]),
    ]
    for load in loads:
        load.start()
    part = edge // 2
    barrier = pltpu.get_barrier_semaphore()
    others = [lax.rem(me + k, columns) for k in range(1, columns)]
    senders = [lax.rem(me + columns - k, columns) for k in range(1, columns)]
    for target in others:
        signal("gy", target)

    @pl.when(row > 0)
    def _():
        signal("gx", row - 1)

    @pl.when(row < rows - 1)
    def _():
        signal("gx", row + 1)

    cells = range(phase.shape[0])
    loads[2].wait()
    home = [lax.div(corner[1, c], edge) for c in cells]
    lane = lax.broadcasted_iota(jnp.int32, table.shape[1:], 1)
    loads[0].wait()

    def fill(s, carry):
        source, found = jnp.int32(0), jnp.int32(0)
        for c in cells:
            source = jnp.where(home[c] == s, c, source)
            found = jnp.where(home[c] == s, 1, found)
        note = (
            corner[0, source] - row * edge,
            jnp.where(found > 0, corner[1, source] - s * edge, 0),
            corner[2, source],
            found,
        )
        line = jnp.zeros_like(lane)
        for k, value in enumerate(note):
            line = jnp.where(lane == k, value, line)
        table[s] = line
        outbox[s // SIDE, lax.rem(s, SIDE)] = phase[source]
        return carry

    lax.fori_loop(0, columns, fill, 0)
    loads[1].wait()
    low[...] = jnp.swapaxes(matrix[...], 0, 1).astype(low.dtype)

    @pl.when(me == columns - 1)
    def _():
        half[...] = jnp.zeros_like(half)

    boxes_out = Exchange(outbox, boxes, stage, relay, send, recv, own, 3)
    boxes_out.prepare()

    neighbours = (row > 0).astype(jnp.int32) + (row < rows - 1).astype(jnp.int32)
    pl.semaphore_wait(barrier, columns - 1 + neighbours)

    def along_y(k):
        rest = pl.ds(k * part, part)
        return remote(low.at[rest], half.at[rest], y_send.at[k], y_recv.at[k], "gy", me - 1)

    def along_x(k):
        src = low if k == 2 else half.at[pl.ds(k * part, part)]
        rest = pl.ds(0, edge) if k == 2 else pl.ds(edge + k * part, part)
        dst = density.at[rest, pl.ds(edge, edge)]
        return remote(src, dst, x_send.at[k], x_recv.at[k], "gx", row - 1)

    def keep(k):
        src = low if k == 2 else half.at[pl.ds(k * part, part)]
        rest = pl.ds(0, edge) if k == 2 else pl.ds(edge + k * part, part)
        return pltpu.make_async_copy(src, density.at[rest, pl.ds(0, edge)], own.at[2 + k])

    def start_y(k):
        @pl.when(me > 0)
        def _():
            along_y(k).start()

    def start_x(k):
        keep(k).start()

        @pl.when(row > 0)
        def _():
            along_x(k).start()

    def take_y(k):
        @pl.when(me < columns - 1)
        def _():
            along_y(k).wait_recv()

    for h in range(2):
        boxes_out.start(0, h)
    start_x(2)
    notes = [
        remote(table.at[target], places.at[me], table_send.at[k], table_recv.at[k], "gy", target)
        for k, target in enumerate(others)
    ]
    for note in notes:
        note.start()
    note = pltpu.make_async_copy(table.at[me], places.at[me], own.at[5])
    note.start()
    for h in range(2):
        boxes_out.forward(0, h)
    start_y(0)
    start_y(1)
    for h in range(2):
        boxes_out.arrive(0, h)
        boxes_out.start(1, h)
    take_y(0)
    start_x(0)
    for h in range(2):
        boxes_out.forward(1, h)
    take_y(1)
    start_x(1)
    for h in range(2):
        boxes_out.arrive(1, h)
    for k, sender in enumerate(senders):
        remote(
            table.at[me], places.at[sender], table_send.at[k], table_recv.at[k], "gy", sender
        ).wait_recv()
    for copy in notes:
        copy.wait_send()
    note.wait()
    for k in range(3):
        keep(k).wait()

        @pl.when(row > 0)
        def _():
            along_x(k).wait_send()

        @pl.when(row < rows - 1)
        def _():
            along_x(k).wait_recv()

    for k in range(2):

        @pl.when(me > 0)
        def _():
            along_y(k).wait_send()

    boxes_out.finish()


def rim_kernel(
    own, crowd, from_x, full, from_y, done, back,
    x_send, x_recv, y_send, y_recv, b_send, b_recv,
):
    me, row = lax.axis_index("gy"), lax.axis_index("gx")
    columns, rows = lax.axis_size("gy"), lax.axis_size("gx")
    edge = own.shape[1] // 2
    chunks, _, part, _ = full.shape
    count = 0
    for axis, at, size in (("gx", row, rows), ("gy", me, columns)):
        for there, target in ((at > 0, at - 1), (at < size - 1, at + 1)):
            count += there.astype(jnp.int32)

            @pl.when(there)
            def _():
                signal(axis, target)

    pl.semaphore_wait(pltpu.get_barrier_semaphore(), count)
    low, high = slice(0, edge), slice(edge, 2 * edge)
    ups = ((me < columns - 1, me > 0, me + 1, high, low), (me > 0, me < columns - 1, me - 1, low, high))

    def spill(c):
        src = own.at[:, pl.ds(edge + c * part, part)]
        return remote(src, from_x.at[c], x_send.at[c], x_recv.at[c], "gx", row + 1)

    def exchange(c, k):
        _, _, target, sent, _ = ups[k]
        return remote(
            full.at[c, sent], from_y.at[k, c], y_send.at[k, c], y_recv.at[k, c], "gy", target
        )

    def give(c):
        return remote(done.at[c], back.at[c], b_send.at[c], b_recv.at[c], "gx", row - 1)

    @pl.when(row < rows - 1)
    def _():
        for c in range(chunks):
            spill(c).start()

    for c in range(chunks):
        mine = slice(c * part, (c + 1) * part)

        @pl.when(row > 0)
        def _():
            spill(c).wait_recv()
            full[c] = own[:, mine] + from_x[c]

        @pl.when(row == 0)
        def _():
            full[c] = own[:, mine]

        for k in range(2):

            @pl.when(ups[k][0])
            def _():
                exchange(c, k).start()

    for c in range(chunks):
        for k in range(2):
            _, takes, _, _, into = ups[k]

            @pl.when(takes)
            def _():
                exchange(c, k).wait_recv()
                done[c, into] = full[c, into] + from_y[k, c]

            @pl.when(jnp.logical_not(takes))
            def _():
                done[c, into] = full[c, into]

        @pl.when(row > 0)
        def _():
            give(c).start()

        crowd[:, c * part : (c + 1) * part] = done[c].astype(jnp.float32)

    @pl.when(row == rows - 1)
    def _():
        crowd[:, edge:] = jnp.zeros((crowd.shape[0], edge, crowd.shape[2]), jnp.float32)

    @pl.when(row < rows - 1)
    def _():
        for c in range(chunks):
            give(c).wait_recv()
            crowd[:, edge + c * part : edge + (c + 1) * part] = back[c].astype(jnp.float32)

    for c in range(chunks):

        @pl.when(row < rows - 1)
        def _():
            spill(c).wait_send()

        for k in range(2):

            @pl.when(ups[k][0])
            def _():
                exchange(c, k).wait_send()

        @pl.when(row > 0)
        def _():
            give(c).wait_send()


def return_kernel(
    settled, wide, returned, deposit, stage, relay, from_x, outgoing, from_y,
    send, recv, x_send, x_recv, y_send, y_recv, own,
):
    me, row = lax.axis_index("gy"), lax.axis_index("gx")
    columns, rows = lax.axis_size("gy"), lax.axis_size("gx")
    edge = wide.shape[1] // 2
    count = greet()
    boxes_back = Exchange(settled, returned, stage, relay, send, recv, own, 1)
    boxes_back.prepare()
    pl.semaphore_wait(pltpu.get_barrier_semaphore(), count)
    halves = (slice(edge, 2 * edge), slice(0, edge))

    def along_x(k):
        return remote(
            wide.at[halves[k], pl.ds(edge, edge)], from_x.at[k], x_send.at[k], x_recv.at[k], "gx", row + 1
        )

    for h in range(2):
        boxes_back.start(0, h)

    @pl.when(row < rows - 1)
    def _():
        for k in range(2):
            along_x(k).start()

    for h in range(2):
        boxes_back.forward(0, h)

    @pl.when(row > 0)
    def _():
        along_x(0).wait_recv()
        outgoing[...] = wide[edge:, :edge] + from_x[0]

    @pl.when(row == 0)
    def _():
        outgoing[...] = wide[edge:, :edge]

    part = edge // 2

    def along_y(k):
        rest = pl.ds(k * part, part)
        return remote(
            outgoing.at[rest], from_y.at[rest], y_send.at[k], y_recv.at[k], "gy", me + 1
        )

    @pl.when(me < columns - 1)
    def _():
        for k in range(2):
            along_y(k).start()

    for h in range(2):
        boxes_back.arrive(0, h)
        boxes_back.start(1, h)

    @pl.when(row > 0)
    def _():
        along_x(1).wait_recv()
        deposit[...] = wide[:edge, :edge].astype(jnp.float32) + from_x[1].astype(jnp.float32)

    @pl.when(row == 0)
    def _():
        deposit[...] = wide[:edge, :edge].astype(jnp.float32)

    for h in range(2):
        boxes_back.forward(1, h)

    @pl.when(me > 0)
    def _():
        for k in range(2):
            along_y(k).wait_recv()
        deposit[...] = deposit[...] + from_y[...].astype(jnp.float32)

    for h in range(2):
        boxes_back.arrive(1, h)

    boxes_back.finish()

    @pl.when(me < columns - 1)
    def _():
        for k in range(2):
            along_y(k).wait_send()

    @pl.when(row < rows - 1)
    def _():
        for k in range(2):
            along_x(k).wait_send()


def fetch_places(table, places, sem):
    copy = pltpu.make_async_copy(table.at[:, 0], places, sem)
    copy.start()
    copy.wait()


def spread_base(base):
    row = lax.broadcasted_iota(jnp.int32, base.shape, 0)
    lane = lax.broadcasted_iota(jnp.int32, base.shape, 1)
    base[...] = jnp.where(row // LANES == lane // B, lax.rem(row, LANES) - lax.rem(lane, B), -1)


def stacked(boxes, s, here):
    v = jnp.concatenate(
        [boxes[s, :, j * LANES : (j + 1) * LANES] for j in range(B // GROUP)], 0
    )
    return jnp.where(here, v, jnp.zeros_like(v))


def add_box(wide, v, spread, lx, ly):
    placed = lax.dot_general(
        v, spread, (((1,), (1,)), ((), ())), preferred_element_type=jnp.float32
    )
    for j in range(B // GROUP):
        for i in range(GROUP):
            at = (ly + (GROUP * j + i), pl.ds(lx, B), slice(None))
            wide[at] = wide[at] + placed[j * B : (j + 1) * B, i * LANES : (i + 1) * LANES]


def take_box(field, spread, lx, ly):
    rows = []
    for j in range(B // GROUP):
        parts = [field[ly + (GROUP * j + i), pl.ds(lx, B), :] for i in range(GROUP)]
        rows.append(jnp.concatenate([p.astype(jnp.bfloat16) for p in parts], 1))
    return jnp.dot(jnp.concatenate(rows, 0), spread, preferred_element_type=jnp.float32)


def crowd_kernel(table, boxes, out, wide, base, places, sem):
    fetch_places(table, places, sem)
    wide[...] = jnp.zeros_like(wide)
    spread_base(base)

    def one(t, carry):
        slots = [t * TOGETHER + k for k in range(TOGETHER)]

        @pl.when(sum(places[s, 3] for s in slots) > 0)
        def _():
            squares, spreads = [], []
            for s in slots:
                v = stacked(boxes, s, places[s, 3] > 0).astype(jnp.float32)
                squares.append((v * v).astype(jnp.bfloat16))
                spreads.append(jnp.where(base[...] == places[s, 2], 1.0, 0.0).astype(jnp.bfloat16))
            for s, square, spread in zip(slots, squares, spreads):
                add_box(wide, square, spread, places[s, 0], places[s, 1])

        return carry

    lax.fori_loop(0, boxes.shape[0] // TOGETHER, one, 0)
    out[...] = wide[...].astype(out.dtype)


def update_kernel(
    table, boxes, crowd, low, settled, out, density, wide, base, taps, places, sem
):
    fetch_places(table, places, sem)
    density[...] = low[...].astype(jnp.float32)
    wide[...] = jnp.zeros_like(wide)
    spread_base(base)
    from_b = lax.broadcasted_iota(jnp.int32, taps.shape, 0) - LANES
    to_b = lax.broadcasted_iota(jnp.int32, taps.shape, 1)
    gap = from_b - to_b
    beside = (gap == B) | (gap == -B)
    same = (from_b >= 0) & (from_b < LANES) & (lax.rem(from_b + LANES, LANES) // B == to_b // B)
    along = same & ((gap == 1) | (gap == -1))
    taps[...] = jnp.where(gap == 0, -6.0, jnp.where(beside | along, 1.0, 0.0)).astype(taps.dtype)
    step = lax.rem(lax.broadcasted_iota(jnp.int32, (B * B // GROUP, LANES), 0), B)
    edge = jnp.zeros((B, LANES), jnp.bfloat16)
    total = B * B // GROUP

    def one(t, carry):
        slots = [t * TOGETHER + k for k in range(TOGETHER)]
        busy = sum(places[s, 3] for s in slots) > 0

        @pl.when(busy)
        def _():
            spreads, results = [], []
            for s in slots:
                lx, ly, lz = places[s, 0], places[s, 1], places[s, 2]
                spread = jnp.where(base[...] == lz, 1.0, 0.0).astype(jnp.bfloat16)
                cr = take_box(crowd, spread, lx, ly)
                dn = take_box(density, spread, lx, ly)
                v = stacked(boxes, s, places[s, 3] > 0)
                near = jnp.concatenate(
                    [
                        jnp.concatenate([edge, v[: total - B]], 0),
                        v,
                        jnp.concatenate([v[B:], edge], 0),
                    ],
                    1,
                )
                lap = jnp.dot(near, taps[...], preferred_element_type=jnp.float32)
                p = v.astype(jnp.float32)
                across = jnp.where(step < B - 1, pltpu.roll(p, total - 1, 0), 0.0) + jnp.where(
                    step > 0, pltpu.roll(p, 1, 0), 0.0
                )
                others = cr - p * p
                reaction = 4.0 * p * (1.0 - p) * (p - 0.5 + (dn - 0.5))
                fresh = p + 0.1 * (lap + across + reaction - 2.0 * p * others)
                fresh = fresh.astype(jnp.bfloat16)
                for j in range(B // GROUP):
                    settled[s, :, j * LANES : (j + 1) * LANES] = fresh[j * B : (j + 1) * B]
                spreads.append(spread)
                results.append(fresh)
            for s, fresh, spread in zip(slots, results, spreads):
                add_box(wide, fresh, spread, places[s, 0], places[s, 1])

        @pl.when(jnp.logical_not(busy))
        def _():
            for s in slots:
                settled[s] = jnp.zeros(settled.shape[1:], settled.dtype)

        return carry

    lax.fori_loop(0, boxes.shape[0] // TOGETHER, one, 0)
    out[...] = wide[...].astype(out.dtype)


def finish_kernel(
    corner_in, returned, deposit, matrix, phase_next, matrix_next, corner, turned, sem, fetch
):
    edge = matrix.shape[1]
    load = pltpu.make_async_copy(corner_in, corner, fetch.at[0])
    load.start()
    now = matrix[...]
    turned[...] = now - 0.5 * now * jnp.swapaxes(deposit[...], 0, 1)
    store = pltpu.make_async_copy(turned, matrix_next, fetch.at[1])
    store.start()
    load.wait()
    copies = [
        pltpu.make_async_copy(
            returned.at[lax.div(corner[1, c], edge)], phase_next.at[c], sem.at[c]
        )
        for c in range(phase_next.shape[0])
    ]
    for copy in copies:
        copy.start()
    store.wait()
    for copy in copies:
        copy.wait()


VMEM = pl.BlockSpec(memory_space=pltpu.VMEM)
ANY = pl.BlockSpec(memory_space=pl.ANY)
HBM = pl.BlockSpec(memory_space=pltpu.HBM)
LIMIT = 24 * 2**20


def like(shape, dtype):
    return jax.ShapeDtypeStruct(shape, dtype)


def dma(*shape):
    return pltpu.SemaphoreType.DMA(shape)


def linked(number):
    return pltpu.CompilerParams(
        collective_id=number, has_side_effects=True, vmem_limit_bytes=LIMIT
    )


def per_device(phase_box, matrix_density, box_corner):
    slab_rows, slab_cols, grid_depth = matrix_density.shape
    peers = lax.axis_size("gy")
    bf16, f32 = jnp.bfloat16, jnp.float32
    slots = (peers,) + phase_box.shape[1:]
    notes = (peers, 8, LANES)
    torus = (SIDE, SIDE) + phase_box.shape[1:]
    rows = (phase_box.shape[1] // 2,) + phase_box.shape[2:]
    moving = [pltpu.VMEM((2, SIDE, SIDE) + rows, bf16), pltpu.VMEM((2, 2, 2, SIDE - 1) + rows, bf16)]
    wide = (2 * slab_cols, 2 * slab_rows, grid_depth)
    strips = (RIM_CHUNKS, 2 * slab_cols, slab_rows // RIM_CHUNKS, grid_depth)
    quarter = (slab_cols, slab_rows, grid_depth)
    boxes, places, density = pl.pallas_call(
        gather_kernel,
        out_shape=(like(torus, bf16), like(notes, jnp.int32), like(wide, bf16)),
        in_specs=[HBM, HBM, HBM],
        out_specs=(ANY, ANY, ANY),
        scratch_shapes=[
            pltpu.SMEM(box_corner.shape, jnp.int32),
            pltpu.VMEM(phase_box.shape, bf16),
            pltpu.VMEM(matrix_density.shape, f32),
            pltpu.VMEM(notes, jnp.int32),
            pltpu.VMEM(quarter, bf16),
            pltpu.VMEM(torus, bf16),
        ]
        + moving
        + [
            pltpu.VMEM(quarter, bf16),
            dma(2, 2, 6), dma(2, 2, 6), dma(peers - 1), dma(peers - 1),
            dma(2), dma(2), dma(3), dma(3), dma(6), dma(3),
        ],
        compiler_params=linked(0),
        name="gather",
    )(
        *(pltpu.with_memory_space_constraint(a, pltpu.HBM) for a in (box_corner, phase_box, matrix_density))
    )
    boxes = boxes.reshape(slots)

    spread = pltpu.VMEM((GROUP * LANES, LANES), jnp.int32)
    taps = pltpu.VMEM((3 * LANES, LANES), bf16)
    spots = [pltpu.SMEM((peers, LANES), jnp.int32), dma()]
    quiet = pltpu.CompilerParams(vmem_limit_bytes=LIMIT)
    crowd = pl.pallas_call(
        crowd_kernel,
        out_shape=like(wide, bf16),
        in_specs=[ANY, VMEM],
        out_specs=VMEM,
        scratch_shapes=[pltpu.VMEM(wide, f32), spread] + spots,
        compiler_params=quiet,
        name="crowd",
    )(places, boxes)

    crowd = pl.pallas_call(
        rim_kernel,
        out_shape=like(wide, f32),
        in_specs=[VMEM],
        out_specs=VMEM,
        scratch_shapes=[
            pltpu.VMEM(strips, bf16),
            pltpu.VMEM(strips, bf16),
            pltpu.VMEM((2, RIM_CHUNKS, slab_cols) + strips[2:], bf16),
            pltpu.VMEM(strips, bf16),
            pltpu.VMEM(strips, bf16),
            dma(RIM_CHUNKS), dma(RIM_CHUNKS), dma(2, RIM_CHUNKS), dma(2, RIM_CHUNKS),
            dma(RIM_CHUNKS), dma(RIM_CHUNKS),
        ],
        compiler_params=linked(1),
        name="rim",
    )(crowd)

    settled, deposit = pl.pallas_call(
        update_kernel,
        out_shape=(like(slots, bf16), like(wide, bf16)),
        in_specs=[ANY, VMEM, VMEM, VMEM],
        out_specs=(VMEM, VMEM),
        scratch_shapes=[pltpu.VMEM(wide, f32), pltpu.VMEM(wide, f32), spread, taps] + spots,
        compiler_params=quiet,
        name="update",
    )(places, boxes, crowd, density)

    returned, deposit = pl.pallas_call(
        return_kernel,
        out_shape=(like(torus, bf16), like(quarter, f32)),
        in_specs=[VMEM, VMEM],
        out_specs=(ANY, VMEM),
        scratch_shapes=moving
        + [
            pltpu.VMEM((2,) + quarter, bf16),
            pltpu.VMEM(quarter, bf16),
            pltpu.VMEM(quarter, bf16),
            dma(2, 2, 6), dma(2, 2, 6), dma(2), dma(2), dma(2), dma(2), dma(2),
        ],
        compiler_params=linked(2),
        name="return",
    )(settled.reshape(torus), deposit)
    returned = returned.reshape(slots)

    return pl.pallas_call(
        finish_kernel,
        out_shape=(like(phase_box.shape, bf16), like(matrix_density.shape, f32)),
        in_specs=[HBM, VMEM, VMEM, VMEM],
        out_specs=(ANY, ANY),
        scratch_shapes=[
            pltpu.SMEM(box_corner.shape, jnp.int32),
            pltpu.VMEM(matrix_density.shape, f32),
            dma(phase_box.shape[0]),
            dma(2),
        ],
        compiler_params=quiet,
        name="finish",
    )(
        pltpu.with_memory_space_constraint(box_corner, pltpu.HBM), returned, deposit, matrix_density
    )


def solution(mesh):
    return jax.shard_map(
        per_device,
        mesh=mesh,
        in_specs=(P(("gx", "gy"), None, None), P("gx", "gy", None), P(None, ("gx", "gy"))),
        out_specs=(P(("gx", "gy"), None, None), P("gx", "gy", None)),
        check_vma=False,
    )
```
